128 devices in a mesh: vocab: 64 (over y, z, x), dp: 2 (over core).
Axes of the slice: x: 4, y: 4, z: 4, core: 2. Of those that a mesh axis runs over, the one named last changes fastest.
Arguments:
- hidden: bfloat16 [2048, 4096], P('dp', 'vocab'), may hold values from -64 to 64
- head_weight: bfloat16 [65536, 4096], P('vocab'), may hold values from -0.28125 to 0.28125
- targets: int32 [2048], P('dp'), may hold values from 0 to 65535
- loss_cot: float32 [2048], P('dp'), may hold values from -40 to 40
Outputs:
- tok_loss: float32 [2048], P('dp')
- hidden_grad: bfloat16 [2048, 4096], P('dp', 'vocab')
- g_factor: float32 [65536, 1024], P(('vocab', 'dp'))
- a_factor: float32 [4096, 4096], P('vocab')
The draws below stay inside these ranges and needn't reach their ends.
All inputs are finite; a program needn't handle non-finite values.
Results may differ from the reference program's by a relative error of at most 0.0049.
Values may be sent and summed in bfloat16 or wider, within the bound.
No kernel may reach another device: no remote copies, remote signals or barrier semaphores. Data moves between devices by JAX's collectives and lax.ppermute only.
A program may use at most 128 MiB of HBM per device.

```python
import math
import jax
import jax.numpy as jnp
import numpy as np
from jax import lax

D = 4096
VOC_DEV = 1024
TOK_DEV = 1024
VOCAB = 65536
TOKENS = 2048
N_VOCAB = 64


def weight_row(key, row_index):
    spread = 3.0 / D ** 0.5
    drawn = jax.random.normal(jax.random.fold_in(jax.random.fold_in(key, 7), row_index), (D,), jnp.float32) * spread
    return jnp.clip(drawn, -5.9 * spread, 5.9 * spread)


def draw_head_weight(key, part):
    rows = jax.vmap(lambda row_index: weight_row(key, row_index))(jnp.arange(VOCAB, dtype=jnp.int32))
    return rows.astype(jnp.bfloat16)


def draw_hidden(key, part):
    drawn = jax.random.normal(jax.random.fold_in(key, 11), (TOKENS, D), jnp.float32)
    aligned_count = TOKENS // 16
    row_ids = jnp.arange(aligned_count, dtype=jnp.int32) * 16
    chosen = jax.random.randint(jax.random.fold_in(key, 13), (aligned_count,), 0, VOCAB - 1)
    first = jax.vmap(lambda row_index: weight_row(key, row_index))(chosen)
    second = jax.vmap(lambda row_index: weight_row(key, row_index))(chosen + 1)
    level = jax.random.uniform(jax.random.fold_in(key, 14), (aligned_count, 1), jnp.float32, 110.0, 250.0)
    aligned = level * (first + 0.99 * second) / 9.0
    drawn = drawn.at[row_ids].set(aligned)
    drawn = jnp.clip(drawn, -63.5, 63.5)
    return drawn.astype(jnp.bfloat16)


def with_ends(values, own_key, low, largest):
    longest = values.shape.index(max(values.shape))
    spots = []
    for shift in (0, 1):
        where = [jax.random.randint(jax.random.fold_in(own_key, axis), (), 0, length) for axis, length in enumerate(values.shape)]
        where[longest] = (where[longest] + shift) % values.shape[longest]
        spots.append(tuple(where))
    return values.at[spots[0]].set(low).at[spots[1]].set(largest)


def level_of(key, dims, cuts, smallest, top_value):
    factor_of, own = 1.0, jax.random.fold_in(key, 6)
    for dim, shards_of in cuts:
        steps = jnp.exp(jax.random.uniform(jax.random.fold_in(own, dim), (shards_of,), jnp.float32, smallest / len(cuts), top_value / len(cuts)))
        factor_of = factor_of * jnp.repeat(steps, dims[dim] // shards_of).reshape([-1 if axis == dim else 1 for axis in range(len(dims))])
    return factor_of


def cumulative_ranks(number_of, slope):
    portions = [(1 << 20) // math.isqrt(grade ** slope) + 1 for grade in range(1, number_of + 1)]
    width = 1 + sum(portions) // (1 << 30)
    return np.cumsum(np.array([max(1, weight // width) for weight in portions]))


def ranked(stream_key, shape, number_of, skew):
    grid = cumulative_ranks(number_of, skew)
    ticket = jax.random.randint(jax.random.fold_in(stream_key, 1), shape, 0, int(grid[number_of - 1]))
    grade = jnp.searchsorted(jnp.asarray(grid, jnp.int32), ticket, side="right")
    return jax.random.permutation(jax.random.fold_in(stream_key, 2), number_of)[grade].astype(jnp.int32)


def scatter_about(stream_key, shape, scale, most, split=(), kind=jnp.bfloat16):
    result = scale * jax.random.normal(stream_key, shape, jnp.float32)
    if split:
        result = result * level_of(stream_key, shape, split, -0.22, 0.18)
    return jnp.clip(result, -most, most).astype(kind)


def setup_inputs(seed: int = 0) -> dict:
    arg_keys = jax.random.split(jax.random.key(seed), 5)
    hidden = draw_hidden(jax.random.fold_in(arg_keys[4], 71), 0)
    head_weight = draw_head_weight(jax.random.fold_in(arg_keys[4], 71), 0)
    targets = with_ends(ranked(arg_keys[2], (TOKENS,), VOCAB, 2), jax.random.fold_in(arg_keys[2], 3), 0, VOCAB - 1).astype(jnp.int32)
    loss_cot = scatter_about(arg_keys[3], (TOKENS,), 8.0, 40.0, ((0, 2),), jnp.float32)
    return {"hidden": hidden, "head_weight": head_weight, "targets": targets, "loss_cot": loss_cot}


def block_gram(block):
    return jnp.dot(block.T, block, preferred_element_type=jnp.float32) / TOK_DEV


def reference(hidden, head_weight, targets, loss_cot):
    logits = jnp.dot(hidden, head_weight.T, preferred_element_type=jnp.float32)
    row_top = jnp.max(logits, axis=1)
    scaled = jnp.exp(logits - row_top[:, None])
    row_total = jnp.sum(scaled, axis=1)
    onehot = targets[:, None] == jnp.arange(VOCAB, dtype=jnp.int32)[None, :]
    target_logit = jnp.sum(jnp.where(onehot, logits, jnp.float32(0.0)), axis=1)
    tok_loss = jnp.log(row_total) + row_top - target_logit
    prob = scaled / row_total[:, None]
    out_grad = (loss_cot[:, None] * (prob - onehot.astype(jnp.float32))).astype(jnp.bfloat16)
    hidden_grad = jnp.dot(out_grad, head_weight, preferred_element_type=jnp.float32).astype(jnp.bfloat16)
    blocks = jnp.transpose(out_grad.reshape(TOKENS, N_VOCAB, VOC_DEV), (1, 0, 2))
    g_factor = lax.map(block_gram, blocks).reshape(VOCAB, VOC_DEV)
    a_factor = jnp.dot(hidden.T, hidden, preferred_element_type=jnp.float32) / TOK_DEV
    return tok_loss, hidden_grad, g_factor, a_factor
```

```python
import jax
import jax.numpy as jnp
import numpy as np
from jax import lax
from jax.sharding import Mesh
from jax.sharding import PartitionSpec as P

TOK_DEV = 1024
VOCAB = ("vocab_0", "vocab_1", "vocab_2")
ALL = ("vocab_0", "vocab_1", "vocab_2", "dp")

ORDER = (((0, 1), (2, 3)), ((0, 3), (1, 2)))
SMALL = (((0, 1), (2, 3)), ((0, 3), (1, 2)))
LARGE = (((1, 2), (0, 3)), ((0, 1), (3, 2)))


def cubes(pairs):
    groups = []
    for core in (0, 1):
        for a in pairs[core]:
            for b in pairs[core]:
                for c in pairs[core]:
                    groups.append(
                        [((y * 4 + z) * 4 + x) * 2 + core for y in a for z in b for x in c]
                    )
    return groups


def chip_order(core):
    o = ORDER[core]
    bits = (0, 1)
    return [
        (o[jy][iy] * 4 + o[jz][iz]) * 4 + o[jx][ix]
        for jy in bits for jz in bits for jx in bits
        for iy in bits for iz in bits for ix in bits
    ]


SMALL_CUBES = cubes(SMALL)
LARGE_CUBES = cubes(LARGE)
CHIPS = np.array([chip_order(0), chip_order(1)], np.int32)
PLACES = np.argsort(CHIPS, axis=1).astype(np.int32)
SWAP = [(0, 1), (1, 0)]


def exchanged(x, groups):
    return lax.all_to_all(x, ALL, 0, 0, axis_index_groups=groups, tiled=True)


def to_cube(x, groups):
    return exchanged(jnp.broadcast_to(x[None], (8, *x.shape)), groups)


def body(hidden, head_weight, targets, loss_cot):
    vocab_rows, width = head_weight.shape
    own = hidden.T
    feats, tokens = own.shape
    core = lax.axis_index("dp")
    some = to_cube(own, SMALL_CUBES).reshape(8 * feats, tokens)
    gathered = to_cube(some, LARGE_CUBES).reshape(64, feats, tokens)
    everything = jnp.take(gathered, jnp.asarray(PLACES)[core], axis=0).reshape(width, tokens)
    logits = jnp.dot(head_weight, everything, preferred_element_type=jnp.float32)
    a_part = lax.dot_general(
        own, everything, (((1,), (1,)), ((), ())), preferred_element_type=jnp.float32
    )
    offset = lax.axis_index(VOCAB) * vocab_rows
    onehot = jnp.arange(vocab_rows, dtype=jnp.int32)[:, None] == (targets - offset)[None, :]
    local_top = jnp.max(logits, axis=0)
    local_target = jnp.sum(jnp.where(onehot, logits, jnp.float32(0.0)), axis=0)
    local_total = jnp.sum(jnp.exp(logits - local_top[None, :]), axis=0)
    stats = jnp.stack([local_top, local_total, local_target])
    stats = lax.all_to_all(
        jnp.broadcast_to(stats.reshape(1, 24, 128), (64, 24, 128)), VOCAB, 0, 0, tiled=True
    ).reshape(64, 3, tokens)
    row_top = jnp.max(stats[:, 0], axis=0)
    row_total = jnp.sum(stats[:, 1] * jnp.exp(stats[:, 0] - row_top[None, :]), axis=0)
    target_logit = jnp.sum(stats[:, 2], axis=0)
    tok_loss = jnp.log(row_total) + row_top - target_logit
    prob = jnp.exp(logits - row_top[None, :]) / row_total[None, :]
    out_grad = (loss_cot[None, :] * (prob - onehot.astype(jnp.float32))).astype(jnp.bfloat16)
    part = lax.dot_general(
        head_weight, out_grad, (((0,), (0,)), ((), ())), preferred_element_type=jnp.float32
    ).astype(jnp.bfloat16)
    part = jnp.take(part.reshape(64, feats, tokens), jnp.asarray(CHIPS)[core], axis=0)
    part = exchanged(part.reshape(8, 8 * feats, tokens), LARGE_CUBES)
    part = jnp.sum(part.astype(jnp.float32), axis=0).astype(jnp.bfloat16)
    part = exchanged(part.reshape(8, feats, tokens), SMALL_CUBES)
    hidden_grad = jnp.sum(part.astype(jnp.float32), axis=0).astype(jnp.bfloat16).T
    other = lax.ppermute(out_grad, "dp", SWAP)
    rows = vocab_rows // 2

    def gram(x):
        mine = lax.dynamic_slice_in_dim(x, core * rows, rows, 0)
        return lax.dot_general(mine, x, (((1,), (1,)), ((), ())), preferred_element_type=jnp.float32)

    g_factor = (gram(out_grad) + gram(other)) / TOK_DEV
    a_factor = (a_part + lax.ppermute(a_part, "dp", SWAP)) / TOK_DEV
    return (tok_loss, hidden_grad, g_factor, a_factor)


def solution(mesh):
    finer = Mesh(mesh.devices.reshape(4, 4, 4, mesh.shape["dp"]), ALL)
    return jax.shard_map(
        body,
        mesh=finer,
        in_specs=(P("dp", VOCAB), P(VOCAB, None), P("dp"), P("dp")),
        out_specs=(P("dp"), P("dp", VOCAB), P(ALL, None), P(VOCAB, None)),
        check_vma=False,
    )
```

```python
import jax
import jax.numpy as jnp
import numpy as np
from jax import lax
from jax.experimental import pallas as pl
from jax.experimental.pallas import tpu as pltpu
from jax.sharding import Mesh
from jax.sharding import PartitionSpec as P

TOK_DEV = 1024
HALVES = 2
VOCAB = ("vocab_0", "vocab_1", "vocab_2")
ALL = ("vocab_0", "vocab_1", "vocab_2", "dp")

ORDER = (((0, 1), (2, 3)), ((0, 3), (1, 2)))
SMALL = (((0, 1), (2, 3)), ((0, 3), (1, 2)))
LARGE = (((1, 2), (0, 3)), ((0, 1), (3, 2)))


def cubes(pairs):
    groups = []
    for core in (0, 1):
        for a in pairs[core]:
            for b in pairs[core]:
                for c in pairs[core]:
                    groups.append(
                        [((y * 4 + z) * 4 + x) * 2 + core for y in a for z in b for x in c]
                    )
    return groups


def steps_of(core):
    flat = [c for pair in ORDER[core] for c in pair]
    return [flat.index(c) // 2 for c in range(4)] + [flat.index(c) % 2 for c in range(4)]


SMALL_CUBES = cubes(SMALL)
LARGE_CUBES = cubes(LARGE)
STEPS = np.array([steps_of(0), steps_of(1)], np.int32)
SWAP = [(0, 1), (1, 0)]
F32 = jnp.float32
BF16 = jnp.bfloat16


def exchanged(x, groups):
    return lax.all_to_all(x, ALL, 0, 0, axis_index_groups=groups, tiled=True)


def to_cube(x, groups):
    return exchanged(jnp.broadcast_to(x[None], (8, *x.shape)), groups)


def place_of(steps, chip):
    y, z, x = chip // 16, (chip // 4) % 4, chip % 4
    large = (steps[y] * 2 + steps[z]) * 2 + steps[x]
    small = (steps[4 + y] * 2 + steps[4 + z]) * 2 + steps[4 + x]
    return large * 8 + small


def logits_kernel(steps, got, w, tgt, logits, stats, h, top, total, hit, sem):
    step = pl.program_id(0)
    rows, tokens = logits.shape

    @pl.when(step == 0)
    def _():
        def start(chip, carry):
            src = pl.multiple_of(place_of(steps, chip) * 64, 64)
            dst = pl.multiple_of(chip * 64, 64)
            pltpu.make_async_copy(got.at[pl.ds(src, 64)], h.at[pl.ds(dst, 64)], sem).start()
            return carry

        lax.fori_loop(0, 64, start, 0)
        top[...] = jnp.full(top.shape, -jnp.inf, F32)
        total[...] = jnp.zeros(total.shape, F32)
        hit[...] = jnp.zeros(hit.shape, F32)
        pltpu.make_async_copy(got, h, sem).wait()

    block = jnp.dot(w[...], h[...], preferred_element_type=F32)
    logits[...] = block
    at = lax.broadcasted_iota(jnp.int32, block.shape, 0) + step * rows
    hit[...] += jnp.sum(jnp.where(at == tgt[...], block, F32(0.0)), axis=0, keepdims=True)
    now = jnp.maximum(top[...], jnp.max(block, axis=0, keepdims=True))
    added = jnp.sum(jnp.exp(block - now), axis=0, keepdims=True)
    total[...] = total[...] * jnp.exp(top[...] - now) + added
    top[...] = now

    @pl.when(step == pl.num_programs(0) - 1)
    def _():
        lse = top[...] + jnp.log(total[...])
        both = [r[:, k : k + 128] for r in (lse, hit[...]) for k in range(0, tokens, 128)]
        stats[...] = jnp.broadcast_to(jnp.concatenate(both, axis=0)[None], stats.shape)


def logits_of(steps, got, w, tgt):
    vocab_rows, width = w.shape
    tokens = got.shape[1]
    rows = 256
    lines = 2 * tokens // 128
    return pl.pallas_call(
        logits_kernel,
        grid_spec=pltpu.PrefetchScalarGridSpec(
            num_scalar_prefetch=1,
            grid=(vocab_rows // rows,),
            in_specs=[
                pl.BlockSpec(memory_space=pl.ANY),
                pl.BlockSpec((rows, width), lambda i, s: (i, 0)),
                pl.BlockSpec((1, tokens), lambda i, s: (0, 0)),
            ],
            out_specs=[
                pl.BlockSpec((rows, tokens), lambda i, s: (i, 0)),
                pl.BlockSpec((64, lines, 128), lambda i, s: (0, 0, 0)),
            ],
            scratch_shapes=[
                pltpu.VMEM((width, tokens), BF16),
                pltpu.VMEM((1, tokens), F32),
                pltpu.VMEM((1, tokens), F32),
                pltpu.VMEM((1, tokens), F32),
                pltpu.SemaphoreType.DMA,
            ],
        ),
        out_shape=[
            jax.ShapeDtypeStruct((vocab_rows, tokens), F32),
            jax.ShapeDtypeStruct((64, lines, 128), F32),
        ],
        compiler_params=pltpu.CompilerParams(
            dimension_semantics=("arbitrary",), vmem_limit_bytes=48 << 20
        ),
        cost_estimate=pl.CostEstimate(
            flops=2 * vocab_rows * width * tokens,
            bytes_accessed=2 * width * (vocab_rows + tokens) + 4 * vocab_rows * tokens,
            transcendentals=vocab_rows * tokens,
        ),
    )(steps, got, w, tgt)


def grad_kernel(steps, stats, logits, cot, tgt, wt, part, grad, loss):
    step = pl.program_id(0)
    vocab_rows, tokens = logits.shape
    lines = tokens // 128

    @pl.when(step == 0)
    def _():
        lse = stats[:, :lines]
        top = jnp.max(lse, axis=0)
        full = top + jnp.log(jnp.sum(jnp.exp(lse - top[None]), axis=0))
        tok = full - jnp.sum(stats[:, lines:], axis=0)
        full = jnp.concatenate([full[k : k + 1] for k in range(lines)], axis=1)
        loss[...] = jnp.concatenate([tok[k : k + 1] for k in range(lines)], axis=1)
        for k in range(0, vocab_rows, 128):
            block = logits[k : k + 128, :]
            at = lax.broadcasted_iota(jnp.int32, block.shape, 0) + k
            one = jnp.where(at == tgt[...], F32(1.0), F32(0.0))
            grad[k : k + 128, :] = (cot[...] * (jnp.exp(block - full) - one)).astype(BF16)

    out = jnp.dot(wt[...], grad[...], preferred_element_type=F32).astype(BF16)
    for x in range(4):
        part[steps[x], steps[4 + x]] = out[64 * x : 64 * x + 64]


def grads_of(steps, stats, logits, cot, tgt, wt):
    width, vocab_rows = wt.shape
    tokens = logits.shape[1]
    whole = lambda *shape: pl.BlockSpec(shape, lambda i, s: (0,) * len(shape))
    part, grad, loss = pl.pallas_call(
        grad_kernel,
        grid_spec=pltpu.PrefetchScalarGridSpec(
            num_scalar_prefetch=1,
            grid=(16,),
            in_specs=[
                whole(*stats.shape),
                whole(vocab_rows, tokens),
                whole(1, tokens),
                whole(1, tokens),
                pl.BlockSpec((width // 16, vocab_rows), lambda i, s: (i, 0)),
            ],
            out_specs=[
                pl.BlockSpec(
                    (None, None, 2, None, None, 2, 64, tokens),
                    lambda i, s: (s[i // 4], s[i % 4], 0, s[4 + i // 4], s[4 + i % 4], 0, 0, 0),
                ),
                whole(vocab_rows, tokens),
                whole(1, tokens),
            ],
        ),
        out_shape=[
            jax.ShapeDtypeStruct((2, 2, 2, 2, 2, 2, 64, tokens), BF16),
            jax.ShapeDtypeStruct((vocab_rows, tokens), BF16),
            jax.ShapeDtypeStruct((1, tokens), F32),
        ],
        compiler_params=pltpu.CompilerParams(
            dimension_semantics=("arbitrary",), vmem_limit_bytes=48 << 20
        ),
        cost_estimate=pl.CostEstimate(
            flops=2 * vocab_rows * width * tokens,
            bytes_accessed=2 * width * (vocab_rows + tokens) + 6 * vocab_rows * tokens,
            transcendentals=vocab_rows * tokens,
        ),
    )(steps, stats, logits, cot, tgt, wt)
    return part.reshape(8, width // 8, tokens), grad, loss


def sum_kernel(pieces, out):
    out[...] = jnp.sum(pieces[...].astype(F32), axis=0).astype(BF16)


def summed(pieces):
    count, rows, tokens = pieces.shape
    step = min(rows, 64)
    return pl.pallas_call(
        sum_kernel,
        grid=(rows // step,),
        in_specs=[pl.BlockSpec((count, step, tokens), lambda i: (0, i, 0))],
        out_specs=pl.BlockSpec((step, tokens), lambda i: (i, 0)),
        out_shape=jax.ShapeDtypeStruct((rows, tokens), BF16),
        compiler_params=pltpu.CompilerParams(
            dimension_semantics=("arbitrary",), vmem_limit_bytes=16 << 20
        ),
        cost_estimate=pl.CostEstimate(
            flops=count * rows * tokens, bytes_accessed=2 * (count + 1) * rows * tokens,
            transcendentals=0,
        ),
    )(pieces)


def a_kernel(steps, own, *refs):
    *halves, out = refs
    done = None
    for k, half in enumerate(halves):
        tokens = half.shape[-1]
        block = jnp.concatenate([half[steps[x], steps[4 + x]] for x in range(4)], axis=0)
        now = lax.dot_general(
            own[:, k * tokens : (k + 1) * tokens], block, (((1,), (1,)), ((), ())),
            preferred_element_type=F32,
        )
        done = now if done is None else done + now
    out[...] = done


def a_part_of(steps, own, halves):
    feats, all_tokens = own.shape
    tokens = all_tokens // len(halves)
    width = halves[0].shape[0]
    half = pl.BlockSpec(
        (None, None, 2, None, None, 2, 64, tokens),
        lambda i, s: (s[i // 4], s[i % 4], 0, s[4 + i // 4], s[4 + i % 4], 0, 0, 0),
    )
    return pl.pallas_call(
        a_kernel,
        grid_spec=pltpu.PrefetchScalarGridSpec(
            num_scalar_prefetch=1,
            grid=(16,),
            in_specs=[pl.BlockSpec((feats, all_tokens), lambda i, s: (0, 0))] + [half] * len(halves),
            out_specs=pl.BlockSpec((feats, width // 16), lambda i, s: (0, i)),
        ),
        out_shape=jax.ShapeDtypeStruct((feats, width), F32),
        compiler_params=pltpu.CompilerParams(
            dimension_semantics=("arbitrary",), vmem_limit_bytes=16 << 20
        ),
        cost_estimate=pl.CostEstimate(
            flops=2 * feats * width * all_tokens, bytes_accessed=2 * width * all_tokens,
            transcendentals=0,
        ),
    )(steps, own, *[h.reshape(2, 2, 2, 2, 2, 2, 64, tokens) for h in halves])


def body(hidden, head_weight, targets, loss_cot):
    vocab_rows, width = head_weight.shape
    own = hidden.T
    feats, tokens = own.shape
    core = lax.axis_index("dp")
    steps = jnp.where(core == 0, jnp.asarray(STEPS[0]), jnp.asarray(STEPS[1]))
    some = to_cube(own, SMALL_CUBES).reshape(8 * feats, tokens)
    part_tokens = tokens // HALVES
    cuts = [slice(k * part_tokens, (k + 1) * part_tokens) for k in range(HALVES)]
    tgt = (targets - lax.axis_index(VOCAB) * vocab_rows)[None, :]
    cot = loss_cot[None, :]
    wt = head_weight.T
    gathered = [to_cube(some[:, c], LARGE_CUBES).reshape(width, part_tokens) for c in cuts]
    made = [logits_of(steps, g, head_weight, tgt[:, c]) for g, c in zip(gathered, cuts)]
    stats = [lax.all_to_all(s, VOCAB, 0, 0, tiled=True) for _, s in made]
    grads = [
        grads_of(steps, s, l, cot[:, c], tgt[:, c], wt) for s, (l, _), c in zip(stats, made, cuts)
    ]
    parts = [summed(exchanged(p, LARGE_CUBES)) for p, _, _ in grads]
    parts = [summed(exchanged(p.reshape(8, feats, part_tokens), SMALL_CUBES)) for p in parts]
    hidden_grad = jnp.concatenate(parts, axis=1).T
    tok_loss = jnp.concatenate([l[0] for _, _, l in grads])
    rows = vocab_rows // 2

    def gram(x):
        mine = lax.dynamic_slice_in_dim(x, core * rows, rows, 0)
        return lax.dot_general(mine, x, (((1,), (1,)), ((), ())), preferred_element_type=F32)

    mine = jnp.concatenate([g for _, g, _ in grads], axis=1)
    g_factor = (gram(mine) + gram(lax.ppermute(mine, "dp", SWAP))) / TOK_DEV
    a_part = a_part_of(steps, own, gathered)
    a_factor = (a_part + lax.ppermute(a_part, "dp", SWAP)) / TOK_DEV
    return (tok_loss, hidden_grad, g_factor, a_factor)


def solution(mesh):
    finer = Mesh(mesh.devices.reshape(4, 4, 4, mesh.shape["dp"]), ALL)
    return jax.shard_map(
        body,
        mesh=finer,
        in_specs=(P("dp", VOCAB), P(VOCAB, None), P("dp"), P("dp")),
        out_specs=(P("dp"), P("dp", VOCAB), P(ALL, None), P(VOCAB, None)),
        check_vma=False,
    )
```

```python
import jax
import jax.numpy as jnp
import numpy as np
from jax import lax
from jax.experimental import pallas as pl
from jax.experimental.pallas import tpu as pltpu
from jax.sharding import Mesh
from jax.sharding import PartitionSpec as P

TOK_DEV = 1024
VOCAB = ("vocab_0", "vocab_1", "vocab_2")
ALL = ("vocab_0", "vocab_1", "vocab_2", "dp")

SMALL = (((0, 1), (2, 3)), ((0, 3), (1, 2)))
LARGE = (((1, 2), (0, 3)), ((0, 1), (3, 2)))
SWAP = [(0, 1), (1, 0)]
F32 = jnp.float32
BF16 = jnp.bfloat16

GROUPS = (
    ((0, 64, 0), (1, 64, 0), (2, 48, 0)),
    ((2, 16, 48), (3, 64, 0), (4, 64, 0), (5, 32, 0)),
    ((5, 32, 32), (6, 64, 0), (7, 64, 0)),
)
SIZES = [sum(rows for _, rows, _ in group) for group in GROUPS]
STARTS = [0, SIZES[0], SIZES[0] + SIZES[1]]


def device(y, z, x, core):
    return ((y * 4 + z) * 4 + x) * 2 + core


def small_cubes():
    return [
        [device(y, z, x, core) for y in a for z in b for x in c]
        for core in (0, 1) for a in SMALL[core] for b in SMALL[core] for c in SMALL[core]
    ]


def partner(core, c):
    return next(p[1 - p.index(c)] for p in LARGE[core] if c in p)


def spots():
    return [(y, z, x, core) for y in range(4) for z in range(4) for x in range(4) for core in (0, 1)]


def large_pairs(axis):
    out = []
    for at in spots():
        to = list(at)
        to[axis] = partner(at[3], at[axis])
        out.append((device(*at), device(*to)))
    return out


def chip_table():
    table = np.zeros((128, 3, 8, 8), np.int32)
    for at in spots():
        core = at[3]
        for group in range(3):
            for l in range(8):
                for s in range(8):
                    chip = 0
                    for axis in range(3):
                        c = at[axis]
                        if l >> ((axis - group) % 3) & 1:
                            c = partner(core, c)
                        pair = next(p for p in SMALL[core] if c in p)
                        chip = chip * 4 + pair[s >> (2 - axis) & 1]
                    table[device(*at), group, l, s] = chip
    return table.reshape(128, 192)


SMALL_CUBES = small_cubes()
LARGE_PAIRS = [large_pairs(axis) for axis in range(3)]
CHIPS = chip_table()


def small_stage(x):
    return lax.all_to_all(x, ALL, 0, 0, axis_index_groups=SMALL_CUBES, tiled=True)


def gathered_groups(some):
    held = [some[start : start + size] for start, size in zip(STARTS, SIZES)]
    got = [lax.ppermute(held[g], ALL, LARGE_PAIRS[g]) for g in range(3)]
    first = [jnp.concatenate([h, r]) for h, r in zip(held, got)]
    second = [lax.ppermute(first[g], ALL, LARGE_PAIRS[(g + 1) % 3]) for g in range(3)]
    third = [
        [lax.ppermute(part, ALL, LARGE_PAIRS[(g + 2) % 3]) for part in (first[g], second[g])]
        for g in range(3)
    ]
    return [[first[g], second[g], *third[g]] for g in range(3)]


def summed_groups(sends, keeps):
    for step in (2, 1, 0):
        got = [lax.ppermute(sends[g], ALL, LARGE_PAIRS[(g + step) % 3]) for g in range(3)]
        now = [k + r.astype(F32) for k, r in zip(keeps, got)]
        if step:
            half = 1 << (step - 1)
            sends = [n[half:].astype(BF16) for n in now]
            keeps = [n[:half] for n in now]
    return jnp.concatenate([n[0].astype(BF16) for n in now])


def logits_kernel(chips, *refs):
    got, (w, tgt, logits, stats, every, h, top, total, hit, sem, sem_out) = refs[:12], refs[12:]
    step = pl.program_id(0)
    rows, tokens = logits.shape

    @pl.when(step == 0)
    def _():
        for g, group in enumerate(GROUPS):
            for l in range(8):
                src, at = got[4 * g + l // 2], (l % 2) * SIZES[g]
                for s, count, first in group:
                    dst = pl.multiple_of(chips[64 * g + 8 * l + s] * 64 + first, 16)
                    pltpu.make_async_copy(
                        src.at[pl.ds(at, count)], h.at[pl.ds(dst, count)], sem
                    ).start()
                    at += count
        top[...] = jnp.full(top.shape, -jnp.inf, F32)
        total[...] = jnp.zeros(total.shape, F32)
        hit[...] = jnp.zeros(hit.shape, F32)
        pltpu.make_async_copy(every, h, sem).wait()
        pltpu.make_async_copy(h, every, sem_out).start()

    block = jnp.dot(w[...], h[...], preferred_element_type=F32)
    logits[...] = block
    at = lax.broadcasted_iota(jnp.int32, block.shape, 0) + step * rows
    hit[...] += jnp.sum(jnp.where(at == tgt[...], block, F32(0.0)), axis=0, keepdims=True)
    now = jnp.maximum(top[...], jnp.max(block, axis=0, keepdims=True))
    added = jnp.sum(jnp.exp(block - now), axis=0, keepdims=True)
    total[...] = total[...] * jnp.exp(top[...] - now) + added
    top[...] = now

    @pl.when(step == pl.num_programs(0) - 1)
    def _():
        lse = top[...] + jnp.log(total[...])
        both = [r[:, k : k + 128] for r in (lse, hit[...]) for k in range(0, tokens, 128)]
        stats[...] = jnp.broadcast_to(jnp.concatenate(both, axis=0)[None], stats.shape)
        pltpu.make_async_copy(h, every, sem_out).wait()


def logits_of(chips, got, w, tgt):
    vocab_rows, width = w.shape
    tokens = tgt.shape[1]
    rows = 256
    lines = 2 * tokens // 128
    return pl.pallas_call(
        logits_kernel,
        grid_spec=pltpu.PrefetchScalarGridSpec(
            num_scalar_prefetch=1,
            grid=(vocab_rows // rows,),
            in_specs=[pl.BlockSpec(memory_space=pl.ANY)] * len(got) + [
                pl.BlockSpec((rows, width), lambda i, s: (i, 0)),
                pl.BlockSpec((1, tokens), lambda i, s: (0, 0)),
            ],
            out_specs=[
                pl.BlockSpec((rows, tokens), lambda i, s: (i, 0)),
                pl.BlockSpec((64, lines, 128), lambda i, s: (0, 0, 0)),
                pl.BlockSpec(memory_space=pl.ANY),
            ],
            scratch_shapes=[
                pltpu.VMEM((width, tokens), BF16),
                pltpu.VMEM((1, tokens), F32),
                pltpu.VMEM((1, tokens), F32),
                pltpu.VMEM((1, tokens), F32),
                pltpu.SemaphoreType.DMA,
                pltpu.SemaphoreType.DMA,
            ],
        ),
        out_shape=[
            jax.ShapeDtypeStruct((vocab_rows, tokens), F32),
            jax.ShapeDtypeStruct((64, lines, 128), F32),
            jax.ShapeDtypeStruct((width, tokens), BF16),
        ],
        compiler_params=pltpu.CompilerParams(
            dimension_semantics=("arbitrary",), vmem_limit_bytes=40 << 20
        ),
        cost_estimate=pl.CostEstimate(
            flops=2 * vocab_rows * width * tokens,
            bytes_accessed=2 * width * (vocab_rows + 2 * tokens) + 4 * vocab_rows * tokens,
            transcendentals=vocab_rows * tokens,
        ),
    )(chips, *got, w, tgt)


def signal_kernel(stats, logits, cot, tgt, grad, loss, row):
    step = pl.program_id(0)
    rows, tokens = logits.shape
    lines = tokens // 128

    @pl.when(step == 0)
    def _():
        lse = stats[:, :lines]
        top = jnp.max(lse, axis=0)
        full = top + jnp.log(jnp.sum(jnp.exp(lse - top[None]), axis=0))
        tok = full - jnp.sum(stats[:, lines:], axis=0)
        row[...] = jnp.concatenate([full[k : k + 1] for k in range(lines)], axis=1)
        loss[...] = jnp.concatenate([tok[k : k + 1] for k in range(lines)], axis=1)

    block = logits[...]
    at = lax.broadcasted_iota(jnp.int32, block.shape, 0) + step * rows
    one = jnp.where(at == tgt[...], F32(1.0), F32(0.0))
    grad[...] = (cot[...] * (jnp.exp(block - row[...]) - one)).astype(BF16)


def signal_of(stats, logits, cot, tgt):
    vocab_rows, tokens = logits.shape
    rows = 128
    whole = lambda *shape: pl.BlockSpec(shape, lambda i: (0,) * len(shape))
    return pl.pallas_call(
        signal_kernel,
        grid=(vocab_rows // rows,),
        in_specs=[
            whole(*stats.shape),
            pl.BlockSpec((rows, tokens), lambda i: (i, 0)),
            whole(1, tokens),
            whole(1, tokens),
        ],
        out_specs=[pl.BlockSpec((rows, tokens), lambda i: (i, 0)), whole(1, tokens)],
        out_shape=[
            jax.ShapeDtypeStruct((vocab_rows, tokens), BF16),
            jax.ShapeDtypeStruct((1, tokens), F32),
        ],
        scratch_shapes=[pltpu.VMEM((1, tokens), F32)],
        compiler_params=pltpu.CompilerParams(
            dimension_semantics=("arbitrary",), vmem_limit_bytes=16 << 20
        ),
        cost_estimate=pl.CostEstimate(
            flops=8 * vocab_rows * tokens, bytes_accessed=6 * vocab_rows * tokens,
            transcendentals=vocab_rows * tokens,
        ),
    )(stats, logits, cot, tgt)


def grad_kernel(chips, *refs):
    pieces, (grad, send, keep) = refs[:-3], refs[-3:]
    step = pl.program_id(0)
    rows = jnp.concatenate([p[...] for p in pieces], axis=0)
    out = jnp.dot(rows, grad[...], preferred_element_type=F32)

    @pl.when(step < 4)
    def _():
        send[...] = out.astype(BF16)

    @pl.when(step >= 4)
    def _():
        keep[...] = out


def piece_spec(group, s, count, first, vocab_rows):
    place = lambda i, t: (t[64 * group + 8 * ((i + 4) % 8) + s], first // count, 0)
    return pl.BlockSpec((None, count, vocab_rows), place)


def grads_of(chips, wt, grad, group):
    vocab_rows, tokens = grad.shape
    size = SIZES[group]
    wt = wt.reshape(64, -1, vocab_rows)
    pieces = [piece_spec(group, s, count, first, vocab_rows) for s, count, first in GROUPS[group]]
    return pl.pallas_call(
        grad_kernel,
        grid_spec=pltpu.PrefetchScalarGridSpec(
            num_scalar_prefetch=1,
            grid=(8,),
            in_specs=pieces + [pl.BlockSpec((vocab_rows, tokens), lambda i, t: (0, 0))],
            out_specs=[
                pl.BlockSpec((None, size, tokens), lambda i, t: (jnp.minimum(i, 3), 0, 0)),
                pl.BlockSpec((None, size, tokens), lambda i, t: (jnp.maximum(i - 4, 0), 0, 0)),
            ],
        ),
        out_shape=[
            jax.ShapeDtypeStruct((4, size, tokens), BF16),
            jax.ShapeDtypeStruct((4, size, tokens), F32),
        ],
        compiler_params=pltpu.CompilerParams(
            dimension_semantics=("arbitrary",), vmem_limit_bytes=32 << 20
        ),
        cost_estimate=pl.CostEstimate(
            flops=16 * vocab_rows * size * tokens,
            bytes_accessed=16 * size * vocab_rows + 24 * size * tokens,
            transcendentals=0,
        ),
    )(chips, *[wt] * len(pieces), grad)


def body(hidden, head_weight, targets, loss_cot):
    vocab_rows, width = head_weight.shape
    own = hidden.T
    feats, tokens = own.shape
    core = lax.axis_index("dp")
    chips = lax.dynamic_index_in_dim(jnp.asarray(CHIPS), lax.axis_index(ALL), 0, keepdims=False)
    tgt = (targets - lax.axis_index(VOCAB) * vocab_rows)[None, :]
    wt = head_weight.T
    some = small_stage(jnp.broadcast_to(own[None], (8, feats, tokens))).reshape(8 * feats, tokens)
    got = [array for group in gathered_groups(some) for array in group]
    logits, stats, every = logits_of(chips, got, head_weight, tgt)
    stats = lax.all_to_all(stats, VOCAB, 0, 0, tiled=True)
    grad, tok_loss = signal_of(stats, logits, loss_cot[None, :], tgt)
    pieces = [grads_of(chips, wt, grad, group) for group in range(3)]
    part = summed_groups([send for send, _ in pieces], [keep for _, keep in pieces])
    part = small_stage(part.reshape(8, feats, tokens))
    hidden_grad = jnp.sum(part.astype(F32), axis=0).astype(BF16).T
    rows = vocab_rows // 2

    def gram(x):
        mine = lax.dynamic_slice_in_dim(x, core * rows, rows, 0)
        return lax.dot_general(mine, x, (((1,), (1,)), ((), ())), preferred_element_type=F32)

    g_factor = (gram(grad) + gram(lax.ppermute(grad, "dp", SWAP))) / TOK_DEV
    a_part = lax.dot_general(own, every, (((1,), (1,)), ((), ())), preferred_element_type=F32)
    a_factor = (a_part + lax.ppermute(a_part, "dp", SWAP)) / TOK_DEV
    return (tok_loss[0], hidden_grad, g_factor, a_factor)


def solution(mesh):
    finer = Mesh(mesh.devices.reshape(4, 4, 4, mesh.shape["dp"]), ALL)
    return jax.shard_map(
        body,
        mesh=finer,
        in_specs=(P("dp", VOCAB), P(VOCAB, None), P("dp"), P("dp")),
        out_specs=(P("dp"), P("dp", VOCAB), P(ALL, None), P(VOCAB, None)),
        check_vma=False,
    )
```

```python
import jax
import jax.numpy as jnp
import numpy as np
from jax import lax
from jax.experimental import pallas as pl
from jax.experimental.pallas import tpu as pltpu
from jax.sharding import Mesh
from jax.sharding import PartitionSpec as P

TOK_DEV = 1024
VOCAB = ("vocab_0", "vocab_1", "vocab_2")
ALL = ("vocab_0", "vocab_1", "vocab_2", "dp")

SMALL = (((0, 1), (2, 3)), ((0, 3), (1, 2)))
LARGE = (((1, 2), (0, 3)), ((0, 1), (3, 2)))
SWAP = [(0, 1), (1, 0)]
F32 = jnp.float32
BF16 = jnp.bfloat16

GROUPS = (
    ((0, 64, 0), (1, 64, 0), (2, 48, 0)),
    ((2, 16, 48), (3, 64, 0), (4, 64, 0), (5, 32, 0)),
    ((5, 32, 32), (6, 64, 0), (7, 64, 0)),
)
SIZES = [sum(rows for _, rows, _ in group) for group in GROUPS]
STARTS = [0, SIZES[0], SIZES[0] + SIZES[1]]


def device(y, z, x, core):
    return ((y * 4 + z) * 4 + x) * 2 + core


def small_cubes():
    return [
        [device(y, z, x, core) for y in a for z in b for x in c]
        for core in (0, 1) for a in SMALL[core] for b in SMALL[core] for c in SMALL[core]
    ]


def partner(core, c):
    return next(p[1 - p.index(c)] for p in LARGE[core] if c in p)


def spots():
    return [(y, z, x, core) for y in range(4) for z in range(4) for x in range(4) for core in (0, 1)]


def large_pairs(axis):
    out = []
    for at in spots():
        to = list(at)
        to[axis] = partner(at[3], at[axis])
        out.append((device(*at), device(*to)))
    return out


def chip_table():
    table = np.zeros((128, 3, 8, 8), np.int32)
    for at in spots():
        core = at[3]
        for group in range(3):
            for l in range(8):
                for s in range(8):
                    chip = 0
                    for axis in range(3):
                        c = at[axis]
                        if l >> ((axis - group) % 3) & 1:
                            c = partner(core, c)
                        pair = next(p for p in SMALL[core] if c in p)
                        chip = chip * 4 + pair[s >> (2 - axis) & 1]
                    table[device(*at), group, l, s] = chip
    return table.reshape(128, 192)


SMALL_CUBES = small_cubes()
LARGE_PAIRS = [large_pairs(axis) for axis in range(3)]
CHIPS = chip_table()


def small_stage(x):
    return lax.all_to_all(x, ALL, 0, 0, axis_index_groups=SMALL_CUBES, tiled=True)


def gathered_groups(some):
    held = [some[start : start + size] for start, size in zip(STARTS, SIZES)]
    got = [lax.ppermute(held[g], ALL, LARGE_PAIRS[g]) for g in range(3)]
    first = [jnp.concatenate([h, r]) for h, r in zip(held, got)]
    second = [lax.ppermute(first[g], ALL, LARGE_PAIRS[(g + 1) % 3]) for g in range(3)]
    third = [
        [lax.ppermute(part, ALL, LARGE_PAIRS[(g + 2) % 3]) for part in (first[g], second[g])]
        for g in range(3)
    ]
    return [[first[g], second[g], *third[g]] for g in range(3)]


def summed_groups(sends, keeps):
    for step in (2, 1, 0):
        got = [lax.ppermute(sends[g], ALL, LARGE_PAIRS[(g + step) % 3]) for g in range(3)]
        now = [k.astype(F32) + r.astype(F32) for k, r in zip(keeps, got)]
        if step:
            half = 1 << (step - 1)
            sends = [n[half:].astype(BF16) for n in now]
            keeps = [n[:half] for n in now]
    return jnp.concatenate([n[0].astype(BF16) for n in now])


def gather_copies(chips, got, h):
    quarters = []
    for large in (0, 1):
        for small in (0, 1):
            copies = []
            for g, group in enumerate(GROUPS):
                for l in range(8):
                    if l >> (-g % 3) & 1 != large:
                        continue
                    src, at = got[4 * g + l // 2], (l % 2) * SIZES[g]
                    for s, count, first in group:
                        if s >> 2 == small:
                            dst = pl.multiple_of(chips[64 * g + 8 * l + s] * 64 + first, 16)
                            copies.append((src.at[pl.ds(at, count)], h.at[pl.ds(dst, count)]))
                        at += count
            quarters.append((chips[8 * large + 4 * small] // 16, copies))
    return quarters


def logits_kernel(chips, *refs):
    got, (w, tgt, logits, stats, h, top, total, hit, sem) = refs[:12], refs[12:]
    step = pl.program_id(0)
    rows, tokens = logits.shape
    quarter = h.shape[0] // 4
    quarters = gather_copies(chips, got, h)

    @pl.when(step == 0)
    def _():
        for q, (_, copies) in enumerate(quarters):
            for src, dst in copies:
                pltpu.make_async_copy(src, dst, sem.at[q]).start()
        top[...] = jnp.full(top.shape, -jnp.inf, F32)
        total[...] = jnp.zeros(total.shape, F32)
        hit[...] = jnp.zeros(hit.shape, F32)

    block = None
    for q, (y, _) in enumerate(quarters):
        some = h.at[pl.ds(0, quarter)]
        pl.when(step == 0)(lambda: pltpu.make_async_copy(some, some, sem.at[q]).wait())
        here = pl.ds(pl.multiple_of(y * quarter, quarter), quarter)
        now = jnp.dot(w[:, here], h[here, :], preferred_element_type=F32)
        block = now if block is None else block + now
    logits[...] = block
    at = lax.broadcasted_iota(jnp.int32, block.shape, 0) + step * rows
    hit[...] += jnp.sum(jnp.where(at == tgt[...], block, F32(0.0)), axis=0, keepdims=True)
    now = jnp.maximum(top[...], jnp.max(block, axis=0, keepdims=True))
    added = jnp.sum(jnp.exp(block - now), axis=0, keepdims=True)
    total[...] = total[...] * jnp.exp(top[...] - now) + added
    top[...] = now

    @pl.when(step == pl.num_programs(0) - 1)
    def _():
        lse = top[...] + jnp.log(total[...])
        both = [r[:, k : k + 128] for r in (lse, hit[...]) for k in range(0, tokens, 128)]
        stats[...] = jnp.broadcast_to(jnp.concatenate(both, axis=0)[None], stats.shape)


LOGIT_ROWS = 256


def logits_of(chips, got, w, tgt):
    vocab_rows, width = w.shape
    tokens = tgt.shape[1]
    rows = LOGIT_ROWS
    lines = 2 * tokens // 128
    return pl.pallas_call(
        logits_kernel,
        grid_spec=pltpu.PrefetchScalarGridSpec(
            num_scalar_prefetch=1,
            grid=(vocab_rows // rows,),
            in_specs=[pl.BlockSpec(memory_space=pl.ANY)] * len(got) + [
                pl.BlockSpec((rows, width), lambda i, s: (i, 0)),
                pl.BlockSpec((1, tokens), lambda i, s: (0, 0)),
            ],
            out_specs=[
                pl.BlockSpec((rows, tokens), lambda i, s: (i, 0)),
                pl.BlockSpec((64, lines, 128), lambda i, s: (0, 0, 0)),
            ],
            scratch_shapes=[
                pltpu.VMEM((width, tokens), BF16),
                pltpu.VMEM((1, tokens), F32),
                pltpu.VMEM((1, tokens), F32),
                pltpu.VMEM((1, tokens), F32),
                pltpu.SemaphoreType.DMA((4,)),
            ],
        ),
        out_shape=[
            pltpu.HBM((vocab_rows, tokens), F32),
            jax.ShapeDtypeStruct((64, lines, 128), F32),
        ],
        compiler_params=pltpu.CompilerParams(
            dimension_semantics=("arbitrary",), vmem_limit_bytes=40 << 20
        ),
        cost_estimate=pl.CostEstimate(
            flops=2 * vocab_rows * width * tokens,
            bytes_accessed=2 * width * (vocab_rows + tokens) + 4 * vocab_rows * tokens,
            transcendentals=vocab_rows * tokens,
        ),
    )(chips, *got, w, tgt)


def a_kernel(chips, *refs):
    got, (own, out, h, sem) = refs[:12], refs[12:]
    for _, copies in gather_copies(chips, got, h):
        for src, dst in copies:
            pltpu.make_async_copy(src, dst, sem).start()
    pltpu.make_async_copy(h, h, sem).wait()
    out[...] = lax.dot_general(
        own[...], h[...], (((1,), (1,)), ((), ())), preferred_element_type=F32
    )


def a_part_of(chips, got, own):
    feats, tokens = own.shape
    width = 64 * feats
    return pl.pallas_call(
        a_kernel,
        grid_spec=pltpu.PrefetchScalarGridSpec(
            num_scalar_prefetch=1,
            grid=(),
            in_specs=[pl.BlockSpec(memory_space=pl.ANY)] * len(got)
            + [pl.BlockSpec(memory_space=pltpu.VMEM)],
            out_specs=pl.BlockSpec(memory_space=pltpu.VMEM),
            scratch_shapes=[pltpu.VMEM((width, tokens), BF16), pltpu.SemaphoreType.DMA],
        ),
        out_shape=jax.ShapeDtypeStruct((feats, width), F32),
        compiler_params=pltpu.CompilerParams(vmem_limit_bytes=32 << 20),
        cost_estimate=pl.CostEstimate(
            flops=2 * feats * width * tokens, bytes_accessed=2 * width * tokens, transcendentals=0
        ),
    )(chips, *got, own)


def signal_kernel(stats, logits, cot, tgt, grad, loss, row):
    step = pl.program_id(0)
    rows, tokens = logits.shape
    lines = tokens // 128

    @pl.when(step == 0)
    def _():
        lse = stats[:, :lines]
        top = jnp.max(lse, axis=0)
        full = top + jnp.log(jnp.sum(jnp.exp(lse - top[None]), axis=0))
        tok = full - jnp.sum(stats[:, lines:], axis=0)
        row[...] = jnp.concatenate([full[k : k + 1] for k in range(lines)], axis=1)
        loss[...] = jnp.concatenate([tok[k : k + 1] for k in range(lines)], axis=1)

    block = logits[...]
    at = lax.broadcasted_iota(jnp.int32, block.shape, 0) + step * rows
    one = jnp.where(at == tgt[...], F32(1.0), F32(0.0))
    grad[...] = (cot[...] * (jnp.exp(block - row[...]) - one)).astype(BF16)


def signal_of(stats, logits, cot, tgt):
    vocab_rows, tokens = logits.shape
    rows = 128
    whole = lambda *shape: pl.BlockSpec(shape, lambda i: (0,) * len(shape))
    return pl.pallas_call(
        signal_kernel,
        grid=(vocab_rows // rows,),
        in_specs=[
            whole(*stats.shape),
            pl.BlockSpec((rows, tokens), lambda i: (i, 0)),
            whole(1, tokens),
            whole(1, tokens),
        ],
        out_specs=[pl.BlockSpec((rows, tokens), lambda i: (i, 0)), whole(1, tokens)],
        out_shape=[
            jax.ShapeDtypeStruct((vocab_rows, tokens), BF16),
            jax.ShapeDtypeStruct((1, tokens), F32),
        ],
        scratch_shapes=[pltpu.VMEM((1, tokens), F32)],
        compiler_params=pltpu.CompilerParams(
            dimension_semantics=("arbitrary",), vmem_limit_bytes=16 << 20
        ),
        cost_estimate=pl.CostEstimate(
            flops=8 * vocab_rows * tokens, bytes_accessed=6 * vocab_rows * tokens,
            transcendentals=vocab_rows * tokens,
        ),
    )(stats, logits, cot, tgt)


def grad_kernel(chips, *refs):
    pieces, (grad, *outs), (stage, sem) = refs[:8], refs[8:-2], refs[-2:]
    step = pl.program_id(0)
    rows = jnp.concatenate([p[...] for p in pieces], axis=0)
    stage[step] = jnp.dot(rows, grad[...], preferred_element_type=F32).astype(BF16)
    for g in range(3):
        send, keep = outs[2 * g : 2 * g + 2]
        l = sum(((step >> axis) & 1) << ((axis - g) % 3) for axis in range(3))
        src = stage.at[step, pl.ds(STARTS[g], SIZES[g])]

        @pl.when(l >= 4)
        def _():
            pltpu.make_async_copy(src, send.at[l - 4], sem.at[2 * g]).start()

        @pl.when(l < 4)
        def _():
            pltpu.make_async_copy(src, keep.at[l], sem.at[2 * g + 1]).start()

    @pl.when(step == pl.num_programs(0) - 1)
    def _():
        for k, out in enumerate(outs):
            pltpu.make_async_copy(out, out, sem.at[k]).wait()


def grads_of(chips, wt, grad):
    vocab_rows, tokens = grad.shape
    width = wt.shape[0]
    feats = width // 64
    spec = lambda s: pl.BlockSpec((None, feats, vocab_rows), lambda i, t: (t[8 * i + s], 0, 0))
    outs = pl.pallas_call(
        grad_kernel,
        grid_spec=pltpu.PrefetchScalarGridSpec(
            num_scalar_prefetch=1,
            grid=(8,),
            in_specs=[spec(s) for s in range(8)]
            + [pl.BlockSpec((vocab_rows, tokens), lambda i, t: (0, 0))],
            out_specs=[pl.BlockSpec(memory_space=pl.ANY)] * 6,
            scratch_shapes=[
                pltpu.VMEM((8, 8 * feats, tokens), BF16), pltpu.SemaphoreType.DMA((6,)),
            ],
        ),
        out_shape=[pltpu.HBM((4, size, tokens), BF16) for size in SIZES for _ in range(2)],
        compiler_params=pltpu.CompilerParams(
            dimension_semantics=("arbitrary",), vmem_limit_bytes=40 << 20
        ),
        cost_estimate=pl.CostEstimate(
            flops=2 * vocab_rows * width * tokens,
            bytes_accessed=2 * width * (vocab_rows + tokens),
            transcendentals=0,
        ),
    )(chips, *[wt.reshape(64, feats, vocab_rows)] * 8, grad)
    return outs[::2], outs[1::2]


def body(hidden, head_weight, targets, loss_cot):
    vocab_rows, width = head_weight.shape
    own = hidden.T
    feats, tokens = own.shape
    core = lax.axis_index("dp")
    chips = lax.dynamic_index_in_dim(jnp.asarray(CHIPS), lax.axis_index(ALL), 0, keepdims=False)
    tgt = (targets - lax.axis_index(VOCAB) * vocab_rows)[None, :]
    wt, tgt = lax.optimization_barrier((head_weight.T, tgt))
    some = small_stage(jnp.broadcast_to(own[None], (8, feats, tokens))).reshape(8 * feats, tokens)
    got = [array for group in gathered_groups(some) for array in group]
    logits, stats = logits_of(chips, got, head_weight, tgt)
    stats = lax.all_to_all(stats, VOCAB, 0, 0, tiled=True)
    grad, tok_loss = signal_of(stats, logits, loss_cot[None, :], tgt)
    part = summed_groups(*grads_of(chips, wt, grad))
    part = small_stage(part.reshape(8, feats, tokens))
    hidden_grad = jnp.sum(part.astype(F32), axis=0).astype(BF16).T
    rows = vocab_rows // 2

    def gram(x):
        mine = lax.dynamic_slice_in_dim(x, core * rows, rows, 0)
        return lax.dot_general(mine, x, (((1,), (1,)), ((), ())), preferred_element_type=F32)

    g_factor = (gram(grad) + gram(lax.ppermute(grad, "dp", SWAP))) / TOK_DEV
    a_part = a_part_of(chips, got, own)
    a_factor = (a_part + lax.ppermute(a_part, "dp", SWAP)) / TOK_DEV
    return (tok_loss[0], hidden_grad, g_factor, a_factor)


def solution(mesh):
    finer = Mesh(mesh.devices.reshape(4, 4, 4, mesh.shape["dp"]), ALL)
    return jax.shard_map(
        body,
        mesh=finer,
        in_specs=(P("dp", VOCAB), P(VOCAB, None), P("dp"), P("dp")),
        out_specs=(P("dp"), P("dp", VOCAB), P(ALL, None), P(VOCAB, None)),
        check_vma=False,
    )
```

```python
import jax
import jax.numpy as jnp
import numpy as np
from jax import lax
from jax.experimental import pallas as pl
from jax.experimental.pallas import tpu as pltpu
from jax.sharding import Mesh
from jax.sharding import PartitionSpec as P

TOK_DEV = 1024
VOCAB = ("vocab_0", "vocab_1", "vocab_2")
ALL = ("vocab_0", "vocab_1", "vocab_2", "dp")

SMALL = (((0, 1), (2, 3)), ((0, 3), (1, 2)))
LARGE = (((1, 2), (0, 3)), ((0, 1), (3, 2)))
SWAP = [(0, 1), (1, 0)]
F32 = jnp.float32
BF16 = jnp.bfloat16

GROUPS = (
    ((0, 64, 0), (1, 64, 0), (2, 48, 0)),
    ((2, 16, 48), (3, 64, 0), (4, 64, 0), (5, 32, 0)),
    ((5, 32, 32), (6, 64, 0), (7, 64, 0)),
)
SIZES = [sum(rows for _, rows, _ in group) for group in GROUPS]
STARTS = [0, SIZES[0], SIZES[0] + SIZES[1]]


def device(y, z, x, core):
    return ((y * 4 + z) * 4 + x) * 2 + core


def small_cubes():
    return [
        [device(y, z, x, core) for y in a for z in b for x in c]
        for core in (0, 1) for a in SMALL[core] for b in SMALL[core] for c in SMALL[core]
    ]


def partner(core, c):
    return next(p[1 - p.index(c)] for p in LARGE[core] if c in p)


def spots():
    return [(y, z, x, core) for y in range(4) for z in range(4) for x in range(4) for core in (0, 1)]


def large_pairs(axis):
    out = []
    for at in spots():
        to = list(at)
        to[axis] = partner(at[3], at[axis])
        out.append((device(*at), device(*to)))
    return out


def chip_table():
    table = np.zeros((128, 3, 8, 8), np.int32)
    for at in spots():
        core = at[3]
        for group in range(3):
            for l in range(8):
                for s in range(8):
                    chip = 0
                    for axis in range(3):
                        c = at[axis]
                        if l >> ((axis - group) % 3) & 1:
                            c = partner(core, c)
                        pair = next(p for p in SMALL[core] if c in p)
                        chip = chip * 4 + pair[s >> (2 - axis) & 1]
                    table[device(*at), group, l, s] = chip
    return table.reshape(128, 192)


SMALL_CUBES = small_cubes()
LARGE_PAIRS = [large_pairs(axis) for axis in range(3)]
CHIPS = chip_table()


def small_stage(x):
    return lax.all_to_all(x, ALL, 0, 0, axis_index_groups=SMALL_CUBES, tiled=True)


def gathered_groups(some):
    held = [some[start : start + size] for start, size in zip(STARTS, SIZES)]
    got = [lax.ppermute(held[g], ALL, LARGE_PAIRS[g]) for g in range(3)]
    first = [jnp.concatenate([h, r]) for h, r in zip(held, got)]
    second = [lax.ppermute(first[g], ALL, LARGE_PAIRS[(g + 1) % 3]) for g in range(3)]
    third = [
        [lax.ppermute(part, ALL, LARGE_PAIRS[(g + 2) % 3]) for part in (first[g], second[g])]
        for g in range(3)
    ]
    return [[first[g], second[g], *third[g]] for g in range(3)]


def add_up(*terms):
    total = terms[0].astype(F32)
    for term in terms[1:]:
        total = total + term.astype(F32)
    return total.astype(BF16)


def summed_groups(sends, keeps):
    trade = lambda x, g, step: lax.ppermute(x, ALL, LARGE_PAIRS[(g + step) % 3])
    far = [trade(sends[g], g, 2) for g in range(3)]
    mid = [trade(add_up(keeps[g][2:], far[g][2:]), g, 1) for g in range(3)]
    near = [trade(add_up(keeps[g][1], far[g][1], mid[g][1]), g, 0) for g in range(3)]
    return jnp.concatenate(
        [add_up(keeps[g][0], far[g][0], mid[g][0], near[g]) for g in range(3)]
    )


def gather_copies(chips, got, h):
    quarters = []
    for large in (0, 1):
        for small in (0, 1):
            copies = []
            for g, group in enumerate(GROUPS):
                for l in range(8):
                    if l >> (-g % 3) & 1 != large:
                        continue
                    src, at = got[4 * g + l // 2], (l % 2) * SIZES[g]
                    for s, count, first in group:
                        if s >> 2 == small:
                            dst = pl.multiple_of(chips[64 * g + 8 * l + s] * 64 + first, 16)
                            copies.append((src.at[pl.ds(at, count)], h.at[pl.ds(dst, count)]))
                        at += count
            quarters.append((chips[8 * large + 4 * small] // 16, copies))
    return quarters


def a_kernel(chips, *refs):
    got, (own, out, h, sem) = refs[:12], refs[12:]
    for _, copies in gather_copies(chips, got, h):
        for src, dst in copies:
            pltpu.make_async_copy(src, dst, sem).start()
    pltpu.make_async_copy(h, h, sem).wait()
    out[...] = lax.dot_general(
        own[...], h[...], (((1,), (1,)), ((), ())), preferred_element_type=F32
    )


def a_part_of(chips, got, own):
    feats, tokens = own.shape
    width = 64 * feats
    return pl.pallas_call(
        a_kernel,
        grid_spec=pltpu.PrefetchScalarGridSpec(
            num_scalar_prefetch=1,
            grid=(),
            in_specs=[pl.BlockSpec(memory_space=pl.ANY)] * len(got)
            + [pl.BlockSpec(memory_space=pltpu.VMEM)],
            out_specs=pl.BlockSpec(memory_space=pltpu.VMEM),
            scratch_shapes=[pltpu.VMEM((width, tokens), BF16), pltpu.SemaphoreType.DMA],
        ),
        out_shape=jax.ShapeDtypeStruct((feats, width), F32),
        compiler_params=pltpu.CompilerParams(vmem_limit_bytes=32 << 20),
        cost_estimate=pl.CostEstimate(
            flops=2 * feats * width * tokens, bytes_accessed=2 * width * tokens, transcendentals=0
        ),
    )(chips, *got, own)


def turn_kernel(chips, w, wide, tall, turned):
    step = pl.program_id(0)
    size = w.shape[1]

    @pl.when(step < 8)
    def _():
        turned[pl.ds(pl.multiple_of(step * size, size), size)] = w[...].T

    @pl.when(step >= 8)
    def _():
        pieces = []
        for g, group in enumerate(GROUPS):
            for s, count, first in group:
                at = pl.multiple_of(chips[64 * g + 8 * (step - 8) + s] * 64 + first, 16)
                pieces.append(turned[pl.ds(at, count)])
        rows = jnp.concatenate(pieces, axis=0)
        tall[...] = rows
        wide[...] = rows.T


def turned_weights(chips, w):
    vocab_rows, width = w.shape
    size = width // 8
    late = lambda i: jnp.maximum(i - 8, 0)
    return pl.pallas_call(
        turn_kernel,
        grid_spec=pltpu.PrefetchScalarGridSpec(
            num_scalar_prefetch=1,
            grid=(16,),
            in_specs=[pl.BlockSpec((vocab_rows, size), lambda i, t: (0, jnp.minimum(i, 7)))],
            out_specs=[
                pl.BlockSpec((vocab_rows, size), lambda i, t: (0, late(i))),
                pl.BlockSpec((size, vocab_rows), lambda i, t: (late(i), 0)),
            ],
            scratch_shapes=[pltpu.VMEM((width, vocab_rows), BF16)],
        ),
        out_shape=[pltpu.HBM((vocab_rows, width), BF16), pltpu.HBM((width, vocab_rows), BF16)],
        compiler_params=pltpu.CompilerParams(
            dimension_semantics=("arbitrary",), vmem_limit_bytes=32 << 20
        ),
        cost_estimate=pl.CostEstimate(
            flops=2048 * vocab_rows * width, bytes_accessed=6 * vocab_rows * width, transcendentals=0
        ),
    )(chips, w)


def half_copies(got, h):
    size = sum(SIZES)
    for g in range(3):
        for l in range(4):
            src = got[2 * g + l // 2].at[pl.ds((l % 2) * SIZES[g], SIZES[g])]
            yield src, h.at[pl.ds(l * size + STARTS[g], SIZES[g])]


def early_kernel(*refs):
    got, (w, part, h, sem) = refs[:6], refs[6:]

    @pl.when(pl.program_id(0) == 0)
    def _():
        for src, dst in half_copies(got, h):
            pltpu.make_async_copy(src, dst, sem).start()
        pltpu.make_async_copy(h, h, sem).wait()

    part[...] = jnp.dot(w[...], h[...], preferred_element_type=F32)


def late_kernel(*refs):
    got, (w, part, tgt, logits, stats, h, top, total, hit, sem) = refs[:6], refs[6:]
    step = pl.program_id(0)
    rows, tokens = logits.shape

    @pl.when(step == 0)
    def _():
        for src, dst in half_copies(got, h):
            pltpu.make_async_copy(src, dst, sem).start()
        top[...] = jnp.full(top.shape, -jnp.inf, F32)
        total[...] = jnp.zeros(total.shape, F32)
        hit[...] = jnp.zeros(hit.shape, F32)
        pltpu.make_async_copy(h, h, sem).wait()

    block = part[...] + jnp.dot(w[...], h[...], preferred_element_type=F32)
    logits[...] = block
    at = lax.broadcasted_iota(jnp.int32, block.shape, 0) + step * rows
    hit[...] += jnp.sum(jnp.where(at == tgt[...], block, F32(0.0)), axis=0, keepdims=True)
    now = jnp.maximum(top[...], jnp.max(block, axis=0, keepdims=True))
    added = jnp.sum(jnp.exp(block - now), axis=0, keepdims=True)
    total[...] = total[...] * jnp.exp(top[...] - now) + added
    top[...] = now

    @pl.when(step == pl.num_programs(0) - 1)
    def _():
        lse = top[...] + jnp.log(total[...])
        both = [r[:, k : k + 128] for r in (lse, hit[...]) for k in range(0, tokens, 128)]
        stats[...] = jnp.broadcast_to(jnp.concatenate(both, axis=0)[None], stats.shape)


LOGIT_ROWS = 256


def half_logits(half, got, wide, part=None, tgt=None):
    vocab_rows, width = wide.shape
    tokens = got[0].shape[1]
    rows, lines = LOGIT_ROWS, 2 * tokens // 128
    block = pl.BlockSpec((rows, tokens), lambda i: (i, 0))
    row = pl.BlockSpec((1, tokens), lambda i: (0, 0))
    late = part is not None
    return pl.pallas_call(
        late_kernel if late else early_kernel,
        grid=(vocab_rows // rows,),
        in_specs=[pl.BlockSpec(memory_space=pl.ANY)] * len(got)
        + [pl.BlockSpec((rows, width // 2), lambda i: (i, half))]
        + ([block, row] if late else []),
        out_specs=[block, pl.BlockSpec((64, lines, 128), lambda i: (0, 0, 0))] if late else block,
        out_shape=[
            pltpu.HBM((vocab_rows, tokens), F32), jax.ShapeDtypeStruct((64, lines, 128), F32),
        ] if late else pltpu.HBM((vocab_rows, tokens), F32),
        scratch_shapes=[pltpu.VMEM((width // 2, tokens), BF16)]
        + [pltpu.VMEM((1, tokens), F32)] * (3 if late else 0)
        + [pltpu.SemaphoreType.DMA],
        compiler_params=pltpu.CompilerParams(
            dimension_semantics=("arbitrary",), vmem_limit_bytes=32 << 20
        ),
        cost_estimate=pl.CostEstimate(
            flops=vocab_rows * width * tokens,
            bytes_accessed=width * (vocab_rows + tokens) + 4 * vocab_rows * tokens,
            transcendentals=vocab_rows * tokens,
        ),
    )(*got, wide, *([part, tgt] if late else []))


def signal_kernel(stats, logits, cot, tgt, grad, loss, row):
    step = pl.program_id(0)
    rows, tokens = logits.shape
    lines = tokens // 128

    @pl.when(step == 0)
    def _():
        lse = stats[:, :lines]
        top = jnp.max(lse, axis=0)
        full = top + jnp.log(jnp.sum(jnp.exp(lse - top[None]), axis=0))
        tok = full - jnp.sum(stats[:, lines:], axis=0)
        row[...] = jnp.concatenate([full[k : k + 1] for k in range(lines)], axis=1)
        loss[...] = jnp.concatenate([tok[k : k + 1] for k in range(lines)], axis=1)

    block = logits[...]
    at = lax.broadcasted_iota(jnp.int32, block.shape, 0) + step * rows
    one = jnp.where(at == tgt[...], F32(1.0), F32(0.0))
    grad[...] = (cot[...] * (jnp.exp(block - row[...]) - one)).astype(BF16)


def signal_of(stats, logits, cot, tgt):
    vocab_rows, tokens = logits.shape
    rows = 128
    whole = lambda *shape: pl.BlockSpec(shape, lambda i: (0,) * len(shape))
    return pl.pallas_call(
        signal_kernel,
        grid=(vocab_rows // rows,),
        in_specs=[
            whole(*stats.shape),
            pl.BlockSpec((rows, tokens), lambda i: (i, 0)),
            whole(1, tokens),
            whole(1, tokens),
        ],
        out_specs=[pl.BlockSpec((rows, tokens), lambda i: (i, 0)), whole(1, tokens)],
        out_shape=[
            jax.ShapeDtypeStruct((vocab_rows, tokens), BF16),
            jax.ShapeDtypeStruct((1, tokens), F32),
        ],
        scratch_shapes=[pltpu.VMEM((1, tokens), F32)],
        compiler_params=pltpu.CompilerParams(
            dimension_semantics=("arbitrary",), vmem_limit_bytes=16 << 20
        ),
        cost_estimate=pl.CostEstimate(
            flops=8 * vocab_rows * tokens, bytes_accessed=6 * vocab_rows * tokens,
            transcendentals=vocab_rows * tokens,
        ),
    )(stats, logits, cot, tgt)


def grad_kernel(tall, grad, *outs):
    block = jnp.dot(tall[...], grad[...], preferred_element_type=F32).astype(BF16)
    for start, size, out in zip(STARTS, SIZES, outs):
        out[...] = block[start : start + size]


def half_grads(half, tall, grad):
    vocab_rows, tokens = grad.shape
    width = tall.shape[0]
    return pl.pallas_call(
        grad_kernel,
        grid=(4,),
        in_specs=[
            pl.BlockSpec((width // 8, vocab_rows), lambda i: (4 * half + i, 0)),
            pl.BlockSpec((vocab_rows, tokens), lambda i: (0, 0)),
        ],
        out_specs=[pl.BlockSpec((None, size, tokens), lambda i: (i, 0, 0)) for size in SIZES],
        out_shape=[pltpu.HBM((4, size, tokens), BF16) for size in SIZES],
        compiler_params=pltpu.CompilerParams(
            dimension_semantics=("arbitrary",), vmem_limit_bytes=32 << 20
        ),
        cost_estimate=pl.CostEstimate(
            flops=vocab_rows * width * tokens, bytes_accessed=width * (vocab_rows + tokens),
            transcendentals=0,
        ),
    )(tall, grad)


def body(hidden, head_weight, targets, loss_cot):
    vocab_rows, _ = head_weight.shape
    own = hidden.T
    feats, tokens = own.shape
    core = lax.axis_index("dp")
    chips = lax.dynamic_index_in_dim(jnp.asarray(CHIPS), lax.axis_index(ALL), 0, keepdims=False)
    tgt = (targets - lax.axis_index(VOCAB) * vocab_rows)[None, :]
    some = small_stage(jnp.broadcast_to(own[None], (8, feats, tokens)))
    wide, tall = turned_weights(chips, head_weight)
    got = gathered_groups(some.reshape(8 * feats, tokens))
    part = half_logits(0, [a for group in got for a in group[:2]], wide)
    logits, stats = half_logits(1, [a for group in got for a in group[2:]], wide, part, tgt)
    stats = lax.all_to_all(stats, VOCAB, 0, 0, tiled=True)
    a_part = a_part_of(chips, [a for group in got for a in group], own)
    grad, tok_loss = signal_of(stats, logits, loss_cot[None, :], tgt)
    sums = summed_groups(half_grads(1, tall, grad), half_grads(0, tall, grad))
    sums = small_stage(sums.reshape(8, feats, tokens))
    hidden_grad = jnp.sum(sums.astype(F32), axis=0).astype(BF16).T
    rows = vocab_rows // 2

    def gram(x):
        mine = lax.dynamic_slice_in_dim(x, core * rows, rows, 0)
        return lax.dot_general(mine, x, (((1,), (1,)), ((), ())), preferred_element_type=F32)

    g_factor = (gram(grad) + gram(lax.ppermute(grad, "dp", SWAP))) / TOK_DEV
    a_factor = (a_part + lax.ppermute(a_part, "dp", SWAP)) / TOK_DEV
    return (tok_loss[0], hidden_grad, g_factor, a_factor)


def solution(mesh):
    finer = Mesh(mesh.devices.reshape(4, 4, 4, mesh.shape["dp"]), ALL)
    return jax.shard_map(
        body,
        mesh=finer,
        in_specs=(P("dp", VOCAB), P(VOCAB, None), P("dp"), P("dp")),
        out_specs=(P("dp"), P("dp", VOCAB), P(ALL, None), P(VOCAB, None)),
        check_vma=False,
    )
```

```python
import jax
import jax.numpy as jnp
import numpy as np
from jax import lax
from jax.experimental import pallas as pl
from jax.experimental.pallas import tpu as pltpu
from jax.sharding import Mesh
from jax.sharding import PartitionSpec as P

TOK_DEV = 1024
VOCAB = ("vocab_0", "vocab_1", "vocab_2")
ALL = ("vocab_0", "vocab_1", "vocab_2", "dp")
ALL_VMEM = (64 << 20) - (256 << 10)

SMALL = (((0, 1), (2, 3)), ((0, 3), (1, 2)))
LARGE = (((1, 2), (0, 3)), ((0, 1), (3, 2)))
SWAP = [(0, 1), (1, 0)]
F32 = jnp.float32
BF16 = jnp.bfloat16

GROUPS = (
    ((0, 64, 0), (1, 64, 0), (2, 48, 0)),
    ((2, 16, 48), (3, 64, 0), (4, 64, 0), (5, 32, 0)),
    ((5, 32, 32), (6, 64, 0), (7, 64, 0)),
)
SIZES = [sum(rows for _, rows, _ in group) for group in GROUPS]
STARTS = [0, SIZES[0], SIZES[0] + SIZES[1]]


def device(y, z, x, core):
    return ((y * 4 + z) * 4 + x) * 2 + core


def small_cubes():
    return [
        [device(y, z, x, core) for y in a for z in b for x in c]
        for core in (0, 1) for a in SMALL[core] for b in SMALL[core] for c in SMALL[core]
    ]


def partner(core, c):
    return next(p[1 - p.index(c)] for p in LARGE[core] if c in p)


def spots():
    return [(y, z, x, core) for y in range(4) for z in range(4) for x in range(4) for core in (0, 1)]


def large_pairs(axis):
    out = []
    for at in spots():
        to = list(at)
        to[axis] = partner(at[3], at[axis])
        out.append((device(*at), device(*to)))
    return out


def chip_table():
    table = np.zeros((128, 3, 8, 8), np.int32)
    for at in spots():
        core = at[3]
        for group in range(3):
            for l in range(8):
                for s in range(8):
                    chip = 0
                    for axis in range(3):
                        c = at[axis]
                        if l >> ((axis - group) % 3) & 1:
                            c = partner(core, c)
                        pair = next(p for p in SMALL[core] if c in p)
                        chip = chip * 4 + pair[s >> (2 - axis) & 1]
                    table[device(*at), group, l, s] = chip
    return table.reshape(128, 192)


SMALL_CUBES = small_cubes()
LARGE_PAIRS = [large_pairs(axis) for axis in range(3)]
CHIPS = chip_table()


def small_stage(x):
    return lax.all_to_all(x, ALL, 0, 0, axis_index_groups=SMALL_CUBES, tiled=True)


def in_hbm(x):
    return pltpu.with_memory_space_constraint(x, pltpu.HBM)


def gathered_groups(some):
    def get(x, g, step):
        return lax.ppermute(x, ALL, LARGE_PAIRS[(g + step) % 3])

    held = [some[start : start + size] for start, size in zip(STARTS, SIZES)]
    got = [get(held[g], g, 0) for g in range(3)]
    first = [jnp.concatenate([h, r]) for h, r in zip(held, got)]
    second = [get(first[g], g, 1) for g in range(3)]
    third = [get(first[g], g, 2) for g in range(3)]
    fourth = [get(second[g], g, 2) for g in range(3)]
    return [[first[g], second[g], third[g], fourth[g]] for g in range(3)]


def add_kernel(*refs):
    *terms, out = refs
    total = terms[0][...].astype(F32)
    for term in terms[1:]:
        total = total + term[...].astype(F32)
    out[...] = total.astype(BF16)


def add_up(count, *terms):
    _, rows, tokens = terms[0][0].shape
    block = lambda first: pl.BlockSpec((None, rows, tokens), lambda i: (first + i, 0, 0))
    return pl.pallas_call(
        add_kernel,
        grid=(count,),
        in_specs=[block(first) for _, first in terms],
        out_specs=block(0),
        out_shape=jax.ShapeDtypeStruct((count, rows, tokens), BF16),
        compiler_params=pltpu.CompilerParams(
            dimension_semantics=("arbitrary",), vmem_limit_bytes=ALL_VMEM
        ),
        cost_estimate=pl.CostEstimate(
            flops=len(terms) * count * rows * tokens,
            bytes_accessed=2 * (len(terms) + 1) * count * rows * tokens, transcendentals=0,
        ),
    )(*[in_hbm(x) for x, _ in terms])


def summed_groups(sends, keeps):
    trade = lambda x, g, step: lax.ppermute(x, ALL, LARGE_PAIRS[(g + step) % 3])
    far = [trade(sends[g], g, 2) for g in range(3)]
    mid = [trade(add_up(2, (keeps[g], 2), (far[g], 2)), g, 1) for g in range(3)]
    near = [
        trade(add_up(1, (keeps[g], 1), (far[g], 1), (mid[g], 1)), g, 0) for g in range(3)
    ]
    return jnp.concatenate(
        [add_up(1, (keeps[g], 0), (far[g], 0), (mid[g], 0), (near[g], 0))[0] for g in range(3)]
    )


def sum_kernel(pieces, out):
    out[...] = jnp.sum(pieces[...].astype(F32), axis=0).astype(BF16)


def summed(pieces):
    count, rows, tokens = pieces.shape
    return pl.pallas_call(
        sum_kernel,
        grid=(2,),
        in_specs=[pl.BlockSpec((count, rows, tokens // 2), lambda i: (0, 0, i))],
        out_specs=pl.BlockSpec((rows, tokens // 2), lambda i: (0, i)),
        out_shape=jax.ShapeDtypeStruct((rows, tokens), BF16),
        compiler_params=pltpu.CompilerParams(
            dimension_semantics=("arbitrary",), vmem_limit_bytes=8 << 20
        ),
    )(pieces)


def gather_copies(chips, got, h):
    quarters = []
    for large in (0, 1):
        for small in (0, 1):
            copies = []
            for g, group in enumerate(GROUPS):
                for l in range(8):
                    if l >> (-g % 3) & 1 != large:
                        continue
                    src, at = got[4 * g + l // 2], (l % 2) * SIZES[g]
                    for s, count, first in group:
                        if s >> 2 == small:
                            dst = pl.multiple_of(chips[64 * g + 8 * l + s] * 64 + first, 16)
                            copies.append((src.at[pl.ds(at, count)], h.at[pl.ds(dst, count)]))
                        at += count
            quarters.append((chips[8 * large + 4 * small] // 16, copies))
    return quarters


def a_kernel(chips, *refs):
    got, (own, out, h, sem) = refs[:12], refs[12:]
    for _, copies in gather_copies(chips, got, h):
        for src, dst in copies:
            pltpu.make_async_copy(src, dst, sem).start()
    pltpu.make_async_copy(h, h, sem).wait()
    out[...] = lax.dot_general(
        own[...], h[...], (((1,), (1,)), ((), ())), preferred_element_type=F32
    )


def a_part_of(chips, got, own):
    feats, tokens = own.shape
    width = 64 * feats
    return pl.pallas_call(
        a_kernel,
        grid_spec=pltpu.PrefetchScalarGridSpec(
            num_scalar_prefetch=1,
            grid=(),
            in_specs=[pl.BlockSpec(memory_space=pltpu.HBM)] * len(got)
            + [pl.BlockSpec(memory_space=pltpu.VMEM)],
            out_specs=pl.BlockSpec(memory_space=pltpu.VMEM),
            scratch_shapes=[pltpu.VMEM((width, tokens), BF16), pltpu.SemaphoreType.DMA],
        ),
        out_shape=jax.ShapeDtypeStruct((feats, width), F32),
        compiler_params=pltpu.CompilerParams(vmem_limit_bytes=ALL_VMEM),
        cost_estimate=pl.CostEstimate(
            flops=2 * feats * width * tokens, bytes_accessed=2 * width * tokens, transcendentals=0
        ),
    )(chips, *[in_hbm(x) for x in got], own)


def turn_kernel(chips, w, wide, tall, turned):
    step = pl.program_id(0)
    size = w.shape[1]

    @pl.when(step < 8)
    def _():
        turned[pl.ds(pl.multiple_of(step * size, size), size)] = w[...].T

    @pl.when(step >= 8)
    def _():
        pieces = []
        for g, group in enumerate(GROUPS):
            for s, count, first in group:
                at = pl.multiple_of(chips[64 * g + 8 * (step - 8) + s] * 64 + first, 16)
                pieces.append(turned[pl.ds(at, count)])
        rows = jnp.concatenate(pieces, axis=0)
        tall[...] = rows
        wide[...] = rows.T


def turned_weights(chips, w):
    vocab_rows, width = w.shape
    size = width // 8
    late = lambda i: jnp.maximum(i - 8, 0)
    return pl.pallas_call(
        turn_kernel,
        grid_spec=pltpu.PrefetchScalarGridSpec(
            num_scalar_prefetch=1,
            grid=(16,),
            in_specs=[pl.BlockSpec((vocab_rows, size), lambda i, t: (0, jnp.minimum(i, 7)))],
            out_specs=[
                pl.BlockSpec((vocab_rows, size), lambda i, t: (0, late(i))),
                pl.BlockSpec((size, vocab_rows), lambda i, t: (late(i), 0)),
            ],
            scratch_shapes=[pltpu.VMEM((width, vocab_rows), BF16)],
        ),
        out_shape=[pltpu.HBM((vocab_rows, width), BF16), pltpu.HBM((width, vocab_rows), BF16)],
        compiler_params=pltpu.CompilerParams(
            dimension_semantics=("arbitrary",), vmem_limit_bytes=32 << 20
        ),
        cost_estimate=pl.CostEstimate(
            flops=2048 * vocab_rows * width, bytes_accessed=6 * vocab_rows * width, transcendentals=0
        ),
    )(chips, in_hbm(w))


def half_copies(got, h):
    size = sum(SIZES)
    for g in range(3):
        for l in range(4):
            src = got[2 * g + l // 2].at[pl.ds((l % 2) * SIZES[g], SIZES[g])]
            yield src, h.at[pl.ds(l * size + STARTS[g], SIZES[g])]


def early_kernel(*refs):
    got, (w, part, h, sem) = refs[:6], refs[6:]

    @pl.when(pl.program_id(0) == 0)
    def _():
        for src, dst in half_copies(got, h):
            pltpu.make_async_copy(src, dst, sem).start()
        pltpu.make_async_copy(h, h, sem).wait()

    part[...] = jnp.dot(w[...], h[...], preferred_element_type=F32)


def late_kernel(*refs):
    got, (w, part, tgt, logits, stats, h, top, total, hit, sem) = refs[:6], refs[6:]
    step = pl.program_id(0)
    rows, tokens = logits.shape

    @pl.when(step == 0)
    def _():
        for src, dst in half_copies(got, h):
            pltpu.make_async_copy(src, dst, sem).start()
        top[...] = jnp.full(top.shape, -jnp.inf, F32)
        total[...] = jnp.zeros(total.shape, F32)
        hit[...] = jnp.zeros(hit.shape, F32)
        pltpu.make_async_copy(h, h, sem).wait()

    block = part[...] + jnp.dot(w[...], h[...], preferred_element_type=F32)
    logits[...] = block
    at = lax.broadcasted_iota(jnp.int32, block.shape, 0) + step * rows
    hit[...] += jnp.sum(jnp.where(at == tgt[...], block, F32(0.0)), axis=0, keepdims=True)
    now = jnp.maximum(top[...], jnp.max(block, axis=0, keepdims=True))
    added = jnp.sum(jnp.exp(block - now), axis=0, keepdims=True)
    total[...] = total[...] * jnp.exp(top[...] - now) + added
    top[...] = now

    @pl.when(step == pl.num_programs(0) - 1)
    def _():
        lse = top[...] + jnp.log(total[...])
        both = [r[:, k : k + 128] for r in (lse, hit[...]) for k in range(0, tokens, 128)]
        stats[...] = jnp.broadcast_to(jnp.concatenate(both, axis=0)[None], stats.shape)


LOGIT_ROWS = 256


def half_logits(half, got, wide, part=None, tgt=None):
    vocab_rows, width = wide.shape
    tokens = got[0].shape[1]
    rows, lines = LOGIT_ROWS, 2 * tokens // 128
    block = pl.BlockSpec((rows, tokens), lambda i: (i, 0))
    row = pl.BlockSpec((1, tokens), lambda i: (0, 0))
    late = part is not None
    return pl.pallas_call(
        late_kernel if late else early_kernel,
        grid=(vocab_rows // rows,),
        in_specs=[pl.BlockSpec(memory_space=pl.ANY)] * len(got)
        + [pl.BlockSpec((rows, width // 2), lambda i: (i, half))]
        + ([block, row] if late else []),
        out_specs=[block, pl.BlockSpec((64, lines, 128), lambda i: (0, 0, 0))] if late else block,
        out_shape=[
            pltpu.HBM((vocab_rows, tokens), F32), jax.ShapeDtypeStruct((64, lines, 128), F32),
        ] if late else pltpu.HBM((vocab_rows, tokens), F32),
        scratch_shapes=[pltpu.VMEM((width // 2, tokens), BF16)]
        + [pltpu.VMEM((1, tokens), F32)] * (3 if late else 0)
        + [pltpu.SemaphoreType.DMA],
        compiler_params=pltpu.CompilerParams(
            dimension_semantics=("arbitrary",), vmem_limit_bytes=ALL_VMEM
        ),
        cost_estimate=pl.CostEstimate(
            flops=vocab_rows * width * tokens,
            bytes_accessed=width * (vocab_rows + tokens) + 4 * vocab_rows * tokens,
            transcendentals=vocab_rows * tokens,
        ),
    )(*got, in_hbm(wide), *([in_hbm(part), tgt] if late else []))


def signal_kernel(stats, logits, cot, tgt, grad, loss, row):
    step = pl.program_id(0)
    rows, tokens = logits.shape
    lines = tokens // 128

    @pl.when(step == 0)
    def _():
        lse = stats[:, :lines]
        top = jnp.max(lse, axis=0)
        full = top + jnp.log(jnp.sum(jnp.exp(lse - top[None]), axis=0))
        tok = full - jnp.sum(stats[:, lines:], axis=0)
        row[...] = jnp.concatenate([full[k : k + 1] for k in range(lines)], axis=1)
        loss[...] = jnp.concatenate([tok[k : k + 1] for k in range(lines)], axis=1)

    block = logits[...]
    at = lax.broadcasted_iota(jnp.int32, block.shape, 0) + step * rows
    one = jnp.where(at == tgt[...], F32(1.0), F32(0.0))
    grad[...] = (cot[...] * (jnp.exp(block - row[...]) - one)).astype(BF16)


def signal_of(stats, logits, cot, tgt):
    vocab_rows, tokens = logits.shape
    rows = 128
    whole = lambda *shape: pl.BlockSpec(shape, lambda i: (0,) * len(shape))
    return pl.pallas_call(
        signal_kernel,
        grid=(vocab_rows // rows,),
        in_specs=[
            whole(*stats.shape),
            pl.BlockSpec((rows, tokens), lambda i: (i, 0)),
            whole(1, tokens),
            whole(1, tokens),
        ],
        out_specs=[pl.BlockSpec((rows, tokens), lambda i: (i, 0)), whole(1, tokens)],
        out_shape=[
            jax.ShapeDtypeStruct((vocab_rows, tokens), BF16),
            jax.ShapeDtypeStruct((1, tokens), F32),
        ],
        scratch_shapes=[pltpu.VMEM((1, tokens), F32)],
        compiler_params=pltpu.CompilerParams(
            dimension_semantics=("arbitrary",), vmem_limit_bytes=16 << 20
        ),
        cost_estimate=pl.CostEstimate(
            flops=8 * vocab_rows * tokens, bytes_accessed=6 * vocab_rows * tokens,
            transcendentals=vocab_rows * tokens,
        ),
    )(stats, in_hbm(logits), cot, tgt)


def grad_kernel(tall, grad, *outs):
    block = jnp.dot(tall[...], grad[...], preferred_element_type=F32).astype(BF16)
    for start, size, out in zip(STARTS, SIZES, outs):
        out[...] = block[start : start + size]


def half_grads(half, tall, grad):
    vocab_rows, tokens = grad.shape
    width = tall.shape[0]
    return pl.pallas_call(
        grad_kernel,
        grid=(4,),
        in_specs=[
            pl.BlockSpec((width // 8, vocab_rows), lambda i: (4 * half + i, 0)),
            pl.BlockSpec((vocab_rows, tokens), lambda i: (0, 0)),
        ],
        out_specs=[pl.BlockSpec((None, size, tokens), lambda i: (i, 0, 0)) for size in SIZES],
        out_shape=[pltpu.HBM((4, size, tokens), BF16) for size in SIZES],
        compiler_params=pltpu.CompilerParams(
            dimension_semantics=("arbitrary",), vmem_limit_bytes=ALL_VMEM
        ),
        cost_estimate=pl.CostEstimate(
            flops=vocab_rows * width * tokens, bytes_accessed=width * (vocab_rows + tokens),
            transcendentals=0,
        ),
    )(in_hbm(tall), grad)


def body(hidden, head_weight, targets, loss_cot):
    vocab_rows, _ = head_weight.shape
    own = hidden.T
    feats, tokens = own.shape
    core = lax.axis_index("dp")
    chips = lax.dynamic_index_in_dim(jnp.asarray(CHIPS), lax.axis_index(ALL), 0, keepdims=False)
    tgt = (targets - lax.axis_index(VOCAB) * vocab_rows)[None, :]
    some = small_stage(jnp.broadcast_to(own[None], (8, feats, tokens)))
    wide, tall = turned_weights(chips, head_weight)
    got = gathered_groups(some.reshape(8 * feats, tokens))
    part = half_logits(0, [a for group in got for a in group[:2]], wide)
    logits, stats = half_logits(1, [a for group in got for a in group[2:]], wide, part, tgt)
    stats = lax.all_to_all(stats, VOCAB, 0, 0, tiled=True)
    a_part = a_part_of(chips, [a for group in got for a in group], own)
    grad, tok_loss = signal_of(stats, logits, loss_cot[None, :], tgt)
    sums = summed_groups(half_grads(1, tall, grad), half_grads(0, tall, grad))
    sums = small_stage(sums.reshape(8, feats, tokens))
    hidden_grad = summed(sums).T
    rows = vocab_rows // 2

    def gram(x):
        mine = lax.dynamic_slice_in_dim(x, core * rows, rows, 0)
        return lax.dot_general(mine, x, (((1,), (1,)), ((), ())), preferred_element_type=F32)

    g_factor = (gram(grad) + gram(lax.ppermute(grad, "dp", SWAP))) / TOK_DEV
    a_factor = (a_part + lax.ppermute(a_part, "dp", SWAP)) / TOK_DEV
    return (tok_loss[0], hidden_grad, g_factor, a_factor)


def solution(mesh):
    finer = Mesh(mesh.devices.reshape(4, 4, 4, mesh.shape["dp"]), ALL)
    return jax.shard_map(
        body,
        mesh=finer,
        in_specs=(P("dp", VOCAB), P(VOCAB, None), P("dp"), P("dp")),
        out_specs=(P("dp"), P("dp", VOCAB), P(ALL, None), P(VOCAB, None)),
        check_vma=False,
    )
```

```python
import jax
import jax.numpy as jnp
import numpy as np
from jax import lax
from jax.experimental import pallas as pl
from jax.experimental.pallas import tpu as pltpu
from jax.sharding import Mesh
from jax.sharding import PartitionSpec as P

TOK_DEV = 1024
VOCAB = ("vocab_0", "vocab_1", "vocab_2")
ALL = ("vocab_0", "vocab_1", "vocab_2", "dp")
ALL_VMEM = (64 << 20) - (256 << 10)

SMALL = (((0, 1), (2, 3)), ((0, 3), (1, 2)))
LARGE = (((1, 2), (0, 3)), ((0, 1), (3, 2)))
SWAP = [(0, 1), (1, 0)]
F32 = jnp.float32
BF16 = jnp.bfloat16

GROUPS = (
    ((0, 64, 0), (1, 64, 0), (2, 48, 0)),
    ((2, 16, 48), (3, 64, 0), (4, 64, 0), (5, 32, 0)),
    ((5, 32, 32), (6, 64, 0), (7, 64, 0)),
)
SIZES = [sum(rows for _, rows, _ in group) for group in GROUPS]
STARTS = [0, SIZES[0], SIZES[0] + SIZES[1]]


def device(y, z, x, core):
    return ((y * 4 + z) * 4 + x) * 2 + core


def small_cubes():
    return [
        [device(y, z, x, core) for y in a for z in b for x in c]
        for core in (0, 1) for a in SMALL[core] for b in SMALL[core] for c in SMALL[core]
    ]


def partner(core, c):
    return next(p[1 - p.index(c)] for p in LARGE[core] if c in p)


def spots():
    return [(y, z, x, core) for y in range(4) for z in range(4) for x in range(4) for core in (0, 1)]


def large_pairs(axis):
    out = []
    for at in spots():
        to = list(at)
        to[axis] = partner(at[3], at[axis])
        out.append((device(*at), device(*to)))
    return out


def chip_table():
    table = np.zeros((128, 3, 8, 8), np.int32)
    for at in spots():
        core = at[3]
        for group in range(3):
            for l in range(8):
                for s in range(8):
                    chip = 0
                    for axis in range(3):
                        c = at[axis]
                        if l >> ((axis - group) % 3) & 1:
                            c = partner(core, c)
                        pair = next(p for p in SMALL[core] if c in p)
                        chip = chip * 4 + pair[s >> (2 - axis) & 1]
                    table[device(*at), group, l, s] = chip
    return table.reshape(128, 192)


SMALL_CUBES = small_cubes()
LARGE_PAIRS = [large_pairs(axis) for axis in range(3)]
CHIPS = chip_table()


def small_stage(x):
    return lax.all_to_all(x, ALL, 0, 0, axis_index_groups=SMALL_CUBES, tiled=True)


def in_hbm(x):
    return pltpu.with_memory_space_constraint(x, pltpu.HBM)


def gathered_groups(some):
    def get(x, g, step):
        return lax.ppermute(x, ALL, LARGE_PAIRS[(g + step) % 3])

    held = [some[start : start + size] for start, size in zip(STARTS, SIZES)]
    got = [get(held[g], g, 0) for g in range(3)]
    first = [jnp.concatenate([h, r]) for h, r in zip(held, got)]
    second = [get(first[g], g, 1) for g in range(3)]
    third = [get(first[g], g, 2) for g in range(3)]
    fourth = [get(second[g], g, 2) for g in range(3)]
    return [[first[g], second[g], third[g], fourth[g]] for g in range(3)]


def add_kernel(*refs):
    *terms, out = refs
    total = terms[0][...].astype(F32)
    for term in terms[1:]:
        total = total + term[...].astype(F32)
    out[...] = total.astype(BF16)


def add_up(count, *terms):
    _, rows, tokens = terms[0][0].shape
    block = lambda first: pl.BlockSpec((None, rows, tokens), lambda i: (first + i, 0, 0))
    return pl.pallas_call(
        add_kernel,
        grid=(count,),
        in_specs=[block(first) for _, first in terms],
        out_specs=block(0),
        out_shape=jax.ShapeDtypeStruct((count, rows, tokens), BF16),
        compiler_params=pltpu.CompilerParams(
            dimension_semantics=("arbitrary",), vmem_limit_bytes=ALL_VMEM
        ),
        cost_estimate=pl.CostEstimate(
            flops=len(terms) * count * rows * tokens,
            bytes_accessed=2 * (len(terms) + 1) * count * rows * tokens, transcendentals=0,
        ),
    )(*[in_hbm(x) for x, _ in terms])


def last_kernel(*refs):
    *terms, out = refs
    for g in range(3):
        total = terms[4 * g][...].astype(F32)
        for term in terms[4 * g + 1 : 4 * g + 4]:
            total = total + term[...].astype(F32)
        out[STARTS[g] : STARTS[g] + SIZES[g]] = total.astype(BF16)


def add_last(terms):
    tokens = terms[0].shape[2]
    part = tokens // 2
    return pl.pallas_call(
        last_kernel,
        grid=(2,),
        in_specs=[
            pl.BlockSpec((None, x.shape[1], part), lambda i: (0, 0, i)) for x in terms
        ],
        out_specs=pl.BlockSpec((sum(SIZES), part), lambda i: (0, i)),
        out_shape=jax.ShapeDtypeStruct((sum(SIZES), tokens), BF16),
        compiler_params=pltpu.CompilerParams(
            dimension_semantics=("arbitrary",), vmem_limit_bytes=ALL_VMEM
        ),
        cost_estimate=pl.CostEstimate(
            flops=4 * sum(SIZES) * tokens, bytes_accessed=10 * sum(SIZES) * tokens, transcendentals=0
        ),
    )(*[in_hbm(x) for x in terms])


def summed_groups(sends, keeps):
    def trade(x, g, step):
        return lax.ppermute(x, ALL, LARGE_PAIRS[(g + step) % 3])

    far = [trade(sends[g], g, 2) for g in range(3)]
    mid = [trade(add_up(2, (keeps[g], 2), (far[g], 2)), g, 1) for g in range(3)]
    near = [
        trade(add_up(1, (keeps[g], 1), (far[g], 1), (mid[g], 1)), g, 0) for g in range(3)
    ]
    return add_last([x for g in range(3) for x in (keeps[g], far[g], mid[g], near[g])])


def sum_kernel(pieces, out):
    out[...] = jnp.sum(pieces[...].astype(F32), axis=0).astype(BF16)


def summed(pieces):
    count, rows, tokens = pieces.shape
    return pl.pallas_call(
        sum_kernel,
        grid=(2,),
        in_specs=[pl.BlockSpec((count, rows, tokens // 2), lambda i: (0, 0, i))],
        out_specs=pl.BlockSpec((rows, tokens // 2), lambda i: (0, i)),
        out_shape=jax.ShapeDtypeStruct((rows, tokens), BF16),
        compiler_params=pltpu.CompilerParams(
            dimension_semantics=("arbitrary",), vmem_limit_bytes=8 << 20
        ),
    )(pieces)


def gather_copies(chips, got, h):
    quarters = []
    for large in (0, 1):
        for small in (0, 1):
            copies = []
            for g, group in enumerate(GROUPS):
                for l in range(8):
                    if l >> (-g % 3) & 1 != large:
                        continue
                    src, at = got[4 * g + l // 2], (l % 2) * SIZES[g]
                    for s, count, first in group:
                        if s >> 2 == small:
                            dst = pl.multiple_of(chips[64 * g + 8 * l + s] * 64 + first, 16)
                            copies.append((src.at[pl.ds(at, count)], h.at[pl.ds(dst, count)]))
                        at += count
            quarters.append((chips[8 * large + 4 * small] // 16, copies))
    return quarters


def a_kernel(chips, *refs):
    got, (own, out, h, sem) = refs[:12], refs[12:]
    for _, copies in gather_copies(chips, got, h):
        for src, dst in copies:
            pltpu.make_async_copy(src, dst, sem).start()
    pltpu.make_async_copy(h, h, sem).wait()
    out[...] = lax.dot_general(
        own[...], h[...], (((1,), (1,)), ((), ())), preferred_element_type=F32
    )


def a_part_of(chips, got, own):
    feats, tokens = own.shape
    width = 64 * feats
    return pl.pallas_call(
        a_kernel,
        grid_spec=pltpu.PrefetchScalarGridSpec(
            num_scalar_prefetch=1,
            grid=(),
            in_specs=[pl.BlockSpec(memory_space=pltpu.HBM)] * len(got)
            + [pl.BlockSpec(memory_space=pltpu.VMEM)],
            out_specs=pl.BlockSpec(memory_space=pltpu.VMEM),
            scratch_shapes=[pltpu.VMEM((width, tokens), BF16), pltpu.SemaphoreType.DMA],
        ),
        out_shape=jax.ShapeDtypeStruct((feats, width), F32),
        compiler_params=pltpu.CompilerParams(vmem_limit_bytes=ALL_VMEM),
        cost_estimate=pl.CostEstimate(
            flops=2 * feats * width * tokens, bytes_accessed=2 * width * tokens, transcendentals=0
        ),
    )(chips, *[in_hbm(x) for x in got], own)


def turn_kernel(chips, w, wide, tall, turned):
    step = pl.program_id(0)
    size = w.shape[1]

    @pl.when(step < 8)
    def _():
        turned[pl.ds(pl.multiple_of(step * size, size), size)] = w[...].T

    @pl.when(step >= 8)
    def _():
        pieces = []
        for g, group in enumerate(GROUPS):
            for s, count, first in group:
                at = pl.multiple_of(chips[64 * g + 8 * (step - 8) + s] * 64 + first, 16)
                pieces.append(turned[pl.ds(at, count)])
        rows = jnp.concatenate(pieces, axis=0)
        tall[...] = rows
        wide[...] = rows.T


def turned_weights(chips, w):
    vocab_rows, width = w.shape
    size = width // 8
    late = lambda i: jnp.maximum(i - 8, 0)
    return pl.pallas_call(
        turn_kernel,
        grid_spec=pltpu.PrefetchScalarGridSpec(
            num_scalar_prefetch=1,
            grid=(16,),
            in_specs=[pl.BlockSpec((vocab_rows, size), lambda i, t: (0, jnp.minimum(i, 7)))],
            out_specs=[
                pl.BlockSpec((vocab_rows, size), lambda i, t: (0, late(i))),
                pl.BlockSpec((size, vocab_rows), lambda i, t: (late(i), 0)),
            ],
            scratch_shapes=[pltpu.VMEM((width, vocab_rows), BF16)],
        ),
        out_shape=[pltpu.HBM((vocab_rows, width), BF16), pltpu.HBM((width, vocab_rows), BF16)],
        compiler_params=pltpu.CompilerParams(
            dimension_semantics=("arbitrary",), vmem_limit_bytes=32 << 20
        ),
        cost_estimate=pl.CostEstimate(
            flops=2048 * vocab_rows * width, bytes_accessed=6 * vocab_rows * width, transcendentals=0
        ),
    )(chips, in_hbm(w))


def half_copies(got, h):
    size = sum(SIZES)
    for g in range(3):
        for l in range(4):
            src = got[2 * g + l // 2].at[pl.ds((l % 2) * SIZES[g], SIZES[g])]
            yield src, h.at[pl.ds(l * size + STARTS[g], SIZES[g])]


def early_kernel(*refs):
    got, (w, part, h, sem) = refs[:6], refs[6:]

    @pl.when(pl.program_id(0) == 0)
    def _():
        for src, dst in half_copies(got, h):
            pltpu.make_async_copy(src, dst, sem).start()
        pltpu.make_async_copy(h, h, sem).wait()

    part[...] = jnp.dot(w[...], h[...], preferred_element_type=F32)


def late_kernel(*refs):
    got, (w, part, tgt, logits, stats, h, top, total, hit, sem) = refs[:6], refs[6:]
    step = pl.program_id(0)
    rows, tokens = logits.shape

    @pl.when(step == 0)
    def _():
        for src, dst in half_copies(got, h):
            pltpu.make_async_copy(src, dst, sem).start()
        top[...] = jnp.full(top.shape, -jnp.inf, F32)
        total[...] = jnp.zeros(total.shape, F32)
        hit[...] = jnp.zeros(hit.shape, F32)
        pltpu.make_async_copy(h, h, sem).wait()

    block = part[...] + jnp.dot(w[...], h[...], preferred_element_type=F32)
    logits[...] = block
    at = lax.broadcasted_iota(jnp.int32, block.shape, 0) + step * rows
    hit[...] += jnp.sum(jnp.where(at == tgt[...], block, F32(0.0)), axis=0, keepdims=True)
    now = jnp.maximum(top[...], jnp.max(block, axis=0, keepdims=True))
    added = jnp.sum(jnp.exp(block - now), axis=0, keepdims=True)
    total[...] = total[...] * jnp.exp(top[...] - now) + added
    top[...] = now

    @pl.when(step == pl.num_programs(0) - 1)
    def _():
        lse = top[...] + jnp.log(total[...])
        both = [r[:, k : k + 128] for r in (lse, hit[...]) for k in range(0, tokens, 128)]
        stats[...] = jnp.broadcast_to(jnp.concatenate(both, axis=0)[None], stats.shape)


LOGIT_ROWS = 256


def half_logits(half, got, wide, part=None, tgt=None):
    vocab_rows, width = wide.shape
    tokens = got[0].shape[1]
    rows, lines = LOGIT_ROWS, 2 * tokens // 128
    block = pl.BlockSpec((rows, tokens), lambda i: (i, 0))
    row = pl.BlockSpec((1, tokens), lambda i: (0, 0))
    late = part is not None
    return pl.pallas_call(
        late_kernel if late else early_kernel,
        grid=(vocab_rows // rows,),
        in_specs=[pl.BlockSpec(memory_space=pl.ANY)] * len(got)
        + [pl.BlockSpec((rows, width // 2), lambda i: (i, half))]
        + ([block, row] if late else []),
        out_specs=[block, pl.BlockSpec((64, lines, 128), lambda i: (0, 0, 0))] if late else block,
        out_shape=[
            pltpu.HBM((vocab_rows, tokens), F32), jax.ShapeDtypeStruct((64, lines, 128), F32),
        ] if late else pltpu.HBM((vocab_rows, tokens), F32),
        scratch_shapes=[pltpu.VMEM((width // 2, tokens), BF16)]
        + [pltpu.VMEM((1, tokens), F32)] * (3 if late else 0)
        + [pltpu.SemaphoreType.DMA],
        compiler_params=pltpu.CompilerParams(
            dimension_semantics=("arbitrary",), vmem_limit_bytes=ALL_VMEM
        ),
        cost_estimate=pl.CostEstimate(
            flops=vocab_rows * width * tokens,
            bytes_accessed=width * (vocab_rows + tokens) + 4 * vocab_rows * tokens,
            transcendentals=vocab_rows * tokens,
        ),
    )(*got, in_hbm(wide), *([in_hbm(part), tgt] if late else []))


def signal_kernel(stats, logits, cot, tgt, tall, grad, loss, *refs):
    outs, (row, whole) = refs[:3], refs[3:]
    step = pl.program_id(0)
    rows, tokens = logits.shape
    lines = tokens // 128
    count = whole.shape[0] // rows

    @pl.when(step == 0)
    def _():
        lse = stats[:, :lines]
        top = jnp.max(lse, axis=0)
        full = top + jnp.log(jnp.sum(jnp.exp(lse - top[None]), axis=0))
        tok = full - jnp.sum(stats[:, lines:], axis=0)
        row[...] = jnp.concatenate([full[k : k + 1] for k in range(lines)], axis=1)
        loss[...] = jnp.concatenate([tok[k : k + 1] for k in range(lines)], axis=1)

    @pl.when(step < count)
    def _():
        block = logits[...]
        at = lax.broadcasted_iota(jnp.int32, block.shape, 0) + step * rows
        one = jnp.where(at == tgt[...], F32(1.0), F32(0.0))
        done = (cot[...] * (jnp.exp(block - row[...]) - one)).astype(BF16)
        grad[...] = done
        whole[pl.ds(pl.multiple_of(step * rows, rows), rows)] = done

    @pl.when(step >= count)
    def _():
        block = jnp.dot(tall[...], whole[...], preferred_element_type=F32).astype(BF16)
        for start, size, out in zip(STARTS, SIZES, outs):
            out[...] = block[start : start + size]


def signal_of(stats, logits, cot, tgt, tall):
    vocab_rows, tokens = logits.shape
    width = tall.shape[0]
    rows = 256
    count = vocab_rows // rows
    early = lambda i: jnp.minimum(i, count - 1)
    late = lambda i: jnp.maximum(i - count, 0)
    whole = lambda *shape: pl.BlockSpec(shape, lambda i: (0,) * len(shape))
    grad, loss, *sums = pl.pallas_call(
        signal_kernel,
        grid=(count + 4,),
        in_specs=[
            whole(*stats.shape),
            pl.BlockSpec((rows, tokens), lambda i: (early(i), 0)),
            whole(1, tokens),
            whole(1, tokens),
            pl.BlockSpec((width // 8, vocab_rows), lambda i: (4 + late(i), 0)),
        ],
        out_specs=[pl.BlockSpec((rows, tokens), lambda i: (early(i), 0)), whole(1, tokens)]
        + [pl.BlockSpec((None, size, tokens), lambda i: (late(i), 0, 0)) for size in SIZES],
        out_shape=[
            pltpu.HBM((vocab_rows, tokens), BF16),
            jax.ShapeDtypeStruct((1, tokens), F32),
        ] + [pltpu.HBM((4, size, tokens), BF16) for size in SIZES],
        scratch_shapes=[pltpu.VMEM((1, tokens), F32), pltpu.VMEM((vocab_rows, tokens), BF16)],
        compiler_params=pltpu.CompilerParams(
            dimension_semantics=("arbitrary",), vmem_limit_bytes=ALL_VMEM
        ),
        cost_estimate=pl.CostEstimate(
            flops=vocab_rows * width * tokens,
            bytes_accessed=6 * vocab_rows * tokens + width * (vocab_rows + tokens),
            transcendentals=vocab_rows * tokens,
        ),
    )(stats, in_hbm(logits), cot, tgt, in_hbm(tall))
    return grad, loss, sums


def grad_kernel(tall, grad, *outs):
    block = jnp.dot(tall[...], grad[...], preferred_element_type=F32).astype(BF16)
    for start, size, out in zip(STARTS, SIZES, outs):
        out[...] = block[start : start + size]


def half_grads(half, tall, grad):
    vocab_rows, tokens = grad.shape
    width = tall.shape[0]
    return pl.pallas_call(
        grad_kernel,
        grid=(4,),
        in_specs=[
            pl.BlockSpec((width // 8, vocab_rows), lambda i: (4 * half + i, 0)),
            pl.BlockSpec((vocab_rows, tokens), lambda i: (0, 0)),
        ],
        out_specs=[pl.BlockSpec((None, size, tokens), lambda i: (i, 0, 0)) for size in SIZES],
        out_shape=[pltpu.HBM((4, size, tokens), BF16) for size in SIZES],
        compiler_params=pltpu.CompilerParams(
            dimension_semantics=("arbitrary",), vmem_limit_bytes=ALL_VMEM
        ),
        cost_estimate=pl.CostEstimate(
            flops=vocab_rows * width * tokens, bytes_accessed=width * (vocab_rows + tokens),
            transcendentals=0,
        ),
    )(in_hbm(tall), grad)


def body(hidden, head_weight, targets, loss_cot):
    vocab_rows, _ = head_weight.shape
    own = hidden.T
    feats, tokens = own.shape
    core = lax.axis_index("dp")
    chips = lax.dynamic_index_in_dim(jnp.asarray(CHIPS), lax.axis_index(ALL), 0, keepdims=False)
    tgt = (targets - lax.axis_index(VOCAB) * vocab_rows)[None, :]
    some = small_stage(jnp.broadcast_to(own[None], (8, feats, tokens)))
    wide, tall = turned_weights(chips, head_weight)
    got = gathered_groups(some.reshape(8 * feats, tokens))
    part = half_logits(0, [a for group in got for a in group[:2]], wide)
    logits, stats = half_logits(1, [a for group in got for a in group[2:]], wide, part, tgt)
    stats = lax.all_to_all(stats, VOCAB, 0, 0, tiled=True)
    a_part = a_part_of(chips, [a for group in got for a in group], own)
    grad, tok_loss, sends = signal_of(stats, logits, loss_cot[None, :], tgt, tall)
    sums = summed_groups(sends, half_grads(0, tall, grad))
    sums = small_stage(sums.reshape(8, feats, tokens))
    hidden_grad = summed(sums).T
    rows = vocab_rows // 2

    def gram(x):
        mine = lax.dynamic_slice_in_dim(x, core * rows, rows, 0)
        return lax.dot_general(mine, x, (((1,), (1,)), ((), ())), preferred_element_type=F32)

    g_factor = (gram(grad) + gram(lax.ppermute(grad, "dp", SWAP))) / TOK_DEV
    a_factor = (a_part + lax.ppermute(a_part, "dp", SWAP)) / TOK_DEV
    return (tok_loss[0], hidden_grad, g_factor, a_factor)


def solution(mesh):
    finer = Mesh(mesh.devices.reshape(4, 4, 4, mesh.shape["dp"]), ALL)
    return jax.shard_map(
        body,
        mesh=finer,
        in_specs=(P("dp", VOCAB), P(VOCAB, None), P("dp"), P("dp")),
        out_specs=(P("dp"), P("dp", VOCAB), P(ALL, None), P(VOCAB, None)),
        check_vma=False,
    )
```

```python
import jax
import jax.numpy as jnp
import numpy as np
from jax import lax
from jax.experimental import pallas as pl
from jax.experimental.pallas import tpu as pltpu
from jax.sharding import Mesh
from jax.sharding import PartitionSpec as P

TOK_DEV = 1024
VOCAB = ("vocab_0", "vocab_1", "vocab_2")
ALL = ("vocab_0", "vocab_1", "vocab_2", "dp")
ALL_VMEM = (64 << 20) - (256 << 10)

SMALL = (((0, 1), (2, 3)), ((0, 3), (1, 2)))
LARGE = (((1, 2), (0, 3)), ((0, 1), (3, 2)))
SWAP = [(0, 1), (1, 0)]
F32 = jnp.float32
BF16 = jnp.bfloat16

GROUPS = (
    ((0, 64, 0), (1, 64, 0), (2, 48, 0)),
    ((2, 16, 48), (3, 64, 0), (4, 64, 0), (5, 32, 0)),
    ((5, 32, 32), (6, 64, 0), (7, 64, 0)),
)
SIZES = [sum(rows for _, rows, _ in group) for group in GROUPS]
STARTS = [0, SIZES[0], SIZES[0] + SIZES[1]]


def device(y, z, x, core):
    return ((y * 4 + z) * 4 + x) * 2 + core


def small_cubes():
    return [
        [device(y, z, x, core) for y in a for z in b for x in c]
        for core in (0, 1) for a in SMALL[core] for b in SMALL[core] for c in SMALL[core]
    ]


def partner(core, c):
    return next(p[1 - p.index(c)] for p in LARGE[core] if c in p)


def spots():
    return [(y, z, x, core) for y in range(4) for z in range(4) for x in range(4) for core in (0, 1)]


def large_pairs(axis):
    out = []
    for at in spots():
        to = list(at)
        to[axis] = partner(at[3], at[axis])
        out.append((device(*at), device(*to)))
    return out


def chip_table():
    table = np.zeros((128, 3, 8, 8), np.int32)
    for at in spots():
        core = at[3]
        for group in range(3):
            for l in range(8):
                for s in range(8):
                    chip = 0
                    for axis in range(3):
                        c = at[axis]
                        if l >> ((axis - group) % 3) & 1:
                            c = partner(core, c)
                        pair = next(p for p in SMALL[core] if c in p)
                        chip = chip * 4 + pair[s >> (2 - axis) & 1]
                    table[device(*at), group, l, s] = chip
    return table.reshape(128, 192)


SMALL_CUBES = small_cubes()
LARGE_PAIRS = [large_pairs(axis) for axis in range(3)]
CHIPS = chip_table()


def small_stage(x):
    return lax.all_to_all(x, ALL, 0, 0, axis_index_groups=SMALL_CUBES, tiled=True)


def in_hbm(x):
    return pltpu.with_memory_space_constraint(x, pltpu.HBM)


def gathered_groups(some):
    def get(x, g, step):
        return lax.ppermute(x, ALL, LARGE_PAIRS[(g + step) % 3])

    held = [some[start : start + size] for start, size in zip(STARTS, SIZES)]
    got = [get(held[g], g, 0) for g in range(3)]
    first = [jnp.concatenate([h, r]) for h, r in zip(held, got)]
    second = [get(first[g], g, 1) for g in range(3)]
    third = [get(first[g], g, 2) for g in range(3)]
    fourth = [get(second[g], g, 2) for g in range(3)]
    return [[first[g], second[g], third[g], fourth[g]] for g in range(3)]


def add_kernel(*refs):
    *terms, out = refs
    total = terms[0][...].astype(F32)
    for term in terms[1:]:
        total = total + term[...].astype(F32)
    out[...] = total.astype(BF16)


def add_up(count, *terms):
    _, rows, tokens = terms[0][0].shape
    block = lambda first: pl.BlockSpec((None, rows, tokens), lambda i: (first + i, 0, 0))
    return pl.pallas_call(
        add_kernel,
        grid=(count,),
        in_specs=[block(first) for _, first in terms],
        out_specs=block(0),
        out_shape=jax.ShapeDtypeStruct((count, rows, tokens), BF16),
        compiler_params=pltpu.CompilerParams(
            dimension_semantics=("arbitrary",), vmem_limit_bytes=ALL_VMEM
        ),
        cost_estimate=pl.CostEstimate(
            flops=len(terms) * count * rows * tokens,
            bytes_accessed=2 * (len(terms) + 1) * count * rows * tokens, transcendentals=0,
        ),
    )(*[in_hbm(x) for x, _ in terms])


def last_kernel(*refs):
    *terms, out = refs
    for g in range(3):
        total = terms[4 * g][...].astype(F32)
        for term in terms[4 * g + 1 : 4 * g + 4]:
            total = total + term[...].astype(F32)
        out[STARTS[g] : STARTS[g] + SIZES[g]] = total.astype(BF16)


def add_last(terms):
    tokens = terms[0].shape[2]
    part = tokens // 2
    return pl.pallas_call(
        last_kernel,
        grid=(2,),
        in_specs=[
            pl.BlockSpec((None, x.shape[1], part), lambda i: (0, 0, i)) for x in terms
        ],
        out_specs=pl.BlockSpec((sum(SIZES), part), lambda i: (0, i)),
        out_shape=jax.ShapeDtypeStruct((sum(SIZES), tokens), BF16),
        compiler_params=pltpu.CompilerParams(
            dimension_semantics=("arbitrary",), vmem_limit_bytes=ALL_VMEM
        ),
        cost_estimate=pl.CostEstimate(
            flops=4 * sum(SIZES) * tokens, bytes_accessed=10 * sum(SIZES) * tokens, transcendentals=0
        ),
    )(*[in_hbm(x) for x in terms])


def summed_groups(sends, keeps):
    def trade(x, g, step):
        return lax.ppermute(x, ALL, LARGE_PAIRS[(g + step) % 3])

    far = [trade(sends[g], g, 2) for g in range(3)]
    mid = [trade(add_up(2, (keeps[g], 2), (far[g], 2)), g, 1) for g in range(3)]
    near = [
        trade(add_up(1, (keeps[g], 1), (far[g], 1), (mid[g], 1)), g, 0) for g in range(3)
    ]
    return add_last([x for g in range(3) for x in (keeps[g], far[g], mid[g], near[g])])


def sum_kernel(pieces, out):
    out[...] = jnp.sum(pieces[...].astype(F32), axis=0).astype(BF16)


def summed(pieces):
    count, rows, tokens = pieces.shape
    return pl.pallas_call(
        sum_kernel,
        grid=(2,),
        in_specs=[pl.BlockSpec((count, rows, tokens // 2), lambda i: (0, 0, i))],
        out_specs=pl.BlockSpec((rows, tokens // 2), lambda i: (0, i)),
        out_shape=jax.ShapeDtypeStruct((rows, tokens), BF16),
        compiler_params=pltpu.CompilerParams(
            dimension_semantics=("arbitrary",), vmem_limit_bytes=8 << 20
        ),
    )(pieces)


def gather_copies(chips, got, h):
    quarters = []
    for large in (0, 1):
        for small in (0, 1):
            copies = []
            for g, group in enumerate(GROUPS):
                for l in range(8):
                    if l >> (-g % 3) & 1 != large:
                        continue
                    src, at = got[4 * g + l // 2], (l % 2) * SIZES[g]
                    for s, count, first in group:
                        if s >> 2 == small:
                            dst = pl.multiple_of(chips[64 * g + 8 * l + s] * 64 + first, 16)
                            copies.append((src.at[pl.ds(at, count)], h.at[pl.ds(dst, count)]))
                        at += count
            quarters.append((chips[8 * large + 4 * small] // 16, copies))
    return quarters


def a_kernel(chips, *refs):
    got, (own, out, h, sem) = refs[:12], refs[12:]
    for _, copies in gather_copies(chips, got, h):
        for src, dst in copies:
            pltpu.make_async_copy(src, dst, sem).start()
    pltpu.make_async_copy(h, h, sem).wait()
    out[...] = lax.dot_general(
        own[...], h[...], (((1,), (1,)), ((), ())), preferred_element_type=F32
    )


def a_part_of(chips, got, own):
    feats, tokens = own.shape
    width = 64 * feats
    return pl.pallas_call(
        a_kernel,
        grid_spec=pltpu.PrefetchScalarGridSpec(
            num_scalar_prefetch=1,
            grid=(),
            in_specs=[pl.BlockSpec(memory_space=pltpu.HBM)] * len(got)
            + [pl.BlockSpec(memory_space=pltpu.VMEM)],
            out_specs=pl.BlockSpec(memory_space=pltpu.VMEM),
            scratch_shapes=[pltpu.VMEM((width, tokens), BF16), pltpu.SemaphoreType.DMA],
        ),
        out_shape=jax.ShapeDtypeStruct((feats, width), F32),
        compiler_params=pltpu.CompilerParams(vmem_limit_bytes=ALL_VMEM),
        cost_estimate=pl.CostEstimate(
            flops=2 * feats * width * tokens, bytes_accessed=2 * width * tokens, transcendentals=0
        ),
    )(chips, *[in_hbm(x) for x in got], own)


def columns_kernel(chips, w, wide):
    rows = w.shape[0]
    lane = lax.broadcasted_iota(jnp.int32, (rows, 128), 1)
    for l in range(8):
        for tile in range(4):
            done = None
            for g, group in enumerate(GROUPS):
                for s, count, first in group:
                    if s // 2 != tile:
                        continue
                    chip, side = chips[64 * g + 8 * l + s], s % 2
                    block = w[:, pl.ds(pl.multiple_of(chip // 2 * 128, 128), 128)].astype(F32)
                    block = pltpu.roll(block, 64 * (chip % 2 != side).astype(jnp.int32), 1)
                    done = block if done is None else jnp.where(
                        lane >= 64 * side + first, block, done
                    )
            wide[:, (4 * l + tile) * 128 : (4 * l + tile + 1) * 128] = done.astype(BF16)


def columns_turned(chips, w):
    vocab_rows, width = w.shape
    block = pl.BlockSpec((128, width), lambda i, t: (i, 0))
    return pl.pallas_call(
        columns_kernel,
        grid_spec=pltpu.PrefetchScalarGridSpec(
            num_scalar_prefetch=1, grid=(vocab_rows // 128,), in_specs=[block], out_specs=block
        ),
        out_shape=pltpu.HBM((vocab_rows, width), BF16),
        compiler_params=pltpu.CompilerParams(
            dimension_semantics=("arbitrary",), vmem_limit_bytes=24 << 20
        ),
        cost_estimate=pl.CostEstimate(
            flops=1024 * vocab_rows * width, bytes_accessed=4 * vocab_rows * width, transcendentals=0
        ),
    )(chips, in_hbm(w))


def rows_kernel(w, tall):
    tall[...] = w[...].T


def rows_turned(w):
    vocab_rows, width = w.shape
    size = width // 8
    return pl.pallas_call(
        rows_kernel,
        grid=(8,),
        in_specs=[pl.BlockSpec((vocab_rows, size), lambda i: (0, i))],
        out_specs=pl.BlockSpec((size, vocab_rows), lambda i: (i, 0)),
        out_shape=pltpu.HBM((width, vocab_rows), BF16),
        compiler_params=pltpu.CompilerParams(
            dimension_semantics=("arbitrary",), vmem_limit_bytes=24 << 20
        ),
        cost_estimate=pl.CostEstimate(
            flops=1024 * vocab_rows * width, bytes_accessed=4 * vocab_rows * width, transcendentals=0
        ),
    )(in_hbm(w))


def row_pieces(step, vocab_rows):
    def spec(g, s, count, first):
        place = lambda i, t: (t[64 * g + 8 * step(i) + s], first // count, 0)
        return pl.BlockSpec((None, count, vocab_rows), place)

    return [spec(g, s, count, first) for g, group in enumerate(GROUPS) for s, count, first in group]


PIECES = sum(len(group) for group in GROUPS)


def half_copies(got, h):
    size = sum(SIZES)
    for g in range(3):
        for l in range(4):
            src = got[2 * g + l // 2].at[pl.ds((l % 2) * SIZES[g], SIZES[g])]
            yield src, h.at[pl.ds(l * size + STARTS[g], SIZES[g])]


def early_kernel(*refs):
    got, (w, part, h, sem) = refs[:6], refs[6:]

    @pl.when(pl.program_id(0) == 0)
    def _():
        for src, dst in half_copies(got, h):
            pltpu.make_async_copy(src, dst, sem).start()
        pltpu.make_async_copy(h, h, sem).wait()

    part[...] = jnp.dot(w[...], h[...], preferred_element_type=F32)


def late_kernel(*refs):
    got, (w, part, tgt, logits, stats, h, top, total, hit, sem) = refs[:6], refs[6:]
    step = pl.program_id(0)
    rows, tokens = logits.shape

    @pl.when(step == 0)
    def _():
        for src, dst in half_copies(got, h):
            pltpu.make_async_copy(src, dst, sem).start()
        top[...] = jnp.full(top.shape, -jnp.inf, F32)
        total[...] = jnp.zeros(total.shape, F32)
        hit[...] = jnp.zeros(hit.shape, F32)
        pltpu.make_async_copy(h, h, sem).wait()

    block = part[...] + jnp.dot(w[...], h[...], preferred_element_type=F32)
    logits[...] = block
    at = lax.broadcasted_iota(jnp.int32, block.shape, 0) + step * rows
    hit[...] += jnp.sum(jnp.where(at == tgt[...], block, F32(0.0)), axis=0, keepdims=True)
    now = jnp.maximum(top[...], jnp.max(block, axis=0, keepdims=True))
    added = jnp.sum(jnp.exp(block - now), axis=0, keepdims=True)
    total[...] = total[...] * jnp.exp(top[...] - now) + added
    top[...] = now

    @pl.when(step == pl.num_programs(0) - 1)
    def _():
        lse = top[...] + jnp.log(total[...])
        both = [r[:, k : k + 128] for r in (lse, hit[...]) for k in range(0, tokens, 128)]
        stats[...] = jnp.broadcast_to(jnp.concatenate(both, axis=0)[None], stats.shape)


LOGIT_ROWS = 256


def half_logits(half, got, wide, part=None, tgt=None):
    vocab_rows, width = wide.shape
    tokens = got[0].shape[1]
    rows, lines = LOGIT_ROWS, 2 * tokens // 128
    block = pl.BlockSpec((rows, tokens), lambda i: (i, 0))
    row = pl.BlockSpec((1, tokens), lambda i: (0, 0))
    late = part is not None
    return pl.pallas_call(
        late_kernel if late else early_kernel,
        grid=(vocab_rows // rows,),
        in_specs=[pl.BlockSpec(memory_space=pl.ANY)] * len(got)
        + [pl.BlockSpec((rows, width // 2), lambda i: (i, half))]
        + ([block, row] if late else []),
        out_specs=[block, pl.BlockSpec((64, lines, 128), lambda i: (0, 0, 0))] if late else block,
        out_shape=[
            pltpu.HBM((vocab_rows, tokens), F32), jax.ShapeDtypeStruct((64, lines, 128), F32),
        ] if late else pltpu.HBM((vocab_rows, tokens), F32),
        scratch_shapes=[pltpu.VMEM((width // 2, tokens), BF16)]
        + [pltpu.VMEM((1, tokens), F32)] * (3 if late else 0)
        + [pltpu.SemaphoreType.DMA],
        compiler_params=pltpu.CompilerParams(
            dimension_semantics=("arbitrary",), vmem_limit_bytes=ALL_VMEM
        ),
        cost_estimate=pl.CostEstimate(
            flops=vocab_rows * width * tokens,
            bytes_accessed=width * (vocab_rows + tokens) + 4 * vocab_rows * tokens,
            transcendentals=vocab_rows * tokens,
        ),
    )(*got, in_hbm(wide), *([in_hbm(part), tgt] if late else []))


def signal_kernel(chips, stats, logits, cot, tgt, *refs):
    pieces, (grad, loss), outs, (row, whole) = (
        refs[:PIECES], refs[PIECES : PIECES + 2], refs[PIECES + 2 : -2], refs[-2:]
    )
    step = pl.program_id(0)
    rows, tokens = logits.shape
    lines = tokens // 128
    count = whole.shape[0] // rows

    @pl.when(step == 0)
    def _():
        lse = stats[:, :lines]
        top = jnp.max(lse, axis=0)
        full = top + jnp.log(jnp.sum(jnp.exp(lse - top[None]), axis=0))
        tok = full - jnp.sum(stats[:, lines:], axis=0)
        row[...] = jnp.concatenate([full[k : k + 1] for k in range(lines)], axis=1)
        loss[...] = jnp.concatenate([tok[k : k + 1] for k in range(lines)], axis=1)

    @pl.when(step < count)
    def _():
        block = logits[...]
        at = lax.broadcasted_iota(jnp.int32, block.shape, 0) + step * rows
        one = jnp.where(at == tgt[...], F32(1.0), F32(0.0))
        done = (cot[...] * (jnp.exp(block - row[...]) - one)).astype(BF16)
        grad[...] = done
        whole[pl.ds(pl.multiple_of(step * rows, rows), rows)] = done

    @pl.when(step >= count)
    def _():
        rows_here = jnp.concatenate([p[...] for p in pieces], axis=0)
        block = jnp.dot(rows_here, whole[...], preferred_element_type=F32).astype(BF16)
        for start, size, out in zip(STARTS, SIZES, outs):
            out[...] = block[start : start + size]


def signal_of(chips, stats, logits, cot, tgt, tall):
    vocab_rows, tokens = logits.shape
    width = tall.shape[0]
    rows = 256
    count = vocab_rows // rows
    early = lambda i: jnp.minimum(i, count - 1)
    late = lambda i: jnp.maximum(i - count, 0)
    whole = lambda *shape: pl.BlockSpec(shape, lambda i, t: (0,) * len(shape))
    grad, loss, *sums = pl.pallas_call(
        signal_kernel,
        grid_spec=pltpu.PrefetchScalarGridSpec(num_scalar_prefetch=1, grid=(count + 4,), in_specs=[
            whole(*stats.shape),
            pl.BlockSpec((rows, tokens), lambda i, t: (early(i), 0)),
            whole(1, tokens),
            whole(1, tokens),
        ] + row_pieces(lambda i: 4 + late(i), vocab_rows),
        out_specs=[pl.BlockSpec((rows, tokens), lambda i, t: (early(i), 0)), whole(1, tokens)]
        + [pl.BlockSpec((None, size, tokens), lambda i, t: (late(i), 0, 0)) for size in SIZES],
        scratch_shapes=[pltpu.VMEM((1, tokens), F32), pltpu.VMEM((vocab_rows, tokens), BF16)]),
        out_shape=[
            pltpu.HBM((vocab_rows, tokens), BF16),
            jax.ShapeDtypeStruct((1, tokens), F32),
        ] + [pltpu.HBM((4, size, tokens), BF16) for size in SIZES],
        compiler_params=pltpu.CompilerParams(
            dimension_semantics=("arbitrary",), vmem_limit_bytes=ALL_VMEM
        ),
        cost_estimate=pl.CostEstimate(
            flops=vocab_rows * width * tokens,
            bytes_accessed=6 * vocab_rows * tokens + width * (vocab_rows + tokens),
            transcendentals=vocab_rows * tokens,
        ),
    )(
        chips, stats, in_hbm(logits), cot, tgt,
        *[in_hbm(tall.reshape(64, width // 64, vocab_rows))] * PIECES,
    )
    return grad, loss, sums


def grad_kernel(chips, *refs):
    pieces, grad, outs = refs[:PIECES], refs[PIECES], refs[PIECES + 1 :]
    rows_here = jnp.concatenate([p[...] for p in pieces], axis=0)
    block = jnp.dot(rows_here, grad[...], preferred_element_type=F32).astype(BF16)
    for start, size, out in zip(STARTS, SIZES, outs):
        out[...] = block[start : start + size]


def half_grads(chips, half, tall, grad):
    vocab_rows, tokens = grad.shape
    width = tall.shape[0]
    return pl.pallas_call(
        grad_kernel,
        grid_spec=pltpu.PrefetchScalarGridSpec(
            num_scalar_prefetch=1,
            grid=(4,),
            in_specs=row_pieces(lambda i: 4 * half + i, vocab_rows)
            + [pl.BlockSpec((vocab_rows, tokens), lambda i, t: (0, 0))],
            out_specs=[pl.BlockSpec((None, size, tokens), lambda i, t: (i, 0, 0)) for size in SIZES],
        ),
        out_shape=[pltpu.HBM((4, size, tokens), BF16) for size in SIZES],
        compiler_params=pltpu.CompilerParams(
            dimension_semantics=("arbitrary",), vmem_limit_bytes=ALL_VMEM
        ),
        cost_estimate=pl.CostEstimate(
            flops=vocab_rows * width * tokens, bytes_accessed=width * (vocab_rows + tokens),
            transcendentals=0,
        ),
    )(chips, *[in_hbm(tall.reshape(64, width // 64, vocab_rows))] * PIECES, grad)


def body(hidden, head_weight, targets, loss_cot):
    vocab_rows, _ = head_weight.shape
    own = hidden.T
    feats, tokens = own.shape
    core = lax.axis_index("dp")
    chips = lax.dynamic_index_in_dim(jnp.asarray(CHIPS), lax.axis_index(ALL), 0, keepdims=False)
    tgt = (targets - lax.axis_index(VOCAB) * vocab_rows)[None, :]
    some = small_stage(jnp.broadcast_to(own[None], (8, feats, tokens)))
    wide = columns_turned(chips, head_weight)
    got = gathered_groups(some.reshape(8 * feats, tokens))
    part = half_logits(0, [a for group in got for a in group[:2]], wide)
    logits, stats = half_logits(1, [a for group in got for a in group[2:]], wide, part, tgt)
    stats = lax.all_to_all(stats, VOCAB, 0, 0, tiled=True)
    tall = rows_turned(head_weight)
    a_part = a_part_of(chips, [a for group in got for a in group], own)
    grad, tok_loss, sends = signal_of(chips, stats, logits, loss_cot[None, :], tgt, tall)
    sums = summed_groups(sends, half_grads(chips, 0, tall, grad))
    sums = small_stage(sums.reshape(8, feats, tokens))
    hidden_grad = summed(sums).T
    rows = vocab_rows // 2

    def gram(x):
        mine = lax.dynamic_slice_in_dim(x, core * rows, rows, 0)
        return lax.dot_general(mine, x, (((1,), (1,)), ((), ())), preferred_element_type=F32)

    g_factor = (gram(grad) + gram(lax.ppermute(grad, "dp", SWAP))) / TOK_DEV
    a_factor = (a_part + lax.ppermute(a_part, "dp", SWAP)) / TOK_DEV
    return (tok_loss[0], hidden_grad, g_factor, a_factor)


def solution(mesh):
    finer = Mesh(mesh.devices.reshape(4, 4, 4, mesh.shape["dp"]), ALL)
    return jax.shard_map(
        body,
        mesh=finer,
        in_specs=(P("dp", VOCAB), P(VOCAB, None), P("dp"), P("dp")),
        out_specs=(P("dp"), P("dp", VOCAB), P(ALL, None), P(VOCAB, None)),
        check_vma=False,
    )
```

```python
import jax
import jax.numpy as jnp
import numpy as np
from jax import lax
from jax.experimental import pallas as pl
from jax.experimental.pallas import tpu as pltpu
from jax.sharding import Mesh
from jax.sharding import PartitionSpec as P

TOK_DEV = 1024
VOCAB = ("vocab_0", "vocab_1", "vocab_2")
ALL = ("vocab_0", "vocab_1", "vocab_2", "dp")
ALL_VMEM = (64 << 20) - (256 << 10)

SMALL = (((0, 1), (2, 3)), ((0, 3), (1, 2)))
LARGE = (((1, 2), (0, 3)), ((0, 1), (3, 2)))
SWAP = [(0, 1), (1, 0)]
F32 = jnp.float32
BF16 = jnp.bfloat16

GROUPS = (
    ((0, 64, 0), (1, 64, 0), (2, 48, 0)),
    ((2, 16, 48), (3, 64, 0), (4, 64, 0), (5, 32, 0)),
    ((5, 32, 32), (6, 64, 0), (7, 64, 0)),
)
SIZES = [sum(rows for _, rows, _ in group) for group in GROUPS]
STARTS = [0, SIZES[0], SIZES[0] + SIZES[1]]


def device(y, z, x, core):
    return ((y * 4 + z) * 4 + x) * 2 + core


def small_cubes():
    return [
        [device(y, z, x, core) for y in a for z in b for x in c]
        for core in (0, 1) for a in SMALL[core] for b in SMALL[core] for c in SMALL[core]
    ]


def partner(core, c):
    return next(p[1 - p.index(c)] for p in LARGE[core] if c in p)


def spots():
    return [(y, z, x, core) for y in range(4) for z in range(4) for x in range(4) for core in (0, 1)]


def large_pairs(axis):
    out = []
    for at in spots():
        to = list(at)
        to[axis] = partner(at[3], at[axis])
        out.append((device(*at), device(*to)))
    return out


def chip_table():
    table = np.zeros((128, 3, 8, 8), np.int32)
    for at in spots():
        core = at[3]
        for group in range(3):
            for l in range(8):
                for s in range(8):
                    chip = 0
                    for axis in range(3):
                        c = at[axis]
                        if l >> ((axis - group) % 3) & 1:
                            c = partner(core, c)
                        pair = next(p for p in SMALL[core] if c in p)
                        chip = chip * 4 + pair[s >> (2 - axis) & 1]
                    table[device(*at), group, l, s] = chip
    return table.reshape(128, 192)


SMALL_CUBES = small_cubes()
LARGE_PAIRS = [large_pairs(axis) for axis in range(3)]
CHIPS = chip_table()


def small_stage(x):
    return lax.all_to_all(x, ALL, 0, 0, axis_index_groups=SMALL_CUBES, tiled=True)


def in_hbm(x):
    return pltpu.with_memory_space_constraint(x, pltpu.HBM)


def gathered_groups(some):
    def get(x, g, step):
        return lax.ppermute(x, ALL, LARGE_PAIRS[(g + step) % 3])

    held = [some[start : start + size] for start, size in zip(STARTS, SIZES)]
    got = [get(held[g], g, 0) for g in range(3)]
    first = [jnp.concatenate([h, r]) for h, r in zip(held, got)]
    second = [get(first[g], g, 1) for g in range(3)]
    third = [get(first[g], g, 2) for g in range(3)]
    fourth = [get(second[g], g, 2) for g in range(3)]
    return [[first[g], second[g], third[g], fourth[g]] for g in range(3)]


def add_kernel(*refs):
    *terms, out = refs
    total = terms[0][...].astype(F32)
    for term in terms[1:]:
        total = total + term[...].astype(F32)
    out[...] = total.astype(BF16)


def add_up(count, *terms):
    _, rows, tokens = terms[0][0].shape
    block = lambda first: pl.BlockSpec((None, rows, tokens), lambda i: (first + i, 0, 0))
    return pl.pallas_call(
        add_kernel,
        grid=(count,),
        in_specs=[block(first) for _, first in terms],
        out_specs=block(0),
        out_shape=jax.ShapeDtypeStruct((count, rows, tokens), BF16),
        compiler_params=pltpu.CompilerParams(
            dimension_semantics=("arbitrary",), vmem_limit_bytes=12 << 20
        ),
        cost_estimate=pl.CostEstimate(
            flops=len(terms) * count * rows * tokens,
            bytes_accessed=2 * (len(terms) + 1) * count * rows * tokens, transcendentals=0,
        ),
    )(*[in_hbm(x) if x.shape[0] == 4 else x for x, _ in terms])


def last_kernel(*refs):
    *terms, out = refs
    for g in range(3):
        total = terms[4 * g][...].astype(F32)
        for term in terms[4 * g + 1 : 4 * g + 4]:
            total = total + term[...].astype(F32)
        out[STARTS[g] : STARTS[g] + SIZES[g]] = total.astype(BF16)


def add_last(terms):
    tokens = terms[0].shape[2]
    part = tokens // 2
    return pl.pallas_call(
        last_kernel,
        grid=(2,),
        in_specs=[
            pl.BlockSpec((None, x.shape[1], part), lambda i: (0, 0, i)) for x in terms
        ],
        out_specs=pl.BlockSpec((sum(SIZES), part), lambda i: (0, i)),
        out_shape=jax.ShapeDtypeStruct((sum(SIZES), tokens), BF16),
        compiler_params=pltpu.CompilerParams(
            dimension_semantics=("arbitrary",), vmem_limit_bytes=16 << 20
        ),
        cost_estimate=pl.CostEstimate(
            flops=4 * sum(SIZES) * tokens, bytes_accessed=10 * sum(SIZES) * tokens, transcendentals=0
        ),
    )(*[in_hbm(x) if x.shape[0] == 4 else x for x in terms])


def summed_groups(sends, keeps):
    def trade(x, g, step):
        return lax.ppermute(x, ALL, LARGE_PAIRS[(g + step) % 3])

    far = [trade(sends[g], g, 2) for g in range(3)]
    mid = [trade(add_up(2, (keeps[g], 2), (far[g], 2)), g, 1) for g in range(3)]
    near = [
        trade(add_up(1, (keeps[g], 1), (far[g], 1), (mid[g], 1)), g, 0) for g in range(3)
    ]
    return add_last([x for g in range(3) for x in (keeps[g], far[g], mid[g], near[g])])


def sum_kernel(pieces, out):
    out[...] = jnp.sum(pieces[...].astype(F32), axis=0).astype(BF16)


def summed(pieces):
    count, rows, tokens = pieces.shape
    return pl.pallas_call(
        sum_kernel,
        grid=(2,),
        in_specs=[pl.BlockSpec((count, rows, tokens // 2), lambda i: (0, 0, i))],
        out_specs=pl.BlockSpec((rows, tokens // 2), lambda i: (0, i)),
        out_shape=jax.ShapeDtypeStruct((rows, tokens), BF16),
        compiler_params=pltpu.CompilerParams(
            dimension_semantics=("arbitrary",), vmem_limit_bytes=8 << 20
        ),
    )(pieces)


def gather_copies(chips, got, h):
    quarters = []
    for large in (0, 1):
        for small in (0, 1):
            copies = []
            for g, group in enumerate(GROUPS):
                for l in range(8):
                    if l >> (-g % 3) & 1 != large:
                        continue
                    src, at = got[4 * g + l // 2], (l % 2) * SIZES[g]
                    for s, count, first in group:
                        if s >> 2 == small:
                            dst = pl.multiple_of(chips[64 * g + 8 * l + s] * 64 + first, 16)
                            copies.append((src.at[pl.ds(at, count)], h.at[pl.ds(dst, count)]))
                        at += count
            quarters.append((chips[8 * large + 4 * small] // 16, copies))
    return quarters


def a_kernel(chips, *refs):
    got, (own, out, h, sem) = refs[:12], refs[12:]
    for _, copies in gather_copies(chips, got, h):
        for src, dst in copies:
            pltpu.make_async_copy(src, dst, sem).start()
    pltpu.make_async_copy(h, h, sem).wait()
    out[...] = lax.dot_general(
        own[...], h[...], (((1,), (1,)), ((), ())), preferred_element_type=F32
    )


def a_part_of(chips, got, own):
    feats, tokens = own.shape
    width = 64 * feats
    return pl.pallas_call(
        a_kernel,
        grid_spec=pltpu.PrefetchScalarGridSpec(
            num_scalar_prefetch=1,
            grid=(),
            in_specs=[pl.BlockSpec(memory_space=pltpu.HBM)] * len(got)
            + [pl.BlockSpec(memory_space=pltpu.VMEM)],
            out_specs=pl.BlockSpec(memory_space=pltpu.VMEM),
            scratch_shapes=[pltpu.VMEM((width, tokens), BF16), pltpu.SemaphoreType.DMA],
        ),
        out_shape=jax.ShapeDtypeStruct((feats, width), F32),
        compiler_params=pltpu.CompilerParams(vmem_limit_bytes=ALL_VMEM),
        cost_estimate=pl.CostEstimate(
            flops=2 * feats * width * tokens, bytes_accessed=2 * width * tokens, transcendentals=0
        ),
    )(chips, *[in_hbm(x) for x in got], own)


def columns_kernel(chips, w, wide):
    rows = w.shape[0]
    lane = lax.broadcasted_iota(jnp.int32, (rows, 128), 1)
    for l in range(8):
        for tile in range(4):
            done = None
            for g, group in enumerate(GROUPS):
                for s, count, first in group:
                    if s // 2 != tile:
                        continue
                    chip, side = chips[64 * g + 8 * l + s], s % 2
                    block = w[:, pl.ds(pl.multiple_of(chip // 2 * 128, 128), 128)].astype(F32)
                    block = pltpu.roll(block, 64 * (chip % 2 != side).astype(jnp.int32), 1)
                    done = block if done is None else jnp.where(
                        lane >= 64 * side + first, block, done
                    )
            wide[:, (4 * l + tile) * 128 : (4 * l + tile + 1) * 128] = done.astype(BF16)


def columns_turned(chips, w):
    vocab_rows, width = w.shape
    block = pl.BlockSpec((128, width), lambda i, t: (i, 0))
    return pl.pallas_call(
        columns_kernel,
        grid_spec=pltpu.PrefetchScalarGridSpec(
            num_scalar_prefetch=1, grid=(vocab_rows // 128,), in_specs=[block], out_specs=block
        ),
        out_shape=pltpu.HBM((vocab_rows, width), BF16),
        compiler_params=pltpu.CompilerParams(
            dimension_semantics=("arbitrary",), vmem_limit_bytes=24 << 20
        ),
        cost_estimate=pl.CostEstimate(
            flops=1024 * vocab_rows * width, bytes_accessed=4 * vocab_rows * width, transcendentals=0
        ),
    )(chips, in_hbm(w))


def rows_kernel(chips, w, tall, turned, sem):
    step = pl.program_id(0)
    size = w.shape[1]
    turned[pl.ds(pl.multiple_of(step * size, size), size)] = w[...].T

    @pl.when(step == pl.num_programs(0) - 1)
    def _():
        for g, group in enumerate(GROUPS):
            for l in range(8):
                at = l * sum(SIZES) + STARTS[g]
                for s, count, first in group:
                    src = pl.multiple_of(chips[64 * g + 8 * l + s] * 64 + first, 16)
                    pltpu.make_async_copy(
                        turned.at[pl.ds(src, count)], tall.at[pl.ds(at, count)], sem
                    ).start()
                    at += count
        pltpu.make_async_copy(tall, tall, sem).wait()


def rows_turned(chips, w):
    vocab_rows, width = w.shape
    size = width // 8
    return pl.pallas_call(
        rows_kernel,
        grid_spec=pltpu.PrefetchScalarGridSpec(
            num_scalar_prefetch=1,
            grid=(8,),
            in_specs=[pl.BlockSpec((vocab_rows, size), lambda i, t: (0, i))],
            out_specs=pl.BlockSpec(memory_space=pl.ANY),
            scratch_shapes=[pltpu.VMEM((width, vocab_rows), BF16), pltpu.SemaphoreType.DMA],
        ),
        out_shape=pltpu.HBM((width, vocab_rows), BF16),
        compiler_params=pltpu.CompilerParams(
            dimension_semantics=("arbitrary",), vmem_limit_bytes=24 << 20
        ),
        cost_estimate=pl.CostEstimate(
            flops=1024 * vocab_rows * width, bytes_accessed=4 * vocab_rows * width, transcendentals=0
        ),
    )(chips, in_hbm(w))


def half_copies(got, h):
    size = sum(SIZES)
    for g in range(3):
        for l in range(4):
            src = got[2 * g + l // 2].at[pl.ds((l % 2) * SIZES[g], SIZES[g])]
            yield src, h.at[pl.ds(l * size + STARTS[g], SIZES[g])]


def early_kernel(*refs):
    got, (w, part, h, sem) = refs[:6], refs[6:]

    @pl.when(pl.program_id(0) == 0)
    def _():
        for src, dst in half_copies(got, h):
            pltpu.make_async_copy(src, dst, sem).start()
        pltpu.make_async_copy(h, h, sem).wait()

    part[...] = jnp.dot(w[...], h[...], preferred_element_type=F32)


def late_kernel(*refs):
    got, (w, part, tgt, logits, stats, h, top, total, hit, sem) = refs[:6], refs[6:]
    step = pl.program_id(0)
    rows, tokens = logits.shape

    @pl.when(step == 0)
    def _():
        for src, dst in half_copies(got, h):
            pltpu.make_async_copy(src, dst, sem).start()
        top[...] = jnp.full(top.shape, -jnp.inf, F32)
        total[...] = jnp.zeros(total.shape, F32)
        hit[...] = jnp.zeros(hit.shape, F32)
        pltpu.make_async_copy(h, h, sem).wait()

    block = part[...] + jnp.dot(w[...], h[...], preferred_element_type=F32)
    logits[...] = block
    at = lax.broadcasted_iota(jnp.int32, block.shape, 0) + step * rows
    hit[...] += jnp.sum(jnp.where(at == tgt[...], block, F32(0.0)), axis=0, keepdims=True)
    now = jnp.maximum(top[...], jnp.max(block, axis=0, keepdims=True))
    added = jnp.sum(jnp.exp(block - now), axis=0, keepdims=True)
    total[...] = total[...] * jnp.exp(top[...] - now) + added
    top[...] = now

    @pl.when(step == pl.num_programs(0) - 1)
    def _():
        lse = top[...] + jnp.log(total[...])
        both = [r[:, k : k + 128] for r in (lse, hit[...]) for k in range(0, tokens, 128)]
        stats[...] = jnp.broadcast_to(jnp.concatenate(both, axis=0)[None], stats.shape)


LOGIT_ROWS = 256


def half_logits(half, got, wide, part=None, tgt=None):
    vocab_rows, width = wide.shape
    tokens = got[0].shape[1]
    rows, lines = LOGIT_ROWS, 2 * tokens // 128
    block = pl.BlockSpec((rows, tokens), lambda i: (i, 0))
    row = pl.BlockSpec((1, tokens), lambda i: (0, 0))
    late = part is not None
    return pl.pallas_call(
        late_kernel if late else early_kernel,
        grid=(vocab_rows // rows,),
        in_specs=[pl.BlockSpec(memory_space=pl.ANY)] * len(got)
        + [pl.BlockSpec((rows, width // 2), lambda i: (i, half))]
        + ([block, row] if late else []),
        out_specs=[block, pl.BlockSpec((64, lines, 128), lambda i: (0, 0, 0))] if late else block,
        out_shape=[
            pltpu.HBM((vocab_rows, tokens), F32), jax.ShapeDtypeStruct((64, lines, 128), F32),
        ] if late else pltpu.HBM((vocab_rows, tokens), F32),
        scratch_shapes=[pltpu.VMEM((width // 2, tokens), BF16)]
        + [pltpu.VMEM((1, tokens), F32)] * (3 if late else 0)
        + [pltpu.SemaphoreType.DMA],
        compiler_params=pltpu.CompilerParams(
            dimension_semantics=("arbitrary",), vmem_limit_bytes=32 << 20
        ),
        cost_estimate=pl.CostEstimate(
            flops=vocab_rows * width * tokens,
            bytes_accessed=width * (vocab_rows + tokens) + 4 * vocab_rows * tokens,
            transcendentals=vocab_rows * tokens,
        ),
    )(*got, in_hbm(wide), *([in_hbm(part), tgt] if late else []))


def signal_kernel(stats, logits, cot, tgt, tall, grad, loss, *refs):
    outs, (row, whole) = refs[:3], refs[3:]
    step = pl.program_id(0)
    rows, tokens = logits.shape
    lines = tokens // 128
    count = whole.shape[0] // rows

    @pl.when(step == 0)
    def _():
        lse = stats[:, :lines]
        top = jnp.max(lse, axis=0)
        full = top + jnp.log(jnp.sum(jnp.exp(lse - top[None]), axis=0))
        tok = full - jnp.sum(stats[:, lines:], axis=0)
        row[...] = jnp.concatenate([full[k : k + 1] for k in range(lines)], axis=1)
        loss[...] = jnp.concatenate([tok[k : k + 1] for k in range(lines)], axis=1)

    @pl.when(step < count)
    def _():
        block = logits[...]
        at = lax.broadcasted_iota(jnp.int32, block.shape, 0) + step * rows
        one = jnp.where(at == tgt[...], F32(1.0), F32(0.0))
        done = (cot[...] * (jnp.exp(block - row[...]) - one)).astype(BF16)
        grad[...] = done
        whole[pl.ds(pl.multiple_of(step * rows, rows), rows)] = done

    @pl.when(step >= count)
    def _():
        block = jnp.dot(tall[...], whole[...], preferred_element_type=F32).astype(BF16)
        for start, size, out in zip(STARTS, SIZES, outs):
            out[...] = block[start : start + size]


def signal_of(stats, logits, cot, tgt, tall):
    vocab_rows, tokens = logits.shape
    width = tall.shape[0]
    rows = 256
    count = vocab_rows // rows
    early = lambda i: jnp.minimum(i, count - 1)
    late = lambda i: jnp.maximum(i - count, 0)
    whole = lambda *shape: pl.BlockSpec(shape, lambda i: (0,) * len(shape))
    grad, loss, *sums = pl.pallas_call(
        signal_kernel,
        grid=(count + 4,),
        in_specs=[
            whole(*stats.shape),
            pl.BlockSpec((rows, tokens), lambda i: (early(i), 0)),
            whole(1, tokens),
            whole(1, tokens),
            pl.BlockSpec((width // 8, vocab_rows), lambda i: (4 + late(i), 0)),
        ],
        out_specs=[pl.BlockSpec((rows, tokens), lambda i: (early(i), 0)), whole(1, tokens)]
        + [pl.BlockSpec((None, size, tokens), lambda i: (late(i), 0, 0)) for size in SIZES],
        out_shape=[
            pltpu.HBM((vocab_rows, tokens), BF16),
            jax.ShapeDtypeStruct((1, tokens), F32),
        ] + [pltpu.HBM((4, size, tokens), BF16) for size in SIZES],
        scratch_shapes=[pltpu.VMEM((1, tokens), F32), pltpu.VMEM((vocab_rows, tokens), BF16)],
        compiler_params=pltpu.CompilerParams(
            dimension_semantics=("arbitrary",), vmem_limit_bytes=ALL_VMEM
        ),
        cost_estimate=pl.CostEstimate(
            flops=vocab_rows * width * tokens,
            bytes_accessed=6 * vocab_rows * tokens + width * (vocab_rows + tokens),
            transcendentals=vocab_rows * tokens,
        ),
    )(stats, in_hbm(logits), cot, tgt, in_hbm(tall))
    return grad, loss, sums


def grad_kernel(tall, grad, *outs):
    block = jnp.dot(tall[...], grad[...], preferred_element_type=F32).astype(BF16)
    for start, size, out in zip(STARTS, SIZES, outs):
        out[...] = block[start : start + size]


def half_grads(half, tall, grad):
    vocab_rows, tokens = grad.shape
    width = tall.shape[0]
    return pl.pallas_call(
        grad_kernel,
        grid=(4,),
        in_specs=[
            pl.BlockSpec((width // 8, vocab_rows), lambda i: (4 * half + i, 0)),
            pl.BlockSpec((vocab_rows, tokens), lambda i: (0, 0)),
        ],
        out_specs=[pl.BlockSpec((None, size, tokens), lambda i: (i, 0, 0)) for size in SIZES],
        out_shape=[pltpu.HBM((4, size, tokens), BF16) for size in SIZES],
        compiler_params=pltpu.CompilerParams(
            dimension_semantics=("arbitrary",), vmem_limit_bytes=ALL_VMEM
        ),
        cost_estimate=pl.CostEstimate(
            flops=vocab_rows * width * tokens, bytes_accessed=width * (vocab_rows + tokens),
            transcendentals=0,
        ),
    )(in_hbm(tall), grad)


def body(hidden, head_weight, targets, loss_cot):
    vocab_rows, _ = head_weight.shape
    own = hidden.T
    feats, tokens = own.shape
    core = lax.axis_index("dp")
    chips = lax.dynamic_index_in_dim(jnp.asarray(CHIPS), lax.axis_index(ALL), 0, keepdims=False)
    tgt = (targets - lax.axis_index(VOCAB) * vocab_rows)[None, :]
    some = small_stage(jnp.broadcast_to(own[None], (8, feats, tokens)))
    wide = columns_turned(chips, head_weight)
    got = gathered_groups(some.reshape(8 * feats, tokens))
    part = half_logits(0, [a for group in got for a in group[:2]], wide)
    logits, stats = half_logits(1, [a for group in got for a in group[2:]], wide, part, tgt)
    stats = lax.all_to_all(stats, VOCAB, 0, 0, tiled=True)
    tall = rows_turned(chips, head_weight)
    a_part = a_part_of(chips, [a for group in got for a in group], own)
    grad, tok_loss, sends = signal_of(stats, logits, loss_cot[None, :], tgt, tall)
    sums = summed_groups(sends, half_grads(0, tall, grad))
    sums = small_stage(sums.reshape(8, feats, tokens))
    hidden_grad = summed(sums).T
    rows = vocab_rows // 2

    def gram(x):
        mine = lax.dynamic_slice_in_dim(x, core * rows, rows, 0)
        return lax.dot_general(mine, x, (((1,), (1,)), ((), ())), preferred_element_type=F32)

    g_factor = (gram(grad) + gram(lax.ppermute(grad, "dp", SWAP))) / TOK_DEV
    a_factor = (a_part + lax.ppermute(a_part, "dp", SWAP)) / TOK_DEV
    return (tok_loss[0], hidden_grad, g_factor, a_factor)


def solution(mesh):
    finer = Mesh(mesh.devices.reshape(4, 4, 4, mesh.shape["dp"]), ALL)
    return jax.shard_map(
        body,
        mesh=finer,
        in_specs=(P("dp", VOCAB), P(VOCAB, None), P("dp"), P("dp")),
        out_specs=(P("dp"), P("dp", VOCAB), P(ALL, None), P(VOCAB, None)),
        check_vma=False,
    )
```

```python
import jax
import jax.numpy as jnp
import numpy as np
from jax import lax
from jax.experimental import pallas as pl
from jax.experimental.pallas import tpu as pltpu
from jax.sharding import Mesh
from jax.sharding import PartitionSpec as P

TOK_DEV = 1024
VOCAB = ("vocab_0", "vocab_1", "vocab_2")
ALL = ("vocab_0", "vocab_1", "vocab_2", "dp")
ALL_VMEM = (64 << 20) - (256 << 10)

SMALL = (((0, 1), (2, 3)), ((0, 3), (1, 2)))
LARGE = (((1, 2), (0, 3)), ((0, 1), (3, 2)))
SWAP = [(0, 1), (1, 0)]
F32 = jnp.float32
BF16 = jnp.bfloat16

GROUPS = (
    ((0, 64, 0), (1, 64, 0), (2, 48, 0)),
    ((2, 16, 48), (3, 64, 0), (4, 64, 0), (5, 32, 0)),
    ((5, 32, 32), (6, 64, 0), (7, 64, 0)),
)
SIZES = [sum(rows for _, rows, _ in group) for group in GROUPS]
STARTS = [0, SIZES[0], SIZES[0] + SIZES[1]]


def device(y, z, x, core):
    return ((y * 4 + z) * 4 + x) * 2 + core


def small_cubes():
    return [
        [device(y, z, x, core) for y in a for z in b for x in c]
        for core in (0, 1) for a in SMALL[core] for b in SMALL[core] for c in SMALL[core]
    ]


def partner(core, c):
    return next(p[1 - p.index(c)] for p in LARGE[core] if c in p)


def spots():
    return [(y, z, x, core) for y in range(4) for z in range(4) for x in range(4) for core in (0, 1)]


def large_pairs(axis):
    out = []
    for at in spots():
        to = list(at)
        to[axis] = partner(at[3], at[axis])
        out.append((device(*at), device(*to)))
    return out


def chip_table():
    table = np.zeros((128, 3, 8, 8), np.int32)
    for at in spots():
        core = at[3]
        for group in range(3):
            for l in range(8):
                for s in range(8):
                    chip = 0
                    for axis in range(3):
                        c = at[axis]
                        if l >> ((axis - group) % 3) & 1:
                            c = partner(core, c)
                        pair = next(p for p in SMALL[core] if c in p)
                        chip = chip * 4 + pair[s >> (2 - axis) & 1]
                    table[device(*at), group, l, s] = chip
    return table.reshape(128, 192)


SMALL_CUBES = small_cubes()
LARGE_PAIRS = [large_pairs(axis) for axis in range(3)]
CHIPS = chip_table()


def small_stage(x):
    return lax.all_to_all(x, ALL, 0, 0, axis_index_groups=SMALL_CUBES, tiled=True)


def in_hbm(x):
    return pltpu.with_memory_space_constraint(x, pltpu.HBM)


def gathered_groups(some):
    def get(x, g, step):
        return lax.ppermute(x, ALL, LARGE_PAIRS[(g + step) % 3])

    held = [some[start : start + size] for start, size in zip(STARTS, SIZES)]
    got = [get(held[g], g, 0) for g in range(3)]
    first = [jnp.concatenate([h, r]) for h, r in zip(held, got)]
    second = [get(first[g], g, 1) for g in range(3)]
    third = [get(first[g], g, 2) for g in range(3)]
    fourth = [get(second[g], g, 2) for g in range(3)]
    return [[first[g], second[g], third[g], fourth[g]] for g in range(3)]


def add_kernel(*refs):
    *terms, out = refs
    total = terms[0][...].astype(F32)
    for term in terms[1:]:
        total = total + term[...].astype(F32)
    out[...] = total.astype(BF16)


def add_up(count, *terms):
    _, rows, tokens = terms[0][0].shape
    block = lambda first: pl.BlockSpec((None, rows, tokens), lambda i: (first + i, 0, 0))
    return pl.pallas_call(
        add_kernel,
        grid=(count,),
        in_specs=[block(first) for _, first in terms],
        out_specs=block(0),
        out_shape=jax.ShapeDtypeStruct((count, rows, tokens), BF16),
        compiler_params=pltpu.CompilerParams(
            dimension_semantics=("arbitrary",), vmem_limit_bytes=12 << 20
        ),
        cost_estimate=pl.CostEstimate(
            flops=len(terms) * count * rows * tokens,
            bytes_accessed=2 * (len(terms) + 1) * count * rows * tokens, transcendentals=0,
        ),
    )(*[in_hbm(x) if x.shape[0] == 4 else x for x, _ in terms])


def last_kernel(*refs):
    *terms, out = refs
    for g in range(3):
        total = terms[4 * g][...].astype(F32)
        for term in terms[4 * g + 1 : 4 * g + 4]:
            total = total + term[...].astype(F32)
        out[STARTS[g] : STARTS[g] + SIZES[g]] = total.astype(BF16)


def add_last(terms):
    tokens = terms[0].shape[2]
    part = tokens // 2
    return pl.pallas_call(
        last_kernel,
        grid=(2,),
        in_specs=[
            pl.BlockSpec((None, x.shape[1], part), lambda i: (0, 0, i)) for x in terms
        ],
        out_specs=pl.BlockSpec((sum(SIZES), part), lambda i: (0, i)),
        out_shape=jax.ShapeDtypeStruct((sum(SIZES), tokens), BF16),
        compiler_params=pltpu.CompilerParams(
            dimension_semantics=("arbitrary",), vmem_limit_bytes=16 << 20
        ),
        cost_estimate=pl.CostEstimate(
            flops=4 * sum(SIZES) * tokens, bytes_accessed=10 * sum(SIZES) * tokens, transcendentals=0
        ),
    )(*[in_hbm(x) if x.shape[0] == 4 else x for x in terms])


def summed_groups(sends, keeps):
    def trade(x, g, step):
        return lax.ppermute(x, ALL, LARGE_PAIRS[(g + step) % 3])

    far = [trade(sends[g], g, 2) for g in range(3)]
    mid = [trade(add_up(2, (keeps[g], 2), (far[g], 2)), g, 1) for g in range(3)]
    near = [
        trade(add_up(1, (keeps[g], 1), (far[g], 1), (mid[g], 1)), g, 0) for g in range(3)
    ]
    return add_last([x for g in range(3) for x in (keeps[g], far[g], mid[g], near[g])])


def sum_kernel(pieces, out):
    out[...] = jnp.sum(pieces[...].astype(F32), axis=0).astype(BF16)


def summed(pieces):
    count, rows, tokens = pieces.shape
    return pl.pallas_call(
        sum_kernel,
        grid=(2,),
        in_specs=[pl.BlockSpec((count, rows, tokens // 2), lambda i: (0, 0, i))],
        out_specs=pl.BlockSpec((rows, tokens // 2), lambda i: (0, i)),
        out_shape=jax.ShapeDtypeStruct((rows, tokens), BF16),
        compiler_params=pltpu.CompilerParams(
            dimension_semantics=("arbitrary",), vmem_limit_bytes=8 << 20
        ),
    )(pieces)


def gather_copies(chips, got, h):
    quarters = []
    for large in (0, 1):
        for small in (0, 1):
            copies = []
            for g, group in enumerate(GROUPS):
                for l in range(8):
                    if l >> (-g % 3) & 1 != large:
                        continue
                    src, at = got[4 * g + l // 2], (l % 2) * SIZES[g]
                    for s, count, first in group:
                        if s >> 2 == small:
                            dst = pl.multiple_of(chips[64 * g + 8 * l + s] * 64 + first, 16)
                            copies.append((src.at[pl.ds(at, count)], h.at[pl.ds(dst, count)]))
                        at += count
            quarters.append((chips[8 * large + 4 * small] // 16, copies))
    return quarters


def a_kernel(chips, *refs):
    got, (own, out, h, sem) = refs[:12], refs[12:]
    for _, copies in gather_copies(chips, got, h):
        for src, dst in copies:
            pltpu.make_async_copy(src, dst, sem).start()
    pltpu.make_async_copy(h, h, sem).wait()
    out[...] = lax.dot_general(
        own[...], h[...], (((1,), (1,)), ((), ())), preferred_element_type=F32
    )


def a_part_of(chips, got, own):
    feats, tokens = own.shape
    width = 64 * feats
    return pl.pallas_call(
        a_kernel,
        grid_spec=pltpu.PrefetchScalarGridSpec(
            num_scalar_prefetch=1,
            grid=(),
            in_specs=[pl.BlockSpec(memory_space=pltpu.HBM)] * len(got)
            + [pl.BlockSpec(memory_space=pltpu.VMEM)],
            out_specs=pl.BlockSpec(memory_space=pltpu.VMEM),
            scratch_shapes=[pltpu.VMEM((width, tokens), BF16), pltpu.SemaphoreType.DMA],
        ),
        out_shape=jax.ShapeDtypeStruct((feats, width), F32),
        compiler_params=pltpu.CompilerParams(vmem_limit_bytes=ALL_VMEM),
        cost_estimate=pl.CostEstimate(
            flops=2 * feats * width * tokens, bytes_accessed=2 * width * tokens, transcendentals=0
        ),
    )(chips, *[in_hbm(x) for x in got], own)


def columns_kernel(chips, w, wide):
    rows = w.shape[0]
    lane = lax.broadcasted_iota(jnp.int32, (rows, 128), 1)
    for l in range(8):
        for tile in range(4):
            done = None
            for g, group in enumerate(GROUPS):
                for s, count, first in group:
                    if s // 2 != tile:
                        continue
                    chip, side = chips[64 * g + 8 * l + s], s % 2
                    block = w[:, pl.ds(pl.multiple_of(chip // 2 * 128, 128), 128)]
                    block = pltpu.roll(block, 64 * (chip % 2 != side).astype(jnp.int32), 1)
                    done = block if done is None else jnp.where(
                        lane >= 64 * side + first, block, done
                    )
            wide[:, (4 * l + tile) * 128 : (4 * l + tile + 1) * 128] = done


def columns_turned(chips, w):
    vocab_rows, width = w.shape
    block = pl.BlockSpec((128, width), lambda i, t: (i, 0))
    return pl.pallas_call(
        columns_kernel,
        grid_spec=pltpu.PrefetchScalarGridSpec(
            num_scalar_prefetch=1, grid=(vocab_rows // 128,), in_specs=[block], out_specs=block
        ),
        out_shape=pltpu.HBM((vocab_rows, width), BF16),
        compiler_params=pltpu.CompilerParams(
            dimension_semantics=("arbitrary",), vmem_limit_bytes=24 << 20
        ),
        cost_estimate=pl.CostEstimate(
            flops=1024 * vocab_rows * width, bytes_accessed=4 * vocab_rows * width, transcendentals=0
        ),
    )(chips, in_hbm(w))


def rows_kernel(chips, w, tall, turned, sem):
    step = pl.program_id(0)
    size = w.shape[1]
    turned[pl.ds(pl.multiple_of(step * size, size), size)] = w[...].T

    @pl.when(step == pl.num_programs(0) - 1)
    def _():
        for g, group in enumerate(GROUPS):
            for l in range(8):
                at = l * sum(SIZES) + STARTS[g]
                for s, count, first in group:
                    src = pl.multiple_of(chips[64 * g + 8 * l + s] * 64 + first, 16)
                    pltpu.make_async_copy(
                        turned.at[pl.ds(src, count)], tall.at[pl.ds(at, count)], sem
                    ).start()
                    at += count
        pltpu.make_async_copy(tall, tall, sem).wait()


def rows_turned(chips, w):
    vocab_rows, width = w.shape
    size = width // 8
    return pl.pallas_call(
        rows_kernel,
        grid_spec=pltpu.PrefetchScalarGridSpec(
            num_scalar_prefetch=1,
            grid=(8,),
            in_specs=[pl.BlockSpec((vocab_rows, size), lambda i, t: (0, i))],
            out_specs=pl.BlockSpec(memory_space=pl.ANY),
            scratch_shapes=[pltpu.VMEM((width, vocab_rows), BF16), pltpu.SemaphoreType.DMA],
        ),
        out_shape=pltpu.HBM((width, vocab_rows), BF16),
        compiler_params=pltpu.CompilerParams(
            dimension_semantics=("arbitrary",), vmem_limit_bytes=24 << 20
        ),
        cost_estimate=pl.CostEstimate(
            flops=1024 * vocab_rows * width, bytes_accessed=4 * vocab_rows * width, transcendentals=0
        ),
    )(chips, in_hbm(w))


def half_copies(got, h):
    size = sum(SIZES)
    for l in range(4):
        for g in range(3):
            src = got[2 * g + l // 2].at[pl.ds((l % 2) * SIZES[g], SIZES[g])]
            yield src, h.at[pl.ds(l * size + STARTS[g], SIZES[g])]


def early_kernel(*refs):
    got, (w, part, h, sem) = refs[:6], refs[6:]

    @pl.when(pl.program_id(0) == 0)
    def _():
        for src, dst in half_copies(got, h):
            pltpu.make_async_copy(src, dst, sem).start()
        pltpu.make_async_copy(h, h, sem).wait()

    part[...] = jnp.dot(w[...], h[...], preferred_element_type=F32)


def late_kernel(*refs):
    got, (w, part, tgt, logits, stats, h, top, total, hit, sem) = refs[:6], refs[6:]
    step = pl.program_id(0)
    rows, tokens = logits.shape

    @pl.when(step == 0)
    def _():
        for k, (src, dst) in enumerate(half_copies(got, h)):
            pltpu.make_async_copy(src, dst, sem.at[k // 3]).start()
        top[...] = jnp.full(top.shape, -jnp.inf, F32)
        total[...] = jnp.zeros(total.shape, F32)
        hit[...] = jnp.zeros(hit.shape, F32)
        logits[...] = part[...]
        for l in range(4):
            some = pl.ds(l * sum(SIZES), sum(SIZES))
            pltpu.make_async_copy(h.at[some], h.at[some], sem.at[l]).wait()
            logits[...] += jnp.dot(w[:, some], h[some, :], preferred_element_type=F32)

    @pl.when(step > 0)
    def _():
        logits[...] = part[...] + jnp.dot(w[...], h[...], preferred_element_type=F32)

    block = logits[...]
    at = lax.broadcasted_iota(jnp.int32, block.shape, 0) + step * rows
    hit[...] += jnp.sum(jnp.where(at == tgt[...], block, F32(0.0)), axis=0, keepdims=True)
    now = jnp.maximum(top[...], jnp.max(block, axis=0, keepdims=True))
    added = jnp.sum(jnp.exp(block - now), axis=0, keepdims=True)
    total[...] = total[...] * jnp.exp(top[...] - now) + added
    top[...] = now

    @pl.when(step == pl.num_programs(0) - 1)
    def _():
        lse = top[...] + jnp.log(total[...])
        both = [r[:, k : k + 128] for r in (lse, hit[...]) for k in range(0, tokens, 128)]
        stats[...] = jnp.broadcast_to(jnp.concatenate(both, axis=0)[None], stats.shape)


LOGIT_ROWS = 256


def half_logits(half, got, wide, part=None, tgt=None):
    vocab_rows, width = wide.shape
    tokens = got[0].shape[1]
    rows, lines = LOGIT_ROWS, 2 * tokens // 128
    block = pl.BlockSpec((rows, tokens), lambda i: (i, 0))
    row = pl.BlockSpec((1, tokens), lambda i: (0, 0))
    late = part is not None
    return pl.pallas_call(
        late_kernel if late else early_kernel,
        grid=(vocab_rows // rows,),
        in_specs=[pl.BlockSpec(memory_space=pl.ANY)] * len(got)
        + [pl.BlockSpec((rows, width // 2), lambda i: (i, half))]
        + ([block, row] if late else []),
        out_specs=[block, pl.BlockSpec((64, lines, 128), lambda i: (0, 0, 0))] if late else block,
        out_shape=[
            pltpu.HBM((vocab_rows, tokens), F32), jax.ShapeDtypeStruct((64, lines, 128), F32),
        ] if late else pltpu.HBM((vocab_rows, tokens), F32),
        scratch_shapes=[pltpu.VMEM((width // 2, tokens), BF16)]
        + [pltpu.VMEM((1, tokens), F32)] * (3 if late else 0)
        + [pltpu.SemaphoreType.DMA((4,)) if late else pltpu.SemaphoreType.DMA],
        compiler_params=pltpu.CompilerParams(
            dimension_semantics=("arbitrary",), vmem_limit_bytes=32 << 20
        ),
        cost_estimate=pl.CostEstimate(
            flops=vocab_rows * width * tokens,
            bytes_accessed=width * (vocab_rows + tokens) + 4 * vocab_rows * tokens,
            transcendentals=vocab_rows * tokens,
        ),
    )(*got, in_hbm(wide), *([in_hbm(part), tgt] if late else []))


def signal_kernel(stats, logits, cot, tgt, tall, grad, loss, *refs):
    outs, (row, whole) = refs[:3], refs[3:]
    step = pl.program_id(0)
    rows, tokens = logits.shape
    lines = tokens // 128
    count = whole.shape[0] // rows

    @pl.when(step == 0)
    def _():
        lse = stats[:, :lines]
        top = jnp.max(lse, axis=0)
        full = top + jnp.log(jnp.sum(jnp.exp(lse - top[None]), axis=0))
        tok = full - jnp.sum(stats[:, lines:], axis=0)
        row[...] = jnp.concatenate([full[k : k + 1] for k in range(lines)], axis=1)
        loss[...] = jnp.concatenate([tok[k : k + 1] for k in range(lines)], axis=1)

    @pl.when(step < count)
    def _():
        block = logits[...]
        at = lax.broadcasted_iota(jnp.int32, block.shape, 0) + step * rows
        one = jnp.where(at == tgt[...], F32(1.0), F32(0.0))
        done = (cot[...] * (jnp.exp(block - row[...]) - one)).astype(BF16)
        grad[...] = done
        whole[pl.ds(pl.multiple_of(step * rows, rows), rows)] = done

    @pl.when(step >= count)
    def _():
        block = jnp.dot(tall[...], whole[...], preferred_element_type=F32).astype(BF16)
        for start, size, out in zip(STARTS, SIZES, outs):
            out[...] = block[start : start + size]


def signal_of(stats, logits, cot, tgt, tall):
    vocab_rows, tokens = logits.shape
    width = tall.shape[0]
    rows = 256
    count = vocab_rows // rows
    early = lambda i: jnp.minimum(i, count - 1)
    late = lambda i: jnp.maximum(i - count, 0)
    whole = lambda *shape: pl.BlockSpec(shape, lambda i: (0,) * len(shape))
    grad, loss, *sums = pl.pallas_call(
        signal_kernel,
        grid=(count + 4,),
        in_specs=[
            whole(*stats.shape),
            pl.BlockSpec((rows, tokens), lambda i: (early(i), 0)),
            whole(1, tokens),
            whole(1, tokens),
            pl.BlockSpec((width // 8, vocab_rows), lambda i: (4 + late(i), 0)),
        ],
        out_specs=[pl.BlockSpec((rows, tokens), lambda i: (early(i), 0)), whole(1, tokens)]
        + [pl.BlockSpec((None, size, tokens), lambda i: (late(i), 0, 0)) for size in SIZES],
        out_shape=[
            pltpu.HBM((vocab_rows, tokens), BF16),
            jax.ShapeDtypeStruct((1, tokens), F32),
        ] + [pltpu.HBM((4, size, tokens), BF16) for size in SIZES],
        scratch_shapes=[pltpu.VMEM((1, tokens), F32), pltpu.VMEM((vocab_rows, tokens), BF16)],
        compiler_params=pltpu.CompilerParams(
            dimension_semantics=("arbitrary",), vmem_limit_bytes=ALL_VMEM
        ),
        cost_estimate=pl.CostEstimate(
            flops=vocab_rows * width * tokens,
            bytes_accessed=6 * vocab_rows * tokens + width * (vocab_rows + tokens),
            transcendentals=vocab_rows * tokens,
        ),
    )(stats, in_hbm(logits), cot, tgt, in_hbm(tall))
    return grad, loss, sums


def grad_kernel(tall, grad, *outs):
    block = jnp.dot(tall[...], grad[...], preferred_element_type=F32).astype(BF16)
    for start, size, out in zip(STARTS, SIZES, outs):
        out[...] = block[start : start + size]


def half_grads(half, tall, grad):
    vocab_rows, tokens = grad.shape
    width = tall.shape[0]
    return pl.pallas_call(
        grad_kernel,
        grid=(4,),
        in_specs=[
            pl.BlockSpec((width // 8, vocab_rows), lambda i: (4 * half + i, 0)),
            pl.BlockSpec((vocab_rows, tokens), lambda i: (0, 0)),
        ],
        out_specs=[pl.BlockSpec((None, size, tokens), lambda i: (i, 0, 0)) for size in SIZES],
        out_shape=[pltpu.HBM((4, size, tokens), BF16) for size in SIZES],
        compiler_params=pltpu.CompilerParams(
            dimension_semantics=("arbitrary",), vmem_limit_bytes=ALL_VMEM
        ),
        cost_estimate=pl.CostEstimate(
            flops=vocab_rows * width * tokens, bytes_accessed=width * (vocab_rows + tokens),
            transcendentals=0,
        ),
    )(in_hbm(tall), grad)


def body(hidden, head_weight, targets, loss_cot):
    vocab_rows, _ = head_weight.shape
    own = hidden.T
    feats, tokens = own.shape
    core = lax.axis_index("dp")
    chips = lax.dynamic_index_in_dim(jnp.asarray(CHIPS), lax.axis_index(ALL), 0, keepdims=False)
    tgt = (targets - lax.axis_index(VOCAB) * vocab_rows)[None, :]
    some = small_stage(jnp.broadcast_to(own[None], (8, feats, tokens)))
    wide = columns_turned(chips, head_weight)
    got = gathered_groups(some.reshape(8 * feats, tokens))
    part = half_logits(0, [a for group in got for a in group[:2]], wide)
    logits, stats = half_logits(1, [a for group in got for a in group[2:]], wide, part, tgt)
    stats = lax.all_to_all(stats, VOCAB, 0, 0, tiled=True)
    tall = rows_turned(chips, head_weight)
    a_part = a_part_of(chips, [a for group in got for a in group], own)
    grad, tok_loss, sends = signal_of(stats, logits, loss_cot[None, :], tgt, tall)
    sums = summed_groups(sends, half_grads(0, tall, grad))
    sums = small_stage(sums.reshape(8, feats, tokens))
    hidden_grad = summed(sums).T
    rows = vocab_rows // 2

    def gram(x):
        mine = lax.dynamic_slice_in_dim(x, core * rows, rows, 0)
        return lax.dot_general(mine, x, (((1,), (1,)), ((), ())), preferred_element_type=F32)

    g_factor = (gram(grad) + gram(lax.ppermute(grad, "dp", SWAP))) / TOK_DEV
    a_factor = (a_part + lax.ppermute(a_part, "dp", SWAP)) / TOK_DEV
    return (tok_loss[0], hidden_grad, g_factor, a_factor)


def solution(mesh):
    finer = Mesh(mesh.devices.reshape(4, 4, 4, mesh.shape["dp"]), ALL)
    return jax.shard_map(
        body,
        mesh=finer,
        in_specs=(P("dp", VOCAB), P(VOCAB, None), P("dp"), P("dp")),
        out_specs=(P("dp"), P("dp", VOCAB), P(ALL, None), P(VOCAB, None)),
        check_vma=False,
    )
```

```python
import jax
import jax.numpy as jnp
import numpy as np
from jax import lax
from jax.experimental import pallas as pl
from jax.experimental.pallas import tpu as pltpu
from jax.sharding import Mesh
from jax.sharding import PartitionSpec as P

TOK_DEV = 1024
VOCAB = ("vocab_0", "vocab_1", "vocab_2")
ALL = ("vocab_0", "vocab_1", "vocab_2", "dp")
ALL_VMEM = (64 << 20) - (256 << 10)

SMALL = (((0, 1), (2, 3)), ((0, 3), (1, 2)))
LARGE = (((1, 2), (0, 3)), ((0, 1), (3, 2)))
SWAP = [(0, 1), (1, 0)]
F32 = jnp.float32
BF16 = jnp.bfloat16

GROUPS = (
    ((0, 64, 0), (1, 64, 0), (2, 48, 0)),
    ((2, 16, 48), (3, 64, 0), (4, 64, 0), (5, 32, 0)),
    ((5, 32, 32), (6, 64, 0), (7, 64, 0)),
)
SIZES = [sum(rows for _, rows, _ in group) for group in GROUPS]
STARTS = [0, SIZES[0], SIZES[0] + SIZES[1]]


def device(y, z, x, core):
    return ((y * 4 + z) * 4 + x) * 2 + core


def small_cubes():
    return [
        [device(y, z, x, core) for y in a for z in b for x in c]
        for core in (0, 1) for a in SMALL[core] for b in SMALL[core] for c in SMALL[core]
    ]


def partner(core, c):
    return next(p[1 - p.index(c)] for p in LARGE[core] if c in p)


def spots():
    return [(y, z, x, core) for y in range(4) for z in range(4) for x in range(4) for core in (0, 1)]


def large_pairs(axis):
    out = []
    for at in spots():
        to = list(at)
        to[axis] = partner(at[3], at[axis])
        out.append((device(*at), device(*to)))
    return out


def chip_table():
    table = np.zeros((128, 3, 8, 8), np.int32)
    for at in spots():
        core = at[3]
        for group in range(3):
            for l in range(8):
                for s in range(8):
                    chip = 0
                    for axis in range(3):
                        c = at[axis]
                        if l >> ((axis - group) % 3) & 1:
                            c = partner(core, c)
                        pair = next(p for p in SMALL[core] if c in p)
                        chip = chip * 4 + pair[s >> (2 - axis) & 1]
                    table[device(*at), group, l, s] = chip
    return table.reshape(128, 192)


SMALL_CUBES = small_cubes()
LARGE_PAIRS = [large_pairs(axis) for axis in range(3)]
CHIPS = chip_table()


def small_stage(x):
    return lax.all_to_all(x, ALL, 0, 0, axis_index_groups=SMALL_CUBES, tiled=True)


def in_hbm(x):
    return pltpu.with_memory_space_constraint(x, pltpu.HBM)


def gathered_groups(some):
    def get(x, g, step):
        return lax.ppermute(x, ALL, LARGE_PAIRS[(g + step) % 3])

    held = [some[start : start + size] for start, size in zip(STARTS, SIZES)]
    got = [get(held[g], g, 0) for g in range(3)]
    first = [jnp.concatenate([h, r]) for h, r in zip(held, got)]
    second = [get(first[g], g, 1) for g in range(3)]
    third = [get(first[g], g, 2) for g in range(3)]
    fourth = [get(second[g], g, 2) for g in range(3)]
    return [[first[g], second[g], third[g], fourth[g]] for g in range(3)]


def add_kernel(*refs):
    *terms, out = refs
    total = terms[0][...].astype(F32)
    for term in terms[1:]:
        total = total + term[...].astype(F32)
    out[...] = total.astype(BF16)


def add_up(count, *terms):
    _, rows, tokens = terms[0][0].shape
    block = lambda first: pl.BlockSpec((None, rows, tokens), lambda i: (first + i, 0, 0))
    return pl.pallas_call(
        add_kernel,
        grid=(count,),
        in_specs=[block(first) for _, first in terms],
        out_specs=block(0),
        out_shape=jax.ShapeDtypeStruct((count, rows, tokens), BF16),
        compiler_params=pltpu.CompilerParams(
            dimension_semantics=("arbitrary",), vmem_limit_bytes=12 << 20
        ),
        cost_estimate=pl.CostEstimate(
            flops=len(terms) * count * rows * tokens,
            bytes_accessed=2 * (len(terms) + 1) * count * rows * tokens, transcendentals=0,
        ),
    )(*[in_hbm(x) if x.shape[0] == 4 else x for x, _ in terms])


def last_kernel(*refs):
    *terms, out = refs
    for g in range(3):
        total = terms[4 * g][...].astype(F32)
        for term in terms[4 * g + 1 : 4 * g + 4]:
            total = total + term[...].astype(F32)
        out[STARTS[g] : STARTS[g] + SIZES[g]] = total.astype(BF16)


def add_last(terms):
    tokens = terms[0].shape[2]
    part = tokens // 2
    return pl.pallas_call(
        last_kernel,
        grid=(2,),
        in_specs=[
            pl.BlockSpec((None, x.shape[1], part), lambda i: (0, 0, i)) for x in terms
        ],
        out_specs=pl.BlockSpec((sum(SIZES), part), lambda i: (0, i)),
        out_shape=jax.ShapeDtypeStruct((sum(SIZES), tokens), BF16),
        compiler_params=pltpu.CompilerParams(
            dimension_semantics=("arbitrary",), vmem_limit_bytes=16 << 20
        ),
        cost_estimate=pl.CostEstimate(
            flops=4 * sum(SIZES) * tokens, bytes_accessed=10 * sum(SIZES) * tokens, transcendentals=0
        ),
    )(*[in_hbm(x) if x.shape[0] == 4 else x for x in terms])


def summed_groups(sends, keeps):
    def trade(x, g, step):
        return lax.ppermute(x, ALL, LARGE_PAIRS[(g + step) % 3])

    far = [trade(sends[g], g, 2) for g in range(3)]
    mid = [trade(add_up(2, (keeps[g], 2), (far[g], 2)), g, 1) for g in range(3)]
    near = [
        trade(add_up(1, (keeps[g], 1), (far[g], 1), (mid[g], 1)), g, 0) for g in range(3)
    ]
    return add_last([x for g in range(3) for x in (keeps[g], far[g], mid[g], near[g])])


def sum_kernel(pieces, out):
    out[...] = jnp.sum(pieces[...].astype(F32), axis=0).astype(BF16)


def summed(pieces):
    count, rows, tokens = pieces.shape
    return pl.pallas_call(
        sum_kernel,
        grid=(2,),
        in_specs=[pl.BlockSpec((count, rows, tokens // 2), lambda i: (0, 0, i))],
        out_specs=pl.BlockSpec((rows, tokens // 2), lambda i: (0, i)),
        out_shape=jax.ShapeDtypeStruct((rows, tokens), BF16),
        compiler_params=pltpu.CompilerParams(
            dimension_semantics=("arbitrary",), vmem_limit_bytes=8 << 20
        ),
    )(pieces)


def gather_copies(chips, got, h):
    quarters = []
    for large in (0, 1):
        for small in (0, 1):
            copies = []
            for g, group in enumerate(GROUPS):
                for l in range(8):
                    if l >> (-g % 3) & 1 != large:
                        continue
                    src, at = got[4 * g + l // 2], (l % 2) * SIZES[g]
                    for s, count, first in group:
                        if s >> 2 == small:
                            dst = pl.multiple_of(chips[64 * g + 8 * l + s] * 64 + first, 16)
                            copies.append((src.at[pl.ds(at, count)], h.at[pl.ds(dst, count)]))
                        at += count
            quarters.append((chips[8 * large + 4 * small] // 16, copies))
    return quarters


def a_kernel(chips, *refs):
    got, (own, out, h, sem) = refs[:12], refs[12:]
    quarter = h.shape[0] // 4
    quarters = gather_copies(chips, got, h)
    for q, (_, copies) in enumerate(quarters):
        for src, dst in copies:
            pltpu.make_async_copy(src, dst, sem.at[q]).start()
    for q, (y, _) in enumerate(quarters):
        some = h.at[pl.ds(0, quarter)]
        pltpu.make_async_copy(some, some, sem.at[q]).wait()
        here = pl.ds(pl.multiple_of(y * quarter, quarter), quarter)
        out[:, here] = lax.dot_general(
            own[...], h[here, :], (((1,), (1,)), ((), ())), preferred_element_type=F32
        )


def a_part_of(chips, got, own):
    feats, tokens = own.shape
    width = 64 * feats
    return pl.pallas_call(
        a_kernel,
        grid_spec=pltpu.PrefetchScalarGridSpec(
            num_scalar_prefetch=1,
            grid=(),
            in_specs=[pl.BlockSpec(memory_space=pltpu.HBM)] * len(got)
            + [pl.BlockSpec(memory_space=pltpu.VMEM)],
            out_specs=pl.BlockSpec(memory_space=pltpu.VMEM),
            scratch_shapes=[pltpu.VMEM((width, tokens), BF16), pltpu.SemaphoreType.DMA((4,))],
        ),
        out_shape=jax.ShapeDtypeStruct((feats, width), F32),
        compiler_params=pltpu.CompilerParams(vmem_limit_bytes=ALL_VMEM),
        cost_estimate=pl.CostEstimate(
            flops=2 * feats * width * tokens, bytes_accessed=2 * width * tokens, transcendentals=0
        ),
    )(chips, *[in_hbm(x) for x in got], own)


def columns_kernel(chips, w, wide):
    rows = w.shape[0]
    lane = lax.broadcasted_iota(jnp.int32, (rows, 128), 1)
    for l in range(8):
        for tile in range(4):
            done = None
            for g, group in enumerate(GROUPS):
                for s, count, first in group:
                    if s // 2 != tile:
                        continue
                    chip, side = chips[64 * g + 8 * l + s], s % 2
                    block = w[:, pl.ds(pl.multiple_of(chip // 2 * 128, 128), 128)]
                    block = pltpu.roll(block, 64 * (chip % 2 != side).astype(jnp.int32), 1)
                    done = block if done is None else jnp.where(
                        lane >= 64 * side + first, block, done
                    )
            wide[:, (4 * l + tile) * 128 : (4 * l + tile + 1) * 128] = done


def columns_turned(chips, w):
    vocab_rows, width = w.shape
    block = pl.BlockSpec((128, width), lambda i, t: (i, 0))
    return pl.pallas_call(
        columns_kernel,
        grid_spec=pltpu.PrefetchScalarGridSpec(
            num_scalar_prefetch=1, grid=(vocab_rows // 128,), in_specs=[block], out_specs=block
        ),
        out_shape=pltpu.HBM((vocab_rows, width), BF16),
        compiler_params=pltpu.CompilerParams(
            dimension_semantics=("arbitrary",), vmem_limit_bytes=24 << 20
        ),
        cost_estimate=pl.CostEstimate(
            flops=1024 * vocab_rows * width, bytes_accessed=4 * vocab_rows * width, transcendentals=0
        ),
    )(chips, in_hbm(w))


def rows_kernel(chips, w, tall, turned, sem):
    step = pl.program_id(0)
    size = w.shape[1]
    turned[pl.ds(pl.multiple_of(step * size, size), size)] = w[...].T

    @pl.when(step == pl.num_programs(0) - 1)
    def _():
        for g, group in enumerate(GROUPS):
            for l in range(8):
                at = l * sum(SIZES) + STARTS[g]
                for s, count, first in group:
                    src = pl.multiple_of(chips[64 * g + 8 * l + s] * 64 + first, 16)
                    pltpu.make_async_copy(
                        turned.at[pl.ds(src, count)], tall.at[pl.ds(at, count)], sem
                    ).start()
                    at += count
        pltpu.make_async_copy(tall, tall, sem).wait()


def rows_turned(chips, w):
    vocab_rows, width = w.shape
    size = width // 8
    return pl.pallas_call(
        rows_kernel,
        grid_spec=pltpu.PrefetchScalarGridSpec(
            num_scalar_prefetch=1,
            grid=(8,),
            in_specs=[pl.BlockSpec((vocab_rows, size), lambda i, t: (0, i))],
            out_specs=pl.BlockSpec(memory_space=pl.ANY),
            scratch_shapes=[pltpu.VMEM((width, vocab_rows), BF16), pltpu.SemaphoreType.DMA],
        ),
        out_shape=pltpu.HBM((width, vocab_rows), BF16),
        compiler_params=pltpu.CompilerParams(
            dimension_semantics=("arbitrary",), vmem_limit_bytes=24 << 20
        ),
        cost_estimate=pl.CostEstimate(
            flops=1024 * vocab_rows * width, bytes_accessed=4 * vocab_rows * width, transcendentals=0
        ),
    )(chips, in_hbm(w))


def half_copies(got, h):
    size = sum(SIZES)
    for l in range(4):
        for g in range(3):
            src = got[2 * g + l // 2].at[pl.ds((l % 2) * SIZES[g], SIZES[g])]
            yield src, h.at[pl.ds(l * size + STARTS[g], SIZES[g])]


def early_kernel(*refs):
    got, (w, part, h, sem) = refs[:6], refs[6:]

    @pl.when(pl.program_id(0) == 0)
    def _():
        for src, dst in half_copies(got, h):
            pltpu.make_async_copy(src, dst, sem).start()
        pltpu.make_async_copy(h, h, sem).wait()

    part[...] = jnp.dot(w[...], h[...], preferred_element_type=F32)


def late_kernel(*refs):
    got, (w, part, tgt, logits, stats, h, top, total, hit, sem) = refs[:6], refs[6:]
    step = pl.program_id(0)
    rows, tokens = logits.shape

    @pl.when(step == 0)
    def _():
        for k, (src, dst) in enumerate(half_copies(got, h)):
            pltpu.make_async_copy(src, dst, sem.at[k // 3]).start()
        top[...] = jnp.full(top.shape, -jnp.inf, F32)
        total[...] = jnp.zeros(total.shape, F32)
        hit[...] = jnp.zeros(hit.shape, F32)
        logits[...] = part[...]
        for l in range(4):
            some = pl.ds(l * sum(SIZES), sum(SIZES))
            pltpu.make_async_copy(h.at[some], h.at[some], sem.at[l]).wait()
            logits[...] += jnp.dot(w[:, some], h[some, :], preferred_element_type=F32)

    @pl.when(step > 0)
    def _():
        logits[...] = part[...] + jnp.dot(w[...], h[...], preferred_element_type=F32)

    block = logits[...]
    at = lax.broadcasted_iota(jnp.int32, block.shape, 0) + step * rows
    hit[...] += jnp.sum(jnp.where(at == tgt[...], block, F32(0.0)), axis=0, keepdims=True)
    now = jnp.maximum(top[...], jnp.max(block, axis=0, keepdims=True))
    added = jnp.sum(jnp.exp(block - now), axis=0, keepdims=True)
    total[...] = total[...] * jnp.exp(top[...] - now) + added
    top[...] = now

    @pl.when(step == pl.num_programs(0) - 1)
    def _():
        lse = top[...] + jnp.log(total[...])
        both = [r[:, k : k + 128] for r in (lse, hit[...]) for k in range(0, tokens, 128)]
        stats[...] = jnp.broadcast_to(jnp.concatenate(both, axis=0)[None], stats.shape)


LOGIT_ROWS = 256


def half_logits(half, got, wide, part=None, tgt=None):
    vocab_rows, width = wide.shape
    tokens = got[0].shape[1]
    rows, lines = LOGIT_ROWS, 2 * tokens // 128
    block = pl.BlockSpec((rows, tokens), lambda i: (i, 0))
    row = pl.BlockSpec((1, tokens), lambda i: (0, 0))
    late = part is not None
    return pl.pallas_call(
        late_kernel if late else early_kernel,
        grid=(vocab_rows // rows,),
        in_specs=[pl.BlockSpec(memory_space=pl.ANY)] * len(got)
        + [pl.BlockSpec((rows, width // 2), lambda i: (i, half))]
        + ([block, row] if late else []),
        out_specs=[block, pl.BlockSpec((64, lines, 128), lambda i: (0, 0, 0))] if late else block,
        out_shape=[
            pltpu.HBM((vocab_rows, tokens), F32), jax.ShapeDtypeStruct((64, lines, 128), F32),
        ] if late else jax.ShapeDtypeStruct((vocab_rows, tokens), F32),
        scratch_shapes=[pltpu.VMEM((width // 2, tokens), BF16)]
        + [pltpu.VMEM((1, tokens), F32)] * (3 if late else 0)
        + [pltpu.SemaphoreType.DMA((4,)) if late else pltpu.SemaphoreType.DMA],
        compiler_params=pltpu.CompilerParams(
            dimension_semantics=("arbitrary",), vmem_limit_bytes=32 << 20
        ),
        cost_estimate=pl.CostEstimate(
            flops=vocab_rows * width * tokens,
            bytes_accessed=width * (vocab_rows + tokens) + 4 * vocab_rows * tokens,
            transcendentals=vocab_rows * tokens,
        ),
    )(*got, in_hbm(wide), *([part, tgt] if late else []))


def signal_kernel(stats, logits, cot, tgt, tall, grad, loss, *refs):
    outs, (row, whole) = refs[:3], refs[3:]
    step = pl.program_id(0)
    rows, tokens = logits.shape
    lines = tokens // 128
    count = whole.shape[0] // rows

    @pl.when(step == 0)
    def _():
        lse = stats[:, :lines]
        top = jnp.max(lse, axis=0)
        full = top + jnp.log(jnp.sum(jnp.exp(lse - top[None]), axis=0))
        tok = full - jnp.sum(stats[:, lines:], axis=0)
        row[...] = jnp.concatenate([full[k : k + 1] for k in range(lines)], axis=1)
        loss[...] = jnp.concatenate([tok[k : k + 1] for k in range(lines)], axis=1)

    @pl.when(step < count)
    def _():
        block = logits[...]
        at = lax.broadcasted_iota(jnp.int32, block.shape, 0) + step * rows
        one = jnp.where(at == tgt[...], F32(1.0), F32(0.0))
        done = (cot[...] * (jnp.exp(block - row[...]) - one)).astype(BF16)
        grad[...] = done
        whole[pl.ds(pl.multiple_of(step * rows, rows), rows)] = done

    @pl.when(step >= count)
    def _():
        block = jnp.dot(tall[...], whole[...], preferred_element_type=F32).astype(BF16)
        for start, size, out in zip(STARTS, SIZES, outs):
            out[...] = block[start : start + size]


def signal_of(stats, logits, cot, tgt, tall):
    vocab_rows, tokens = logits.shape
    width = tall.shape[0]
    rows = 256
    count = vocab_rows // rows
    early = lambda i: jnp.minimum(i, count - 1)
    late = lambda i: jnp.maximum(i - count, 0)
    whole = lambda *shape: pl.BlockSpec(shape, lambda i: (0,) * len(shape))
    grad, loss, *sums = pl.pallas_call(
        signal_kernel,
        grid=(count + 4,),
        in_specs=[
            whole(*stats.shape),
            pl.BlockSpec((rows, tokens), lambda i: (early(i), 0)),
            whole(1, tokens),
            whole(1, tokens),
            pl.BlockSpec((width // 8, vocab_rows), lambda i: (4 + late(i), 0)),
        ],
        out_specs=[pl.BlockSpec((rows, tokens), lambda i: (early(i), 0)), whole(1, tokens)]
        + [pl.BlockSpec((None, size, tokens), lambda i: (late(i), 0, 0)) for size in SIZES],
        out_shape=[
            pltpu.HBM((vocab_rows, tokens), BF16),
            jax.ShapeDtypeStruct((1, tokens), F32),
        ] + [pltpu.HBM((4, size, tokens), BF16) for size in SIZES],
        scratch_shapes=[pltpu.VMEM((1, tokens), F32), pltpu.VMEM((vocab_rows, tokens), BF16)],
        compiler_params=pltpu.CompilerParams(
            dimension_semantics=("arbitrary",), vmem_limit_bytes=ALL_VMEM
        ),
        cost_estimate=pl.CostEstimate(
            flops=vocab_rows * width * tokens,
            bytes_accessed=6 * vocab_rows * tokens + width * (vocab_rows + tokens),
            transcendentals=vocab_rows * tokens,
        ),
    )(stats, in_hbm(logits), cot, tgt, in_hbm(tall))
    return grad, loss, sums


def grad_kernel(tall, grad, *outs):
    block = jnp.dot(tall[...], grad[...], preferred_element_type=F32).astype(BF16)
    for start, size, out in zip(STARTS, SIZES, outs):
        out[...] = block[start : start + size]


def half_grads(half, tall, grad):
    vocab_rows, tokens = grad.shape
    width = tall.shape[0]
    return pl.pallas_call(
        grad_kernel,
        grid=(4,),
        in_specs=[
            pl.BlockSpec((width // 8, vocab_rows), lambda i: (4 * half + i, 0)),
            pl.BlockSpec((vocab_rows, tokens), lambda i: (0, 0)),
        ],
        out_specs=[pl.BlockSpec((None, size, tokens), lambda i: (i, 0, 0)) for size in SIZES],
        out_shape=[pltpu.HBM((4, size, tokens), BF16) for size in SIZES],
        compiler_params=pltpu.CompilerParams(
            dimension_semantics=("arbitrary",), vmem_limit_bytes=ALL_VMEM
        ),
        cost_estimate=pl.CostEstimate(
            flops=vocab_rows * width * tokens, bytes_accessed=width * (vocab_rows + tokens),
            transcendentals=0,
        ),
    )(in_hbm(tall), grad)


def body(hidden, head_weight, targets, loss_cot):
    vocab_rows, _ = head_weight.shape
    own = hidden.T
    feats, tokens = own.shape
    core = lax.axis_index("dp")
    chips = lax.dynamic_index_in_dim(jnp.asarray(CHIPS), lax.axis_index(ALL), 0, keepdims=False)
    tgt = (targets - lax.axis_index(VOCAB) * vocab_rows)[None, :]
    some = small_stage(jnp.broadcast_to(own[None], (8, feats, tokens)))
    wide = columns_turned(chips, head_weight)
    got = gathered_groups(some.reshape(8 * feats, tokens))
    part = half_logits(0, [a for group in got for a in group[:2]], wide)
    logits, stats = half_logits(1, [a for group in got for a in group[2:]], wide, part, tgt)
    stats = lax.all_to_all(stats, VOCAB, 0, 0, tiled=True)
    tall = rows_turned(chips, head_weight)
    a_part = a_part_of(chips, [a for group in got for a in group], own)
    grad, tok_loss, sends = signal_of(stats, logits, loss_cot[None, :], tgt, tall)
    sums = summed_groups(sends, half_grads(0, tall, grad))
    sums = small_stage(sums.reshape(8, feats, tokens))
    hidden_grad = summed(sums).T
    rows = vocab_rows // 2

    def gram(x):
        mine = lax.dynamic_slice_in_dim(x, core * rows, rows, 0)
        return lax.dot_general(mine, x, (((1,), (1,)), ((), ())), preferred_element_type=F32)

    g_factor = (gram(grad) + gram(lax.ppermute(grad, "dp", SWAP))) / TOK_DEV
    a_factor = (a_part + lax.ppermute(a_part, "dp", SWAP)) / TOK_DEV
    return (tok_loss[0], hidden_grad, g_factor, a_factor)


def solution(mesh):
    finer = Mesh(mesh.devices.reshape(4, 4, 4, mesh.shape["dp"]), ALL)
    return jax.shard_map(
        body,
        mesh=finer,
        in_specs=(P("dp", VOCAB), P(VOCAB, None), P("dp"), P("dp")),
        out_specs=(P("dp"), P("dp", VOCAB), P(ALL, None), P(VOCAB, None)),
        check_vma=False,
    )
```

```python
import jax
import jax.numpy as jnp
import numpy as np
from jax import lax
from jax.experimental import pallas as pl
from jax.experimental.pallas import tpu as pltpu
from jax.sharding import Mesh
from jax.sharding import PartitionSpec as P

TOK_DEV = 1024
VOCAB = ("vocab_0", "vocab_1", "vocab_2")
ALL = ("vocab_0", "vocab_1", "vocab_2", "dp")
ALL_VMEM = (64 << 20) - (256 << 10)

SMALL = (((0, 1), (2, 3)), ((0, 3), (1, 2)))
LARGE = (((1, 2), (0, 3)), ((0, 1), (3, 2)))
SWAP = [(0, 1), (1, 0)]
F32 = jnp.float32
BF16 = jnp.bfloat16

GROUPS = (
    ((0, 64, 0), (1, 64, 0), (2, 48, 0)),
    ((2, 16, 48), (3, 64, 0), (4, 64, 0), (5, 32, 0)),
    ((5, 32, 32), (6, 64, 0), (7, 64, 0)),
)
SIZES = [sum(rows for _, rows, _ in group) for group in GROUPS]
STARTS = [0, SIZES[0], SIZES[0] + SIZES[1]]


def device(y, z, x, core):
    return ((y * 4 + z) * 4 + x) * 2 + core


def small_cubes():
    return [
        [device(y, z, x, core) for y in a for z in b for x in c]
        for core in (0, 1) for a in SMALL[core] for b in SMALL[core] for c in SMALL[core]
    ]


def partner(core, c):
    return next(p[1 - p.index(c)] for p in LARGE[core] if c in p)


def spots():
    return [(y, z, x, core) for y in range(4) for z in range(4) for x in range(4) for core in (0, 1)]


def large_pairs(axis):
    out = []
    for at in spots():
        to = list(at)
        to[axis] = partner(at[3], at[axis])
        out.append((device(*at), device(*to)))
    return out


def chip_table():
    table = np.zeros((128, 3, 8, 8), np.int32)
    for at in spots():
        core = at[3]
        for group in range(3):
            for l in range(8):
                for s in range(8):
                    chip = 0
                    for axis in range(3):
                        c = at[axis]
                        if l >> ((axis - group) % 3) & 1:
                            c = partner(core, c)
                        pair = next(p for p in SMALL[core] if c in p)
                        chip = chip * 4 + pair[s >> (2 - axis) & 1]
                    table[device(*at), group, l, s] = chip
    return table.reshape(128, 192)


SMALL_CUBES = small_cubes()
LARGE_PAIRS = [large_pairs(axis) for axis in range(3)]
CHIPS = chip_table()


def small_stage(x):
    return lax.all_to_all(x, ALL, 0, 0, axis_index_groups=SMALL_CUBES, tiled=True)


def in_hbm(x):
    return pltpu.with_memory_space_constraint(x, pltpu.HBM)


def gathered_groups(some):
    def get(x, g, step):
        return lax.ppermute(x, ALL, LARGE_PAIRS[(g + step) % 3])

    held = [some[start : start + size] for start, size in zip(STARTS, SIZES)]
    got = [get(held[g], g, 0) for g in range(3)]
    first = [jnp.concatenate([h, r]) for h, r in zip(held, got)]
    second = [get(first[g], g, 1) for g in range(3)]
    third = [get(first[g], g, 2) for g in range(3)]
    fourth = [get(second[g], g, 2) for g in range(3)]
    return [[first[g], second[g], third[g], fourth[g]] for g in range(3)]


def add_kernel(*refs):
    *terms, out = refs
    total = terms[0][...].astype(F32)
    for term in terms[1:]:
        total = total + term[...].astype(F32)
    out[...] = total.astype(BF16)


def add_up(count, *terms):
    _, rows, tokens = terms[0][0].shape
    block = lambda first: pl.BlockSpec((None, rows, tokens), lambda i: (first + i, 0, 0))
    return pl.pallas_call(
        add_kernel,
        grid=(count,),
        in_specs=[block(first) for _, first in terms],
        out_specs=block(0),
        out_shape=jax.ShapeDtypeStruct((count, rows, tokens), BF16),
        compiler_params=pltpu.CompilerParams(
            dimension_semantics=("arbitrary",), vmem_limit_bytes=12 << 20
        ),
        cost_estimate=pl.CostEstimate(
            flops=len(terms) * count * rows * tokens,
            bytes_accessed=2 * (len(terms) + 1) * count * rows * tokens, transcendentals=0,
        ),
    )(*[in_hbm(x) if x.shape[0] == 4 else x for x, _ in terms])


def early_sum_kernel(*refs):
    *terms, out = refs
    for g in range(3):
        total = terms[3 * g][...].astype(F32)
        for term in terms[3 * g + 1 : 3 * g + 3]:
            total = total + term[...].astype(F32)
        out[STARTS[g] : STARTS[g] + SIZES[g]] = total


def last_sum_kernel(*refs):
    *terms, early, out = refs
    for g in range(3):
        here = slice(STARTS[g], STARTS[g] + SIZES[g])
        out[here] = (early[here] + terms[g][...].astype(F32)).astype(BF16)


def stacked_sum(kernel, terms, kind, *more):
    tokens = terms[0].shape[2]
    part = tokens // 2
    rows = pl.BlockSpec((sum(SIZES), part), lambda i: (0, i))
    return pl.pallas_call(
        kernel,
        grid=(2,),
        in_specs=[pl.BlockSpec((None, x.shape[1], part), lambda i: (0, 0, i)) for x in terms]
        + [rows] * len(more),
        out_specs=rows,
        out_shape=jax.ShapeDtypeStruct((sum(SIZES), tokens), kind),
        compiler_params=pltpu.CompilerParams(
            dimension_semantics=("arbitrary",), vmem_limit_bytes=16 << 20
        ),
        cost_estimate=pl.CostEstimate(
            flops=4 * sum(SIZES) * tokens, bytes_accessed=10 * sum(SIZES) * tokens, transcendentals=0
        ),
    )(*[in_hbm(x) if x.shape[0] == 4 else x for x in terms], *more)


def summed_groups(sends, keeps):
    def trade(x, g, step):
        return lax.ppermute(x, ALL, LARGE_PAIRS[(g + step) % 3])

    far = [trade(sends[g], g, 2) for g in range(3)]
    mid = [trade(add_up(2, (keeps[g], 2), (far[g], 2)), g, 1) for g in range(3)]
    near = [
        trade(add_up(1, (keeps[g], 1), (far[g], 1), (mid[g], 1)), g, 0) for g in range(3)
    ]
    early = stacked_sum(
        early_sum_kernel, [x for g in range(3) for x in (keeps[g], far[g], mid[g])], F32
    )
    return stacked_sum(last_sum_kernel, near, BF16, early)


def sum_kernel(pieces, out):
    out[...] = jnp.sum(pieces[...].astype(F32), axis=0).astype(BF16)


def summed(pieces):
    count, rows, tokens = pieces.shape
    return pl.pallas_call(
        sum_kernel,
        grid=(2,),
        in_specs=[pl.BlockSpec((count, rows, tokens // 2), lambda i: (0, 0, i))],
        out_specs=pl.BlockSpec((rows, tokens // 2), lambda i: (0, i)),
        out_shape=jax.ShapeDtypeStruct((rows, tokens), BF16),
        compiler_params=pltpu.CompilerParams(
            dimension_semantics=("arbitrary",), vmem_limit_bytes=8 << 20
        ),
    )(pieces)


def gather_copies(chips, got, h):
    quarters = []
    for large in (0, 1):
        for small in (0, 1):
            copies = []
            for g, group in enumerate(GROUPS):
                for l in range(8):
                    if l >> (-g % 3) & 1 != large:
                        continue
                    src, at = got[4 * g + l // 2], (l % 2) * SIZES[g]
                    for s, count, first in group:
                        if s >> 2 == small:
                            dst = pl.multiple_of(chips[64 * g + 8 * l + s] * 64 + first, 16)
                            copies.append((src.at[pl.ds(at, count)], h.at[pl.ds(dst, count)]))
                        at += count
            quarters.append((chips[8 * large + 4 * small] // 16, copies))
    return quarters


def a_kernel(chips, *refs):
    got, (own, out, h, sem) = refs[:12], refs[12:]
    quarter = h.shape[0] // 4
    quarters = gather_copies(chips, got, h)
    for q, (_, copies) in enumerate(quarters):
        for src, dst in copies:
            pltpu.make_async_copy(src, dst, sem.at[q]).start()
    for q, (y, _) in enumerate(quarters):
        some = h.at[pl.ds(0, quarter)]
        pltpu.make_async_copy(some, some, sem.at[q]).wait()
        here = pl.ds(pl.multiple_of(y * quarter, quarter), quarter)
        out[:, here] = lax.dot_general(
            own[...], h[here, :], (((1,), (1,)), ((), ())), preferred_element_type=F32
        )


def a_part_of(chips, got, own):
    feats, tokens = own.shape
    width = 64 * feats
    return pl.pallas_call(
        a_kernel,
        grid_spec=pltpu.PrefetchScalarGridSpec(
            num_scalar_prefetch=1,
            grid=(),
            in_specs=[pl.BlockSpec(memory_space=pltpu.HBM)] * len(got)
            + [pl.BlockSpec(memory_space=pltpu.VMEM)],
            out_specs=pl.BlockSpec(memory_space=pltpu.VMEM),
            scratch_shapes=[pltpu.VMEM((width, tokens), BF16), pltpu.SemaphoreType.DMA((4,))],
        ),
        out_shape=jax.ShapeDtypeStruct((feats, width), F32),
        compiler_params=pltpu.CompilerParams(vmem_limit_bytes=ALL_VMEM),
        cost_estimate=pl.CostEstimate(
            flops=2 * feats * width * tokens, bytes_accessed=2 * width * tokens, transcendentals=0
        ),
    )(chips, *[in_hbm(x) for x in got], own)


def columns_kernel(chips, w, wide):
    rows = w.shape[0]
    lane = lax.broadcasted_iota(jnp.int32, (rows, 128), 1)
    for l in range(8):
        for tile in range(4):
            done = None
            for g, group in enumerate(GROUPS):
                for s, count, first in group:
                    if s // 2 != tile:
                        continue
                    chip, side = chips[64 * g + 8 * l + s], s % 2
                    block = w[:, pl.ds(pl.multiple_of(chip // 2 * 128, 128), 128)]
                    block = pltpu.roll(block, 64 * (chip % 2 != side).astype(jnp.int32), 1)
                    done = block if done is None else jnp.where(
                        lane >= 64 * side + first, block, done
                    )
            wide[:, (4 * l + tile) * 128 : (4 * l + tile + 1) * 128] = done


def columns_turned(chips, w):
    vocab_rows, width = w.shape
    block = pl.BlockSpec((128, width), lambda i, t: (i, 0))
    return pl.pallas_call(
        columns_kernel,
        grid_spec=pltpu.PrefetchScalarGridSpec(
            num_scalar_prefetch=1, grid=(vocab_rows // 128,), in_specs=[block], out_specs=block
        ),
        out_shape=pltpu.HBM((vocab_rows, width), BF16),
        compiler_params=pltpu.CompilerParams(
            dimension_semantics=("arbitrary",), vmem_limit_bytes=24 << 20
        ),
        cost_estimate=pl.CostEstimate(
            flops=1024 * vocab_rows * width, bytes_accessed=4 * vocab_rows * width, transcendentals=0
        ),
    )(chips, in_hbm(w))


def rows_kernel(chips, w, tall, turned, sem):
    step = pl.program_id(0)
    size = w.shape[1]
    turned[pl.ds(pl.multiple_of(step * size, size), size)] = w[...].T

    @pl.when(step == pl.num_programs(0) - 1)
    def _():
        for g, group in enumerate(GROUPS):
            for l in range(8):
                at = l * sum(SIZES) + STARTS[g]
                for s, count, first in group:
                    src = pl.multiple_of(chips[64 * g + 8 * l + s] * 64 + first, 16)
                    pltpu.make_async_copy(
                        turned.at[pl.ds(src, count)], tall.at[pl.ds(at, count)], sem
                    ).start()
                    at += count
        pltpu.make_async_copy(tall, tall, sem).wait()


def rows_turned(chips, w):
    vocab_rows, width = w.shape
    size = width // 8
    return pl.pallas_call(
        rows_kernel,
        grid_spec=pltpu.PrefetchScalarGridSpec(
            num_scalar_prefetch=1,
            grid=(8,),
            in_specs=[pl.BlockSpec((vocab_rows, size), lambda i, t: (0, i))],
            out_specs=pl.BlockSpec(memory_space=pl.ANY),
            scratch_shapes=[pltpu.VMEM((width, vocab_rows), BF16), pltpu.SemaphoreType.DMA],
        ),
        out_shape=pltpu.HBM((width, vocab_rows), BF16),
        compiler_params=pltpu.CompilerParams(
            dimension_semantics=("arbitrary",), vmem_limit_bytes=24 << 20
        ),
        cost_estimate=pl.CostEstimate(
            flops=1024 * vocab_rows * width, bytes_accessed=4 * vocab_rows * width, transcendentals=0
        ),
    )(chips, in_hbm(w))


def half_copies(got, h):
    size = sum(SIZES)
    for l in range(4):
        for g in range(3):
            src = got[2 * g + l // 2].at[pl.ds((l % 2) * SIZES[g], SIZES[g])]
            yield src, h.at[pl.ds(l * size + STARTS[g], SIZES[g])]


def early_kernel(*refs):
    got, (w, part, h, sem) = refs[:6], refs[6:]

    @pl.when(pl.program_id(0) == 0)
    def _():
        for src, dst in half_copies(got, h):
            pltpu.make_async_copy(src, dst, sem).start()
        pltpu.make_async_copy(h, h, sem).wait()

    part[...] = jnp.dot(w[...], h[...], preferred_element_type=F32)


def late_kernel(*refs):
    got, (w, part, tgt, logits, stats, h, top, total, hit, sem) = refs[:6], refs[6:]
    step = pl.program_id(0)
    rows, tokens = logits.shape

    @pl.when(step == 0)
    def _():
        for k, (src, dst) in enumerate(half_copies(got, h)):
            pltpu.make_async_copy(src, dst, sem.at[k // 3]).start()
        top[...] = jnp.full(top.shape, -jnp.inf, F32)
        total[...] = jnp.zeros(total.shape, F32)
        hit[...] = jnp.zeros(hit.shape, F32)
        logits[...] = part[...]
        for l in range(4):
            some = pl.ds(l * sum(SIZES), sum(SIZES))
            pltpu.make_async_copy(h.at[some], h.at[some], sem.at[l]).wait()
            logits[...] += jnp.dot(w[:, some], h[some, :], preferred_element_type=F32)

    @pl.when(step > 0)
    def _():
        logits[...] = part[...] + jnp.dot(w[...], h[...], preferred_element_type=F32)

    block = logits[...]
    at = lax.broadcasted_iota(jnp.int32, block.shape, 0) + step * rows
    hit[...] += jnp.sum(jnp.where(at == tgt[...], block, F32(0.0)), axis=0, keepdims=True)
    now = jnp.maximum(top[...], jnp.max(block, axis=0, keepdims=True))
    added = jnp.sum(jnp.exp(block - now), axis=0, keepdims=True)
    total[...] = total[...] * jnp.exp(top[...] - now) + added
    top[...] = now

    @pl.when(step == pl.num_programs(0) - 1)
    def _():
        lse = top[...] + jnp.log(total[...])
        both = [r[:, k : k + 128] for r in (lse, hit[...]) for k in range(0, tokens, 128)]
        stats[...] = jnp.broadcast_to(jnp.concatenate(both, axis=0)[None], stats.shape)


LOGIT_ROWS = 512


def half_logits(half, got, wide, part=None, tgt=None):
    vocab_rows, width = wide.shape
    tokens = got[0].shape[1]
    rows, lines = LOGIT_ROWS, 2 * tokens // 128
    block = pl.BlockSpec((rows, tokens), lambda i: (i, 0))
    row = pl.BlockSpec((1, tokens), lambda i: (0, 0))
    late = part is not None
    return pl.pallas_call(
        late_kernel if late else early_kernel,
        grid=(vocab_rows // rows,),
        in_specs=[pl.BlockSpec(memory_space=pl.ANY)] * len(got)
        + [pl.BlockSpec((rows, width // 2), lambda i: (i, half))]
        + ([block, row] if late else []),
        out_specs=[block, pl.BlockSpec((64, lines, 128), lambda i: (0, 0, 0))] if late else block,
        out_shape=[
            pltpu.HBM((vocab_rows, tokens), F32), jax.ShapeDtypeStruct((64, lines, 128), F32),
        ] if late else jax.ShapeDtypeStruct((vocab_rows, tokens), F32),
        scratch_shapes=[pltpu.VMEM((width // 2, tokens), BF16)]
        + [pltpu.VMEM((1, tokens), F32)] * (3 if late else 0)
        + [pltpu.SemaphoreType.DMA((4,)) if late else pltpu.SemaphoreType.DMA],
        compiler_params=pltpu.CompilerParams(
            dimension_semantics=("arbitrary",), vmem_limit_bytes=32 << 20
        ),
        cost_estimate=pl.CostEstimate(
            flops=vocab_rows * width * tokens,
            bytes_accessed=width * (vocab_rows + tokens) + 4 * vocab_rows * tokens,
            transcendentals=vocab_rows * tokens,
        ),
    )(*got, in_hbm(wide), *([part, tgt] if late else []))


def signal_kernel(stats, logits, cot, tgt, tall, grad, loss, *refs):
    outs, (row, whole) = refs[:3], refs[3:]
    step = pl.program_id(0)
    rows, tokens = logits.shape
    lines = tokens // 128
    count = whole.shape[0] // rows

    @pl.when(step == 0)
    def _():
        lse = stats[:, :lines]
        top = jnp.max(lse, axis=0)
        full = top + jnp.log(jnp.sum(jnp.exp(lse - top[None]), axis=0))
        tok = full - jnp.sum(stats[:, lines:], axis=0)
        row[...] = jnp.concatenate([full[k : k + 1] for k in range(lines)], axis=1)
        loss[...] = jnp.concatenate([tok[k : k + 1] for k in range(lines)], axis=1)

    @pl.when(step < count)
    def _():
        block = logits[...]
        at = lax.broadcasted_iota(jnp.int32, block.shape, 0) + step * rows
        one = jnp.where(at == tgt[...], F32(1.0), F32(0.0))
        done = (cot[...] * (jnp.exp(block - row[...]) - one)).astype(BF16)
        grad[...] = done
        whole[pl.ds(pl.multiple_of(step * rows, rows), rows)] = done

    @pl.when(step >= count)
    def _():
        block = jnp.dot(tall[...], whole[...], preferred_element_type=F32).astype(BF16)
        for start, size, out in zip(STARTS, SIZES, outs):
            out[...] = block[start : start + size]


def signal_of(stats, logits, cot, tgt, tall):
    vocab_rows, tokens = logits.shape
    width = tall.shape[0]
    rows = 256
    count = vocab_rows // rows
    early = lambda i: jnp.minimum(i, count - 1)
    late = lambda i: jnp.maximum(i - count, 0)
    whole = lambda *shape: pl.BlockSpec(shape, lambda i: (0,) * len(shape))
    grad, loss, *sums = pl.pallas_call(
        signal_kernel,
        grid=(count + 4,),
        in_specs=[
            whole(*stats.shape),
            pl.BlockSpec((rows, tokens), lambda i: (early(i), 0)),
            whole(1, tokens),
            whole(1, tokens),
            pl.BlockSpec((width // 8, vocab_rows), lambda i: (4 + late(i), 0)),
        ],
        out_specs=[pl.BlockSpec((rows, tokens), lambda i: (early(i), 0)), whole(1, tokens)]
        + [pl.BlockSpec((None, size, tokens), lambda i: (late(i), 0, 0)) for size in SIZES],
        out_shape=[
            pltpu.HBM((vocab_rows, tokens), BF16),
            jax.ShapeDtypeStruct((1, tokens), F32),
        ] + [pltpu.HBM((4, size, tokens), BF16) for size in SIZES],
        scratch_shapes=[pltpu.VMEM((1, tokens), F32), pltpu.VMEM((vocab_rows, tokens), BF16)],
        compiler_params=pltpu.CompilerParams(
            dimension_semantics=("arbitrary",), vmem_limit_bytes=ALL_VMEM
        ),
        cost_estimate=pl.CostEstimate(
            flops=vocab_rows * width * tokens,
            bytes_accessed=6 * vocab_rows * tokens + width * (vocab_rows + tokens),
            transcendentals=vocab_rows * tokens,
        ),
    )(stats, in_hbm(logits), cot, tgt, in_hbm(tall))
    return grad, loss, sums


def grad_kernel(tall, grad, *outs):
    block = jnp.dot(tall[...], grad[...], preferred_element_type=F32).astype(BF16)
    for start, size, out in zip(STARTS, SIZES, outs):
        out[...] = block[start : start + size]


def half_grads(half, tall, grad):
    vocab_rows, tokens = grad.shape
    width = tall.shape[0]
    return pl.pallas_call(
        grad_kernel,
        grid=(4,),
        in_specs=[
            pl.BlockSpec((width // 8, vocab_rows), lambda i: (4 * half + i, 0)),
            pl.BlockSpec((vocab_rows, tokens), lambda i: (0, 0)),
        ],
        out_specs=[pl.BlockSpec((None, size, tokens), lambda i: (i, 0, 0)) for size in SIZES],
        out_shape=[pltpu.HBM((4, size, tokens), BF16) for size in SIZES],
        compiler_params=pltpu.CompilerParams(
            dimension_semantics=("arbitrary",), vmem_limit_bytes=ALL_VMEM
        ),
        cost_estimate=pl.CostEstimate(
            flops=vocab_rows * width * tokens, bytes_accessed=width * (vocab_rows + tokens),
            transcendentals=0,
        ),
    )(in_hbm(tall), grad)


def body(hidden, head_weight, targets, loss_cot):
    vocab_rows, _ = head_weight.shape
    own = hidden.T
    feats, tokens = own.shape
    core = lax.axis_index("dp")
    chips = lax.dynamic_index_in_dim(jnp.asarray(CHIPS), lax.axis_index(ALL), 0, keepdims=False)
    tgt = (targets - lax.axis_index(VOCAB) * vocab_rows)[None, :]
    some = small_stage(jnp.broadcast_to(own[None], (8, feats, tokens)))
    wide = columns_turned(chips, head_weight)
    got = gathered_groups(some.reshape(8 * feats, tokens))
    part = half_logits(0, [a for group in got for a in group[:2]], wide)
    logits, stats = half_logits(1, [a for group in got for a in group[2:]], wide, part, tgt)
    stats = lax.all_to_all(stats, VOCAB, 0, 0, tiled=True)
    tall = rows_turned(chips, head_weight)
    a_part = a_part_of(chips, [a for group in got for a in group], own)
    grad, tok_loss, sends = signal_of(stats, logits, loss_cot[None, :], tgt, tall)
    sums = summed_groups(sends, half_grads(0, tall, grad))
    sums = small_stage(sums.reshape(8, feats, tokens))
    hidden_grad = summed(sums).T
    rows = vocab_rows // 2

    def gram(x):
        mine = lax.dynamic_slice_in_dim(x, core * rows, rows, 0)
        return lax.dot_general(mine, x, (((1,), (1,)), ((), ())), preferred_element_type=F32)

    g_factor = (gram(grad) + gram(lax.ppermute(grad, "dp", SWAP))) / TOK_DEV
    a_factor = (a_part + lax.ppermute(a_part, "dp", SWAP)) / TOK_DEV
    return (tok_loss[0], hidden_grad, g_factor, a_factor)


def solution(mesh):
    finer = Mesh(mesh.devices.reshape(4, 4, 4, mesh.shape["dp"]), ALL)
    return jax.shard_map(
        body,
        mesh=finer,
        in_specs=(P("dp", VOCAB), P(VOCAB, None), P("dp"), P("dp")),
        out_specs=(P("dp"), P("dp", VOCAB), P(ALL, None), P(VOCAB, None)),
        check_vma=False,
    )
```
